32 devices in a mesh: ctx: 16 (over z, x, core), fsdp: 2 (over y).
Axes of the slice: x: 2, y: 2, z: 4, core: 2. Of those that a mesh axis runs over, the one named last changes fastest.
Arguments:
- block_input: bfloat16 [2, 2048, 1536], P('fsdp', 'ctx'), may hold values from -6 to 6
- out_grad: bfloat16 [2, 2048, 1536], P('fsdp', 'ctx'), may hold values from -6 to 6
- block_ids: int32 [32], replicated, may hold values from 0 to 31, as said below
- gain_attn: bfloat16 [1536], P('fsdp'), may hold values from 0.25 to 1.75
- gain_ffn: bfloat16 [1536], P('fsdp'), may hold values from 0.25 to 1.75
- w_query: bfloat16 [1536, 1536], P('fsdp')
- key_weight: bfloat16 [1536, 768], P('fsdp')
- value_weight: bfloat16 [1536, 768], P('fsdp'), may hold values from -0.15625 to 0.15625
- w_out: bfloat16 [1536, 1536], P(None, 'fsdp'), may hold values from -2.5 to 2.5
- w_gate: bfloat16 [1536, 4096], P(None, 'fsdp'), may hold values from -0.15625 to 0.15625
- w_up: bfloat16 [1536, 4096], P(None, 'fsdp'), may hold values from -0.15625 to 0.15625
- w_down: bfloat16 [4096, 1536], P('fsdp'), may hold values from -0.09375 to 0.09375
Outputs:
- block_output: bfloat16 [2, 2048, 1536], P('fsdp', 'ctx')
- input_grad: float32 [2, 2048, 1536], P('fsdp', 'ctx')
- gain_attn_grad: float32 [1536], P(('ctx', 'fsdp'))
- gain_ffn_grad: float32 [1536], P(('ctx', 'fsdp'))
- grad_query: float32 [1536, 1536], P(('ctx', 'fsdp'))
- grad_key: float32 [1536, 768], P(('ctx', 'fsdp'))
- grad_value: float32 [1536, 768], P(('ctx', 'fsdp'))
- grad_out: float32 [1536, 1536], P(None, ('ctx', 'fsdp'))
- grad_gate: float32 [1536, 4096], P('ctx', 'fsdp')
- grad_up: float32 [1536, 4096], P('ctx', 'fsdp')
- grad_down: float32 [4096, 1536], P('fsdp', 'ctx')
The draws below stay inside these ranges and needn't reach their ends.
Inputs may be any that keep to these rules, and one draw needn't show every extreme that they name: block_ids is a permutation of the 32 blocks; entries 2i and 2i + 1 are a mirrored pair b and 31 - b, in either order.
All inputs are finite; a program needn't handle non-finite values.
Results may differ from the reference program's by a relative error of at most 0.014.
Values may be sent and summed in bfloat16 or wider, within the bound.
A program may use at most 576 MiB of HBM per device.

```python
import math
import jax
import jax.numpy as jnp
from jax import lax

MODEL_DIM = 1536
QUERY_HEADS = 16
KEY_HEADS = 8
HEAD_SIZE = 96
FF = 4096
BLK = 64
NBLK = 32
SEQUENCE_TOKENS = 2048
N_FSDP = 2


def paired_weights(key):
    key_sample = jax.random.normal(jax.random.fold_in(key, 11), (MODEL_DIM, KEY_HEADS * HEAD_SIZE), jnp.float32) * MODEL_DIM ** (-0.5)
    noise = jax.random.normal(jax.random.fold_in(key, 12), (MODEL_DIM, QUERY_HEADS * HEAD_SIZE), jnp.float32) * MODEL_DIM ** (-0.5)
    query_draw = noise
    return (query_draw, key_sample)


def draw_w_query(key, part):
    return paired_weights(key)[0].astype(jnp.bfloat16)


def draw_key_weight(key, part):
    return paired_weights(key)[1].astype(jnp.bfloat16)


def draw_block_ids(key, part):
    pairs = NBLK // 2
    order = jax.random.permutation(jax.random.fold_in(key, 21), pairs).astype(jnp.int32)
    flips = jax.random.randint(jax.random.fold_in(key, 22), (pairs,), 0, 2).astype(jnp.int32)
    first = jnp.where(flips == 1, NBLK - 1 - order, order)
    second = NBLK - 1 - first
    return jnp.stack([first, second], axis=1).reshape(NBLK).astype(jnp.int32)


def spiked(array, rng, source, target, shards_of, factor):
    def block_of(dim):
        return (jnp.arange(array.shape[dim]) // (array.shape[dim] // shards_of)).reshape((-1,) + (1,) * (array.ndim - 1 - dim))

    one_side = jax.random.permutation(rng, shards_of)[block_of(target)]
    other_side = (block_of(target) + shards_of // 2) % shards_of
    return jnp.where((block_of(source) == one_side) | (block_of(source) == other_side), factor * array, array)


def level_of(rng, shape, cuts, low, largest):
    factor_of, own = 1.0, jax.random.fold_in(rng, 6)
    for dim, shards_of in cuts:
        draws = jnp.exp(jax.random.uniform(jax.random.fold_in(own, dim), (shards_of,), jnp.float32, low / len(cuts), largest / len(cuts)))
        factor_of = factor_of * jnp.repeat(draws, shape[dim] // shards_of).reshape([-1 if axis == dim else 1 for axis in range(len(shape))])
    return factor_of


def scatter_about(rng, dims, scale, reach, shards=(), kind=jnp.bfloat16):
    loudness = level_of(rng, dims, shards, -0.22, 0.18) if shards else 1.0
    entries = jax.random.normal(rng, dims, jnp.float32) * scale * loudness
    return jnp.minimum(jnp.maximum(entries, -reach), reach).astype(kind)


def bell_draw_with(key, dims, deviation, reach, split, heavy, kind=jnp.bfloat16):
    result = deviation * jax.random.normal(key, dims, jnp.float32)
    if split:
        result = result * level_of(key, dims, split, -0.22, 0.18)
    return jnp.clip(spiked(result, jax.random.fold_in(key, 3), *heavy), -reach, reach).astype(kind)


def setup_inputs(seed: int = 0) -> dict:
    keys = jax.random.split(jax.random.key(seed), 13)
    return {
        "block_input": scatter_about(keys[0], (N_FSDP, SEQUENCE_TOKENS, MODEL_DIM), 1.0, 6.0, ((0, 2), (1, 16))),
        "out_grad": bell_draw_with(keys[1], (N_FSDP, SEQUENCE_TOKENS, MODEL_DIM), 1.0, 6.0, ((0, 2), (1, 16)), (1, 2, 16, 2.0)),
        "block_ids": draw_block_ids(jax.random.fold_in(keys[12], 71), 0),
        "gain_attn": jnp.clip(1.0 + 0.15 * jax.random.normal(keys[3], (MODEL_DIM,), jnp.float32), 0.25, 1.75).astype(jnp.bfloat16),
        "gain_ffn": jnp.clip(1.0 + 0.15 * jax.random.normal(keys[4], (MODEL_DIM,), jnp.float32), 0.25, 1.75).astype(jnp.bfloat16),
        "w_query": draw_w_query(jax.random.fold_in(keys[12], 71), 0),
        "key_weight": draw_key_weight(jax.random.fold_in(keys[12], 71), 0),
        "value_weight": scatter_about(keys[7], (MODEL_DIM, KEY_HEADS * HEAD_SIZE), MODEL_DIM ** -0.5, 0.15625, ((0, 2),)),
        "w_out": scatter_about(keys[8], (QUERY_HEADS * HEAD_SIZE, MODEL_DIM), (max(1, 8 * QUERY_HEADS * HEAD_SIZE // SEQUENCE_TOKENS)) ** -0.5, 2.5, ((1, 2),)),
        "w_gate": scatter_about(keys[9], (MODEL_DIM, FF), MODEL_DIM ** -0.5, 0.15625, ((1, 2),)),
        "w_up": scatter_about(keys[10], (MODEL_DIM, FF), MODEL_DIM ** -0.5, 0.15625, ((1, 2),)),
        "w_down": scatter_about(keys[11], (FF, MODEL_DIM), FF ** -0.5, 0.09375, ((0, 2),)),
    }


EPS = 1e-05
THETA = 100000.0
NEGATIVE_FLOOR = -1e+30

def rounded(value):
    return lax.optimization_barrier(value.astype(jnp.bfloat16)).astype(jnp.float32)

def half_turn(value):
    half = value.shape[-1] // 2
    return jnp.concatenate([-value[..., half:], value[..., :half]], axis=-1)

def angle_tables(positions, head_width):
    half = head_width // 2
    freq = jnp.exp(-math.log(THETA) * 2.0 * jnp.arange(half, dtype=jnp.float32) / head_width)
    angles = positions.astype(jnp.float32)[:, None] * freq[None, :]
    cosine_table = jnp.cos(angles)
    sine_table = jnp.sin(angles)
    return (jnp.concatenate([cosine_table, cosine_table], axis=-1), jnp.concatenate([sine_table, sine_table], axis=-1))

def apply_rotary(value, cosine_table, sine_table):
    return value * cosine_table[:, None, :] + half_turn(value) * sine_table[:, None, :]

def inverse_rotary(value, cosine_table, sine_table):
    return value * cosine_table[:, None, :] - half_turn(value) * sine_table[:, None, :]

def norm_stats(value):
    inverse = lax.rsqrt(lax.optimization_barrier(jnp.mean(value * value, axis=-1, keepdims=True)) + EPS)
    return (value * inverse, inverse)

def norm_back(grad, normed, inverse, gain):
    scaled = grad * gain
    return inverse * (scaled - normed * lax.optimization_barrier(jnp.mean(scaled * normed, axis=-1, keepdims=True)))

def attend_forward(query_matrix, key_collection, value_collection):
    heads_per_group = QUERY_HEADS // KEY_HEADS
    query_row_span = min(256, SEQUENCE_TOKENS)
    query_count = SEQUENCE_TOKENS // query_row_span
    score_scale = HEAD_SIZE ** (-0.5)
    key_f = key_collection.astype(jnp.float32)
    value_f = value_collection.astype(jnp.float32)
    key_pos = jnp.arange(SEQUENCE_TOKENS, dtype=jnp.int32)
    pile_rows = query_matrix.reshape(query_count, query_row_span, KEY_HEADS, heads_per_group, HEAD_SIZE)

    def one_block(inputs):
        query_blk, blk_index = inputs
        query_pos = blk_index * query_row_span + jnp.arange(query_row_span, dtype=jnp.int32)
        scores = jnp.einsum('qgrd,kgd->grqk', query_blk.astype(jnp.float32), key_f) * score_scale
        scores = jnp.where(key_pos[None, :] <= query_pos[:, None], scores, NEGATIVE_FLOOR)
        row_max = lax.optimization_barrier(jnp.max(scores, axis=-1, keepdims=True))
        log_sum = row_max[..., 0] + jnp.log(lax.optimization_barrier(jnp.sum(jnp.exp(scores - row_max), axis=-1)))
        weights = rounded(jnp.exp(scores - log_sum[..., None]))
        blended = jnp.einsum('grqk,kgd->qgrd', weights, value_f)
        return (blended.reshape(query_row_span, QUERY_HEADS * HEAD_SIZE).astype(jnp.bfloat16), log_sum)
    blended, log_sum = lax.map(one_block, (pile_rows, jnp.arange(query_count, dtype=jnp.int32)))
    return (blended.reshape(SEQUENCE_TOKENS, QUERY_HEADS * HEAD_SIZE), log_sum)

def attend_backward(query_matrix, key_collection, value_collection, blended_gradient, log_sum, product_total):
    heads_per_group = QUERY_HEADS // KEY_HEADS
    query_row_span = min(256, SEQUENCE_TOKENS)
    query_count = SEQUENCE_TOKENS // query_row_span
    score_scale = HEAD_SIZE ** (-0.5)
    key_f = key_collection.astype(jnp.float32)
    value_f = value_collection.astype(jnp.float32)
    key_pos = jnp.arange(SEQUENCE_TOKENS, dtype=jnp.int32)
    pile_query = query_matrix.reshape(query_count, query_row_span, KEY_HEADS, heads_per_group, HEAD_SIZE)
    pile_gradient = blended_gradient.reshape(query_count, query_row_span, KEY_HEADS, heads_per_group, HEAD_SIZE)

    def one_block(carry, inputs):
        key_gradient, value_gradient = carry
        query_blk, grad_blk, lse_blk, delta_blk, blk_index = inputs
        query_f = query_blk.astype(jnp.float32)
        grad_f = grad_blk.astype(jnp.float32)
        query_pos = blk_index * query_row_span + jnp.arange(query_row_span, dtype=jnp.int32)
        scores = jnp.einsum('qgrd,kgd->grqk', query_f, key_f) * score_scale
        scores = jnp.where(key_pos[None, :] <= query_pos[:, None], scores, NEGATIVE_FLOOR)
        probs = jnp.exp(scores - lse_blk[..., None])
        weights = rounded(probs)
        grad_probs = jnp.einsum('qgrd,kgd->grqk', grad_f, value_f)
        grad_scores = rounded(probs * (grad_probs - delta_blk[..., None]) * score_scale)
        query_grad = jnp.einsum('grqk,kgd->qgrd', grad_scores, key_f)
        key_gradient = key_gradient + jnp.einsum('grqk,qgrd->kgd', grad_scores, query_f)
        value_gradient = value_gradient + jnp.einsum('grqk,qgrd->kgd', weights, grad_f)
        return ((key_gradient, value_gradient), query_grad.reshape(query_row_span, QUERY_HEADS, HEAD_SIZE))
    zero_filled = jnp.zeros((SEQUENCE_TOKENS, KEY_HEADS, HEAD_SIZE), jnp.float32)
    (key_gradient, value_gradient), query_grad = lax.scan(one_block, (zero_filled, zero_filled), (pile_query, pile_gradient, log_sum, product_total, jnp.arange(query_count, dtype=jnp.int32)))
    return (query_grad.reshape(SEQUENCE_TOKENS, QUERY_HEADS, HEAD_SIZE), key_gradient, value_gradient)

def one_sequence(tokens, cotan, cosine_table, sine_table, gain_one, gain_two, w_query, key_weight, value_weight, w_out, w_gate, w_up, w_down):
    heads_per_group = QUERY_HEADS // KEY_HEADS
    query_row_span = min(256, SEQUENCE_TOKENS)
    query_count = SEQUENCE_TOKENS // query_row_span
    resid_in = tokens.astype(jnp.float32)
    normed_one, inverse_one = norm_stats(resid_in)
    normalized_input = (normed_one * gain_one).astype(jnp.bfloat16)
    query_matrix = apply_rotary(jnp.dot(normalized_input, w_query, preferred_element_type=jnp.float32).reshape(SEQUENCE_TOKENS, QUERY_HEADS, HEAD_SIZE), cosine_table, sine_table).astype(jnp.bfloat16)
    key_collection = apply_rotary(jnp.dot(normalized_input, key_weight, preferred_element_type=jnp.float32).reshape(SEQUENCE_TOKENS, KEY_HEADS, HEAD_SIZE), cosine_table, sine_table).astype(jnp.bfloat16)
    value_collection = jnp.dot(normalized_input, value_weight, preferred_element_type=jnp.float32).astype(jnp.bfloat16).reshape(SEQUENCE_TOKENS, KEY_HEADS, HEAD_SIZE)
    blended, log_sum = attend_forward(query_matrix, key_collection, value_collection)
    resid_mid = resid_in + jnp.dot(blended, w_out, preferred_element_type=jnp.float32)
    normed_two, inverse_two = norm_stats(resid_mid)
    normed_mid = (normed_two * gain_two).astype(jnp.bfloat16)
    gate_act = jnp.dot(normed_mid, w_gate, preferred_element_type=jnp.float32)
    up_act = jnp.dot(normed_mid, w_up, preferred_element_type=jnp.float32)
    gate_sig = jax.nn.sigmoid(gate_act)
    gate_silu = gate_act * gate_sig
    hidden = (gate_silu * up_act).astype(jnp.bfloat16)
    output = (resid_mid + jnp.dot(hidden, w_down, preferred_element_type=jnp.float32)).astype(jnp.bfloat16)
    down_grad = jnp.dot(hidden.T, cotan, preferred_element_type=jnp.float32)
    hidden_grad = jnp.dot(cotan, w_down.T, preferred_element_type=jnp.float32)
    gate_grad = (hidden_grad * up_act * gate_sig * (1.0 + gate_act * (1.0 - gate_sig))).astype(jnp.bfloat16)
    up_grad = (hidden_grad * gate_silu).astype(jnp.bfloat16)
    wgate_grad = jnp.dot(normed_mid.T, gate_grad, preferred_element_type=jnp.float32)
    wup_grad = jnp.dot(normed_mid.T, up_grad, preferred_element_type=jnp.float32)
    normed_grad = jnp.dot(gate_grad, w_gate.T, preferred_element_type=jnp.float32) + jnp.dot(up_grad, w_up.T, preferred_element_type=jnp.float32)
    gain_two_grad = lax.optimization_barrier(jnp.sum(normed_grad * normed_two, axis=0))
    mid_grad = cotan.astype(jnp.float32) + norm_back(normed_grad, normed_two, inverse_two, gain_two)
    mid_grad_b = mid_grad.astype(jnp.bfloat16)
    wout_grad = jnp.dot(blended.T, mid_grad_b, preferred_element_type=jnp.float32)
    blended_gradient_rows = jnp.dot(mid_grad_b, w_out.T, preferred_element_type=jnp.float32).astype(jnp.bfloat16)
    product_total = lax.optimization_barrier(jnp.sum(blended_gradient_rows.astype(jnp.float32).reshape(SEQUENCE_TOKENS, KEY_HEADS, heads_per_group, HEAD_SIZE) * blended.astype(jnp.float32).reshape(SEQUENCE_TOKENS, KEY_HEADS, heads_per_group, HEAD_SIZE), axis=-1))
    product_total = product_total.reshape(query_count, query_row_span, KEY_HEADS, heads_per_group).transpose(0, 2, 3, 1)
    query_grad, key_gradient, value_gradient = attend_backward(query_matrix, key_collection, value_collection, blended_gradient_rows.reshape(SEQUENCE_TOKENS, QUERY_HEADS, HEAD_SIZE), log_sum, product_total)
    query_grad = inverse_rotary(query_grad, cosine_table, sine_table).astype(jnp.bfloat16).reshape(SEQUENCE_TOKENS, QUERY_HEADS * HEAD_SIZE)
    key_gradient = inverse_rotary(key_gradient, cosine_table, sine_table).astype(jnp.bfloat16).reshape(SEQUENCE_TOKENS, KEY_HEADS * HEAD_SIZE)
    value_gradient = value_gradient.astype(jnp.bfloat16).reshape(SEQUENCE_TOKENS, KEY_HEADS * HEAD_SIZE)
    wq_grad = jnp.dot(normalized_input.T, query_grad, preferred_element_type=jnp.float32)
    wk_grad = jnp.dot(normalized_input.T, key_gradient, preferred_element_type=jnp.float32)
    wv_grad = jnp.dot(normalized_input.T, value_gradient, preferred_element_type=jnp.float32)
    in_normed_grad = jnp.dot(query_grad, w_query.T, preferred_element_type=jnp.float32) + jnp.dot(key_gradient, key_weight.T, preferred_element_type=jnp.float32) + jnp.dot(value_gradient, value_weight.T, preferred_element_type=jnp.float32)
    gain_one_grad = lax.optimization_barrier(jnp.sum(in_normed_grad * normed_one, axis=0))
    input_grad = mid_grad + norm_back(in_normed_grad, normed_one, inverse_one, gain_one)
    return (output, input_grad, (gain_one_grad, gain_two_grad, wq_grad, wk_grad, wv_grad, wout_grad, wgate_grad, wup_grad, down_grad))

def reference(block_input, out_grad, block_ids, gain_attn, gain_ffn, w_query, key_weight, value_weight, w_out, w_gate, w_up, w_down):
    block_range = jnp.arange(NBLK, dtype=jnp.int32)
    natural_order_at = lax.optimization_barrier(jnp.sum(jnp.where(block_ids[None, :] == block_range[:, None], block_range[None, :], 0), axis=1)).astype(jnp.int32)
    gain_one = gain_attn.astype(jnp.float32)
    gain_two = gain_ffn.astype(jnp.float32)
    cosine_table, sine_table = angle_tables(jnp.arange(SEQUENCE_TOKENS, dtype=jnp.int32), HEAD_SIZE)
    outputs = []
    in_grads = []
    totals = None
    for seq_index in range(N_FSDP):
        tokens = jnp.take(block_input[seq_index].reshape(NBLK, BLK, MODEL_DIM), natural_order_at, axis=0).reshape(SEQUENCE_TOKENS, MODEL_DIM)
        cotan = jnp.take(out_grad[seq_index].reshape(NBLK, BLK, MODEL_DIM), natural_order_at, axis=0).reshape(SEQUENCE_TOKENS, MODEL_DIM)
        output, input_grad, grads = one_sequence(tokens, cotan, cosine_table, sine_table, gain_one, gain_two, w_query, key_weight, value_weight, w_out, w_gate, w_up, w_down)
        outputs.append(jnp.take(output.reshape(NBLK, BLK, MODEL_DIM), block_ids, axis=0).reshape(SEQUENCE_TOKENS, MODEL_DIM))
        in_grads.append(jnp.take(input_grad.reshape(NBLK, BLK, MODEL_DIM), block_ids, axis=0).reshape(SEQUENCE_TOKENS, MODEL_DIM))
        totals = grads if totals is None else tuple((left + right for left, right in zip(totals, grads)))
    return (jnp.stack(outputs), jnp.stack(in_grads), totals[0], totals[1], totals[2], totals[3], totals[4], totals[5], totals[6], totals[7], totals[8])
```

```python
import functools
import math

import jax
import jax.numpy as jnp
import numpy as np
from jax import lax
from jax.experimental import pallas as pl
from jax.experimental.pallas import tpu as pltpu
from jax.sharding import PartitionSpec as P

QUERY_HEADS = 16
KEY_HEADS = 8
HEAD_SIZE = 96
GROUP = QUERY_HEADS // KEY_HEADS
LANES = 128
HEADS_STEP = 4
TILE_BLOCKS = 4

EPS = 1e-05
THETA = 100000.0
NEGATIVE_FLOOR = -1e30
LOG2E = math.log2(math.e)
SCALE = HEAD_SIZE ** (-0.5)
VMEM_BYTES = 66_000_000

F32 = jnp.float32
BF16 = jnp.bfloat16


def dot_nn(left, right):
    return lax.dot_general(left, right, (((1,), (0,)), ((), ())), preferred_element_type=F32)


def dot_nt(left, right):
    return lax.dot_general(left, right, (((1,), (1,)), ((), ())), preferred_element_type=F32)


def dot_tn(left, right):
    return lax.dot_general(left, right, (((0,), (0,)), ((), ())), preferred_element_type=F32)


def frequency_row(width):
    lane = np.arange(width)
    half = HEAD_SIZE // 2
    freq = np.exp(-math.log(THETA) * 2.0 * (lane % HEAD_SIZE % half) / HEAD_SIZE)
    return freq.astype(np.float32)


def sign_row(width):
    lane = np.arange(width)
    return np.where(lane % HEAD_SIZE < HEAD_SIZE // 2, -1.0, 1.0).astype(np.float32)


def swap_halves(value):
    width = value.shape[1]
    half = HEAD_SIZE // 2
    lane = lax.broadcasted_iota(jnp.int32, value.shape, 1)
    lower = lax.rem(lane, HEAD_SIZE) < half
    return jnp.where(lower, pltpu.roll(value, width - half, 1), pltpu.roll(value, half, 1))


def rotary_kernel(sign, first, second, cosine, sine, out):
    total = first[...].astype(F32) + second[...].astype(F32)
    out[...] = (total * cosine[...] + sign * swap_halves(total) * sine[...]).astype(BF16)


def rotary_sum(first, second, cosine, sine):
    rows, width = first.shape
    part = cosine.shape[1]
    spec = pl.BlockSpec((rows, part), lambda i: (0, i))
    table = pl.BlockSpec((rows, part), lambda i: (0, 0))
    return pl.pallas_call(
        functools.partial(rotary_kernel, 1.0),
        out_shape=jax.ShapeDtypeStruct((rows, width), BF16),
        grid=(width // part,),
        in_specs=[spec, spec, table, table],
        out_specs=spec,
        name="rotary_sum",
        cost_estimate=pl.CostEstimate(
            flops=6 * rows * width, bytes_accessed=8 * rows * width, transcendentals=0
        ),
    )(first, second, cosine, sine)


def inverse_rotary_kernel(value, cosine, sine, out):
    total = value[...].astype(F32)
    out[...] = (total * cosine[...] - swap_halves(total) * sine[...]).astype(BF16)


def inverse_rotary(value, cosine, sine):
    return pl.pallas_call(
        inverse_rotary_kernel,
        out_shape=jax.ShapeDtypeStruct(value.shape, BF16),
        name="rotary_back",
        cost_estimate=pl.CostEstimate(
            flops=6 * value.size, bytes_accessed=10 * value.size, transcendentals=0
        ),
    )(value, cosine, sine)


def head_slice(rows, head):
    piece = rows[:, head * HEAD_SIZE : (head + 1) * HEAD_SIZE]
    pad = jnp.zeros((rows.shape[0], LANES - HEAD_SIZE), rows.dtype)
    return jnp.concatenate([piece, pad], axis=1)


def group_rows(rows, key_head):
    return jnp.concatenate(
        [head_slice(rows, key_head * GROUP + r) for r in range(GROUP)], axis=0
    )


def tile_rows(ref, slot_of, tile, block):
    pieces = []
    for i in range(TILE_BLOCKS):
        start = pl.multiple_of(slot_of[tile * TILE_BLOCKS + i] * block, block)
        pieces.append(ref[pl.ds(start, block), :])
    return jnp.concatenate(pieces, axis=0)


def allowed(tile, tile_len, query_block, block, rows):
    key_pos = tile * tile_len + lax.broadcasted_iota(jnp.int32, (tile_len, rows), 0)
    row = lax.broadcasted_iota(jnp.int32, (tile_len, rows), 1)
    query_pos = query_block * block + lax.rem(row, block)
    return key_pos <= query_pos


def fold(value, how):
    return how(value.reshape(value.shape[0] // 8, 8, value.shape[1]), axis=0)


def merge_heads(pieces):
    return jnp.concatenate([piece[:, :HEAD_SIZE] for piece in pieces], axis=1)


def forward_kernel(
    batch, block, slot_of, owned, q_ref, k_ref, v_ref, o_ref, lse_ref, kn, vt, scores, acc, top, total
):
    tile_len = TILE_BLOCKS * block
    rows = GROUP * block
    counts = [(owned[m] + TILE_BLOCKS) // TILE_BLOCKS for m in range(2)]
    most = jnp.maximum(counts[0], counts[1])
    merged = [[None] * (HEADS_STEP * GROUP) for _ in range(2)]
    for first in range(0, HEADS_STEP, batch):

        def pack(tile, carry, first=first):
            k_rows = tile_rows(k_ref, slot_of, tile, block)
            v_rows = tile_rows(v_ref, slot_of, tile, block)
            start = pl.multiple_of(tile * tile_len, tile_len)
            for h in range(batch):
                kn[h, pl.ds(start, tile_len), :] = head_slice(k_rows, first + h)
                vt[h, :, pl.ds(start, tile_len)] = head_slice(v_rows, first + h).T
            return carry

        lax.fori_loop(0, most, pack, 0)
        for m in range(2):
            member = slice(m * block, (m + 1) * block)
            q_rows = q_ref[member, :]
            queries = [group_rows(q_rows, first + h) for h in range(batch)]
            for h in range(batch):
                top[h] = jnp.full((8, rows), NEGATIVE_FLOOR, F32)
                total[h] = jnp.zeros((8, rows), F32)
                acc[h] = jnp.zeros((LANES, rows), F32)

            def score_pass(tile, carry, queries=queries, m=m):
                start = pl.multiple_of(tile * tile_len, tile_len)
                mask = allowed(tile, tile_len, owned[m], block, rows)
                for h in range(batch):
                    value = dot_nt(kn[h, pl.ds(start, tile_len), :], queries[h])
                    value = jnp.where(mask, value * (SCALE * LOG2E), NEGATIVE_FLOOR)
                    scores[h, pl.ds(start, tile_len), :] = value
                    top[h] = jnp.maximum(top[h], fold(value, jnp.max))
                return carry

            lax.fori_loop(0, counts[m], score_pass, 0)
            peaks = [jnp.max(top[h], axis=0, keepdims=True) for h in range(batch)]

            def mix_pass(tile, carry, peaks=peaks):
                start = pl.multiple_of(tile * tile_len, tile_len)
                for h in range(batch):
                    weight = jnp.exp2(scores[h, pl.ds(start, tile_len), :] - peaks[h])
                    total[h] += fold(weight, jnp.sum)
                    acc[h] += dot_nn(vt[h, :, pl.ds(start, tile_len)], weight.astype(BF16))
                return carry

            lax.fori_loop(0, counts[m], mix_pass, 0)
            for h in range(batch):
                denom = jnp.sum(total[h], axis=0, keepdims=True)
                mixed = (acc[h] / denom).T.astype(BF16)
                for r in range(GROUP):
                    merged[m][(first + h) * GROUP + r] = mixed[r * block : (r + 1) * block, :]
                lse_ref[first + h, m : m + 1, :] = peaks[h] + jnp.log2(denom)
    for m in range(2):
        o_ref[m * block : (m + 1) * block, :] = merge_heads(merged[m])


def kv_specs(length, heads_width):
    mode = {} if length <= 4096 else {"pipeline_mode": pl.Buffered(1)}
    return [pl.BlockSpec((length, heads_width), lambda i, *_: (0, i), **mode)] * 2


def attention_forward(query, key, value, slot_of, owned, block):
    rows = query.shape[0]
    length = key.shape[0]
    batch = HEADS_STEP if length <= 4096 else 1
    steps = KEY_HEADS // HEADS_STEP
    key_width = HEADS_STEP * HEAD_SIZE
    query_width = key_width * GROUP
    pairs = GROUP * block
    query_spec = pl.BlockSpec((rows, query_width), lambda i, *_: (0, i))
    return pl.pallas_call(
        functools.partial(forward_kernel, batch, block),
        out_shape=(
            jax.ShapeDtypeStruct(query.shape, BF16),
            jax.ShapeDtypeStruct((KEY_HEADS, 2, pairs), F32),
        ),
        grid_spec=pltpu.PrefetchScalarGridSpec(
            num_scalar_prefetch=2,
            grid=(steps,),
            in_specs=[query_spec] + kv_specs(length, key_width),
            out_specs=[
                query_spec,
                pl.BlockSpec((HEADS_STEP, 2, pairs), lambda i, *_: (i, 0, 0)),
            ],
            scratch_shapes=[
                pltpu.VMEM((batch, length, LANES), BF16),
                pltpu.VMEM((batch, LANES, length), BF16),
                pltpu.VMEM((batch, length, pairs), F32),
                pltpu.VMEM((batch, LANES, pairs), F32),
                pltpu.VMEM((batch, 8, pairs), F32),
                pltpu.VMEM((batch, 8, pairs), F32),
            ],
        ),
        compiler_params=pltpu.CompilerParams(vmem_limit_bytes=VMEM_BYTES),
        name="attention_forward",
        cost_estimate=pl.CostEstimate(
            flops=4 * rows * length * query.shape[1] // 2,
            bytes_accessed=4 * length * key.shape[1],
            transcendentals=rows * length * QUERY_HEADS // 2,
        ),
    )(slot_of, owned, query, key, value)


def backward_kernel(
    batch,
    block,
    slot_of,
    owned,
    order_ids,
    q_ref,
    do_ref,
    o_ref,
    lse_ref,
    cos_ref,
    sin_ref,
    k_ref,
    v_ref,
    dq_ref,
    dk_keep,
    dk_send,
    dv_keep,
    dv_send,
    kn,
    vn,
    kt,
    dk,
    dv,
    acc,
):
    tile_len = TILE_BLOCKS * block
    rows = GROUP * block
    half = dk_keep.shape[0]
    counts = [(owned[m] + TILE_BLOCKS) // TILE_BLOCKS for m in range(2)]
    most = jnp.maximum(counts[0], counts[1])
    merged = [[None] * (HEADS_STEP * GROUP) for _ in range(2)]
    for first in range(0, HEADS_STEP, batch):

        def pack(tile, carry, first=first):
            k_rows = tile_rows(k_ref, slot_of, tile, block)
            v_rows = tile_rows(v_ref, slot_of, tile, block)
            start = pl.multiple_of(tile * tile_len, tile_len)
            for h in range(batch):
                piece = head_slice(k_rows, first + h)
                kn[h, pl.ds(start, tile_len), :] = piece
                kt[h, :, pl.ds(start, tile_len)] = piece.T
                vn[h, pl.ds(start, tile_len), :] = head_slice(v_rows, first + h)
            return carry

        lax.fori_loop(0, most, pack, 0)
        dk[...] = jnp.zeros_like(dk)
        dv[...] = jnp.zeros_like(dv)
        for m in range(2):
            member = slice(m * block, (m + 1) * block)
            q_rows, g_rows, o_rows = q_ref[member, :], do_ref[member, :], o_ref[member, :]
            queries = [group_rows(q_rows, first + h) for h in range(batch)]
            grads = [group_rows(g_rows, first + h) for h in range(batch)]
            deltas = []
            for h in range(batch):
                product = grads[h].astype(F32) * group_rows(o_rows, first + h).astype(F32)
                deltas.append(jnp.sum(product.T, axis=0, keepdims=True))
                acc[h] = jnp.zeros((LANES, rows), F32)
            lses = [lse_ref[first + h, m : m + 1, :] for h in range(batch)]

            def grad_pass(tile, carry, queries=queries, grads=grads, deltas=deltas, lses=lses, m=m):
                start = pl.multiple_of(tile * tile_len, tile_len)
                mask = allowed(tile, tile_len, owned[m], block, rows)
                for h in range(batch):
                    value = dot_nt(kn[h, pl.ds(start, tile_len), :], queries[h])
                    value = jnp.where(mask, value * (SCALE * LOG2E) - lses[h], NEGATIVE_FLOOR)
                    prob = jnp.exp2(value)
                    weight = prob.astype(BF16)
                    grad_prob = dot_nt(vn[h, pl.ds(start, tile_len), :], grads[h])
                    grad_score = (prob * (grad_prob - deltas[h]) * SCALE).astype(BF16)
                    dk[h, pl.ds(start, tile_len), :] += dot_nn(grad_score, queries[h])
                    dv[h, pl.ds(start, tile_len), :] += dot_nn(weight, grads[h])
                    acc[h] += dot_nn(kt[h, :, pl.ds(start, tile_len)], grad_score)
                return carry

            lax.fori_loop(0, counts[m], grad_pass, 0)
            cosine = jnp.concatenate([cos_ref[member, :]] * GROUP, axis=0)
            sine = jnp.concatenate([sin_ref[member, :]] * GROUP, axis=0)
            for h in range(batch):
                grad = acc[h].T
                grad = (grad * cosine - swap_halves(grad) * sine).astype(BF16)
                for r in range(GROUP):
                    merged[m][(first + h) * GROUP + r] = grad[r * block : (r + 1) * block, :]

        def unpack(chunk, carry, first=first, base=0, targets=None):
            for source, target in targets:
                pieces = []
                for h in range(batch):
                    picked = []
                    for i in range(2):
                        start = pl.multiple_of(order_ids[2 * (base + chunk) + i] * block, block)
                        picked.append(source[h, pl.ds(start, block), :].astype(BF16))
                    pieces.append(jnp.concatenate(picked, axis=0))
                lanes = slice(first * HEAD_SIZE, (first + batch) * HEAD_SIZE)
                target[chunk, :, lanes] = merge_heads(pieces)
            return carry

        lax.fori_loop(
            0, half, functools.partial(unpack, base=half, targets=((dk, dk_send), (dv, dv_send))), 0
        )
        lax.fori_loop(
            0, half, functools.partial(unpack, base=0, targets=((dk, dk_keep), (dv, dv_keep))), 0
        )
    for m in range(2):
        dq_ref[m * block : (m + 1) * block, :] = merge_heads(merged[m])


def attention_backward(
    query, grad, mixed, lse, cosine, sine, key, value, slot_of, owned, order_ids, block
):
    rows = query.shape[0]
    length = key.shape[0]
    chunks = length // rows
    batch = HEADS_STEP if length <= 4096 else 1
    steps = KEY_HEADS // HEADS_STEP
    key_width = HEADS_STEP * HEAD_SIZE
    query_width = key_width * GROUP
    pairs = GROUP * block
    query_spec = pl.BlockSpec((rows, query_width), lambda i, *_: (0, i))
    mode = {} if length <= 4096 else {"pipeline_mode": pl.Buffered(1)}
    out_spec = pl.BlockSpec((chunks // 2, rows, key_width), lambda i, *_: (0, 0, i), **mode)
    table = pl.BlockSpec((rows, LANES), lambda i, *_: (0, 0))
    half_shape = jax.ShapeDtypeStruct((chunks // 2, rows, key.shape[1]), BF16)
    return pl.pallas_call(
        functools.partial(backward_kernel, batch, block),
        out_shape=(jax.ShapeDtypeStruct(query.shape, BF16),) + (half_shape,) * 4,
        grid_spec=pltpu.PrefetchScalarGridSpec(
            num_scalar_prefetch=3,
            grid=(steps,),
            in_specs=[
                query_spec,
                query_spec,
                query_spec,
                pl.BlockSpec((HEADS_STEP, 2, pairs), lambda i, *_: (i, 0, 0)),
                table,
                table,
            ]
            + kv_specs(length, key_width),
            out_specs=[query_spec] + [out_spec] * 4,
            scratch_shapes=[
                pltpu.VMEM((batch, length, LANES), BF16),
                pltpu.VMEM((batch, length, LANES), BF16),
                pltpu.VMEM((batch, LANES, length), BF16),
                pltpu.VMEM((batch, length, LANES), F32),
                pltpu.VMEM((batch, length, LANES), F32),
                pltpu.VMEM((batch, LANES, pairs), F32),
            ],
        ),
        compiler_params=pltpu.CompilerParams(vmem_limit_bytes=VMEM_BYTES),
        name="attention_backward",
        cost_estimate=pl.CostEstimate(
            flops=10 * rows * length * query.shape[1] // 2,
            bytes_accessed=8 * length * key.shape[1],
            transcendentals=rows * length * QUERY_HEADS // 2,
        ),
    )(slot_of, owned, order_ids, query, grad, mixed, lse, cosine, sine, key, value)


def swap_fsdp(value):
    size = lax.axis_size("fsdp")
    return lax.ppermute(value, "fsdp", [(i, size - 1 - i) for i in range(size)])


def swap_bit(value, bit):
    size = lax.axis_size("ctx")
    return lax.ppermute(value, "ctx", [(i, i ^ (1 << bit)) for i in range(size)])


def relative_order(size):
    bits = size.bit_length() - 1
    return [sum(((p >> (bits - 1 - b)) & 1) << b for b in range(bits)) for p in range(size)]


def halve(keep, send):
    size = lax.axis_size("ctx")
    for bit in range(size.bit_length() - 1):
        got = swap_bit(send, bit)
        if keep.shape[0] == 1:
            return keep[0].astype(F32) + got[0].astype(F32)
        mid = keep.shape[0] // 2
        send = (keep[mid:].astype(F32) + got[mid:].astype(F32)).astype(got.dtype)
        keep = keep[:mid].astype(F32) + got[:mid].astype(F32)


def chunk_rows(both, order, parts):
    tokens, width = both.shape
    rows = width // parts
    return jnp.take(both.T.reshape(parts, rows, tokens), order, axis=0)


def weight_grad(left, right, chunks):
    rows = left.shape[1]
    half = chunks // 2
    tokens = left.shape[2]

    def piece(part):
        flat = part.reshape(half * rows, tokens)
        return dot_nn(flat, right).astype(BF16).reshape(half, rows, right.shape[1])

    send = piece(left[half:])
    keep = piece(left[:half])
    return halve(keep, send)


def after(value, anchor):
    return lax.optimization_barrier((value, anchor))[0]


def norm_stats(value):
    inverse = lax.rsqrt(jnp.mean(value * value, axis=-1, keepdims=True) + EPS)
    return (value * inverse, inverse)


def norm_back(grad, normed, inverse, gain):
    scaled = grad * gain
    return inverse * (scaled - normed * jnp.mean(scaled * normed, axis=-1, keepdims=True))


def local(
    block_input,
    out_grad,
    block_ids,
    gain_attn,
    gain_ffn,
    w_query,
    key_weight,
    value_weight,
    w_out,
    w_gate,
    w_up,
    w_down,
):
    ctx_size = lax.axis_size("ctx")
    side = lax.axis_index("fsdp")
    me = lax.axis_index("ctx")
    rows, width = block_input.shape[1:]
    half_width = width // 2
    block = rows // 2
    block_count = 2 * ctx_size

    def by_side(own, other, axis):
        return jnp.where(
            side == 0,
            jnp.concatenate([own, other], axis=axis),
            jnp.concatenate([other, own], axis=axis),
        )

    x_own = block_input[0]
    g_own = out_grad[0]
    x_other = swap_fsdp(x_own)

    block_range = jnp.arange(block_count, dtype=jnp.int32)
    slot_of = jnp.sum(
        jnp.where(block_ids[None, :] == block_range[:, None], block_range[None, :], 0), axis=1
    ).astype(jnp.int32)
    owned = lax.dynamic_slice(block_ids, (2 * me,), (2,))
    positions = (
        owned[:, None] * block + jnp.arange(block, dtype=jnp.int32)[None, :]
    ).reshape(rows)
    part = KEY_HEADS * HEAD_SIZE
    angles = positions.astype(F32)[:, None] * jnp.asarray(frequency_row(part))[None, :]
    cosine = jnp.cos(angles)
    sine = jnp.sin(angles) * jnp.asarray(sign_row(part))[None, :]
    order = jnp.bitwise_xor(me, jnp.asarray(relative_order(ctx_size), jnp.int32))
    order_ids = jnp.take(block_ids.reshape(ctx_size, 2), order, axis=0).reshape(-1)

    x_f = x_own.astype(F32)
    normed_one, inverse_one = norm_stats(x_f)
    normed_both = jnp.concatenate([normed_one, norm_stats(x_other.astype(F32))[0]], axis=0)
    own_columns = lax.dynamic_slice_in_dim(normed_both, side * half_width, half_width, axis=1)
    left = (own_columns * gain_attn.astype(F32)).astype(BF16)

    def partial_product(weight):
        product = dot_nn(left, weight)
        return product[:rows], swap_fsdp(product[rows:].astype(BF16))

    k_own, k_got = partial_product(key_weight)
    v_own, v_got = partial_product(value_weight)
    q_own, q_got = partial_product(w_query)
    keys = rotary_sum(k_own, k_got, cosine, sine)
    values = (v_own + v_got.astype(F32)).astype(BF16)
    key_all = lax.all_gather(keys, "ctx", axis=0, tiled=True)
    value_all = lax.all_gather(values, "ctx", axis=0, tiled=True)
    query = rotary_sum(q_own, q_got, cosine, sine)

    g_other = swap_fsdp(after(g_own, q_got))
    gains = jnp.stack([gain_attn, gain_ffn])
    gains = by_side(gains, swap_fsdp(gains), 1).astype(F32)
    gain_one, gain_two = gains[0], gains[1]
    core = me % 2
    out_half = w_out.shape[0] // 2
    mine = lax.dynamic_slice_in_dim(w_out, core * out_half, out_half, axis=0)
    mine = swap_fsdp(after(mine, q_got))
    theirs = swap_bit(mine, 0)
    out_other = jnp.where(
        core == 0,
        jnp.concatenate([mine, theirs], axis=0),
        jnp.concatenate([theirs, mine], axis=0),
    )
    full_out = by_side(w_out, out_other, 1)
    n1_both = (normed_both * gain_one).astype(BF16)
    g_both = jnp.concatenate([g_own, g_other], axis=0)
    g_chunks = chunk_rows(g_both, order, ctx_size)
    n1_chunks = chunk_rows(n1_both, 2 * order + side, 2 * ctx_size)

    mixed, lse = attention_forward(query, key_all, value_all, slot_of, owned, block)
    mixed_other = swap_fsdp(mixed)
    resid_mid = x_f + dot_nn(mixed, full_out)
    normed_two, inverse_two = norm_stats(resid_mid)
    n2 = (normed_two * gain_two).astype(BF16)
    n2_both = jnp.concatenate([n2, swap_fsdp(n2)], axis=0)

    gate = dot_nn(n2_both, w_gate)
    up = dot_nn(n2_both, w_up)
    sig = jax.nn.sigmoid(gate)
    silu = gate * sig
    hidden = (silu * up).astype(BF16)
    hidden_grad = dot_nt(g_both, w_down)
    gate_grad = (hidden_grad * up * sig * (1.0 + gate * (1.0 - sig))).astype(BF16)
    up_grad = (hidden_grad * silu).astype(BF16)
    n2_grad = dot_nt(gate_grad, w_gate) + dot_nt(up_grad, w_up)
    n2_grad = n2_grad[:rows] + swap_fsdp(n2_grad[rows:].astype(BF16)).astype(F32)
    ffn = dot_nn(hidden, w_down)
    ffn = ffn[:rows] + swap_fsdp(ffn[rows:].astype(BF16)).astype(F32)
    block_output = (resid_mid + ffn).astype(BF16)
    n2_chunks = chunk_rows(n2_both, order, ctx_size)
    grad_gate = weight_grad(n2_chunks, gate_grad, ctx_size)
    grad_up = weight_grad(n2_chunks, up_grad, ctx_size)
    grad_down = weight_grad(g_chunks, hidden, ctx_size).T

    gain_two_grad = jnp.sum(n2_grad * normed_two, axis=0)
    mid_grad = g_own.astype(F32) + norm_back(n2_grad, normed_two, inverse_two, gain_two)
    mid_grad_b = mid_grad.astype(BF16)
    mid_both = jnp.concatenate([mid_grad_b, swap_fsdp(mid_grad_b)], axis=0)
    mid_chunks = chunk_rows(mid_both, 2 * order + side, 2 * ctx_size)
    mixed_both = jnp.concatenate([mixed, mixed_other], axis=0)
    mixed_grad = dot_nt(mid_grad_b, full_out).astype(BF16)
    dq, dk_keep, dk_send, dv_keep, dv_send = attention_backward(
        query,
        mixed_grad,
        mixed,
        lse,
        jnp.where(jnp.arange(LANES) < HEAD_SIZE, cosine[:, :LANES], 0.0),
        jnp.where(jnp.arange(LANES) < HEAD_SIZE, sine[:, :LANES], 0.0),
        key_all,
        value_all,
        slot_of,
        owned,
        order_ids,
        block,
    )
    dk = inverse_rotary(halve(dk_keep, dk_send), cosine, sine)
    dv = halve(dv_keep, dv_send).astype(BF16)
    dq_both = jnp.concatenate([dq, swap_fsdp(dq)], axis=0)
    dk_both = jnp.concatenate([dk, swap_fsdp(dk)], axis=0)
    dv_both = jnp.concatenate([dv, swap_fsdp(dv)], axis=0)

    n1_grad = dot_nt(dq_both, w_query) + dot_nt(dk_both, key_weight) + dot_nt(dv_both, value_weight)
    n1_got = swap_fsdp(n1_grad[rows:].astype(BF16)).astype(F32)
    n1_grad = by_side(n1_grad[:rows], n1_got, 1)
    gain_one_grad = jnp.sum(n1_grad * normed_one, axis=0)
    input_grad = mid_grad + norm_back(n1_grad, normed_one, inverse_one, gain_one)

    grad_out = weight_grad(mid_chunks, mixed_both, ctx_size).T
    grad_query = weight_grad(n1_chunks, dq_both, ctx_size)
    grad_key = weight_grad(n1_chunks, dk_both, ctx_size)
    grad_value = weight_grad(n1_chunks, dv_both, ctx_size)

    gain_parts = jnp.stack([gain_one_grad, gain_two_grad], axis=0)
    gain_parts = gain_parts.reshape(2, ctx_size, 2, -1).transpose(2, 1, 0, 3)
    kept = lax.dynamic_index_in_dim(gain_parts, side, 0, keepdims=False)
    sent = lax.dynamic_index_in_dim(gain_parts, 1 - side, 0, keepdims=False)
    gain_sum = jnp.take(kept + swap_fsdp(sent), order, axis=0)
    gain_sum = halve(gain_sum[: ctx_size // 2], gain_sum[ctx_size // 2 :])

    return (
        block_output[None],
        input_grad[None],
        gain_sum[0],
        gain_sum[1],
        grad_query,
        grad_key,
        grad_value,
        grad_out,
        grad_gate,
        grad_up,
        grad_down,
    )


def solution(mesh):
    return jax.shard_map(
        local,
        mesh=mesh,
        in_specs=(
            P("fsdp", "ctx", None),
            P("fsdp", "ctx", None),
            P(),
            P("fsdp"),
            P("fsdp"),
            P("fsdp", None),
            P("fsdp", None),
            P("fsdp", None),
            P(None, "fsdp"),
            P(None, "fsdp"),
            P(None, "fsdp"),
            P("fsdp", None),
        ),
        out_specs=(
            P("fsdp", "ctx", None),
            P("fsdp", "ctx", None),
            P(("ctx", "fsdp")),
            P(("ctx", "fsdp")),
            P(("ctx", "fsdp"), None),
            P(("ctx", "fsdp"), None),
            P(("ctx", "fsdp"), None),
            P(None, ("ctx", "fsdp")),
            P("ctx", "fsdp"),
            P("ctx", "fsdp"),
            P("fsdp", "ctx"),
        ),
        check_vma=False,
    )
```

```python
import functools
import math

import jax
import jax.numpy as jnp
import numpy as np
from jax import lax
from jax.experimental import pallas as pl
from jax.experimental.pallas import tpu as pltpu
from jax.sharding import PartitionSpec as P


QUERY_HEADS = 16
KEY_HEADS = 8
HEAD_SIZE = 96
GROUP = QUERY_HEADS // KEY_HEADS
LANES = 128
HEADS_STEP = 4
TILE_BLOCKS = 4

EPS = 1e-05
THETA = 100000.0
NEGATIVE_FLOOR = -1e30
LOG2E = math.log2(math.e)
SCALE = HEAD_SIZE ** (-0.5)
VMEM_BYTES = 66_000_000

F32 = jnp.float32
BF16 = jnp.bfloat16


def dot_nn(left, right):
    return lax.dot_general(left, right, (((1,), (0,)), ((), ())), preferred_element_type=F32)


def dot_nt(left, right):
    return lax.dot_general(left, right, (((1,), (1,)), ((), ())), preferred_element_type=F32)


def frequency_row(width):
    lane = np.arange(width)
    half = HEAD_SIZE // 2
    freq = np.exp(-math.log(THETA) * 2.0 * (lane % HEAD_SIZE % half) / HEAD_SIZE)
    return freq.astype(np.float32)


def sign_row(width):
    lane = np.arange(width)
    return np.where(lane % HEAD_SIZE < HEAD_SIZE // 2, -1.0, 1.0).astype(np.float32)


def swap_halves(value):
    width = value.shape[1]
    half = HEAD_SIZE // 2
    lane = lax.broadcasted_iota(jnp.int32, value.shape, 1)
    lower = lax.rem(lane, HEAD_SIZE) < half
    return jnp.where(lower, pltpu.roll(value, width - half, 1), pltpu.roll(value, half, 1))


def rotary_kernel(sign, first, second, cosine, sine, out):
    total = first[...].astype(F32) + second[...].astype(F32)
    out[...] = (total * cosine[...] + sign * swap_halves(total) * sine[...]).astype(BF16)


def rotary_sum(first, second, cosine, sine):
    rows, width = first.shape
    part = cosine.shape[1]
    spec = pl.BlockSpec((rows, part), lambda i: (0, i))
    table = pl.BlockSpec((rows, part), lambda i: (0, 0))
    return pl.pallas_call(
        functools.partial(rotary_kernel, 1.0),
        out_shape=jax.ShapeDtypeStruct((rows, width), BF16),
        grid=(width // part,),
        in_specs=[spec, spec, table, table],
        out_specs=spec,
        name="rotary_sum",
        cost_estimate=pl.CostEstimate(
            flops=6 * rows * width, bytes_accessed=8 * rows * width, transcendentals=0
        ),
    )(first, second, cosine, sine)


def rotary_kv_kernel(k_own, k_got, v_own, v_got, cosine, sine, out):
    width = k_own.shape[1]
    keys = k_own[...] + k_got[...].astype(F32)
    out[:, :width] = (keys * cosine[...] + swap_halves(keys) * sine[...]).astype(BF16)
    out[:, width:] = (v_own[...] + v_got[...].astype(F32)).astype(BF16)


def rotary_kv(k_own, k_got, v_own, v_got, cosine, sine):
    rows, width = k_own.shape
    return pl.pallas_call(
        rotary_kv_kernel,
        out_shape=jax.ShapeDtypeStruct((rows, 2 * width), BF16),
        name="rotary_kv",
        cost_estimate=pl.CostEstimate(
            flops=8 * rows * width, bytes_accessed=20 * rows * width, transcendentals=0
        ),
    )(k_own, k_got, v_own, v_got, cosine, sine)


def rotary_back_kernel(keys, values, cosine, sine, out):
    width = keys.shape[1]
    total = keys[...]
    out[:, :width] = (total * cosine[...] - swap_halves(total) * sine[...]).astype(BF16)
    out[:, width:] = values[...].astype(BF16)


def rotary_back(keys, values, cosine, sine):
    rows, width = keys.shape
    return pl.pallas_call(
        rotary_back_kernel,
        out_shape=jax.ShapeDtypeStruct((rows, 2 * width), BF16),
        name="rotary_back",
        cost_estimate=pl.CostEstimate(
            flops=6 * rows * width, bytes_accessed=20 * rows * width, transcendentals=0
        ),
    )(keys, values, cosine, sine)


def head_slice(rows, head):
    piece = rows[:, head * HEAD_SIZE : (head + 1) * HEAD_SIZE]
    pad = jnp.zeros((rows.shape[0], LANES - HEAD_SIZE), rows.dtype)
    return jnp.concatenate([piece, pad], axis=1)


def group_rows(rows, key_head):
    return jnp.concatenate(
        [head_slice(rows, key_head * GROUP + r) for r in range(GROUP)], axis=0
    )


def tile_rows(ref, slot_of, tile, block):
    pieces = []
    for i in range(TILE_BLOCKS):
        start = pl.multiple_of(slot_of[tile * TILE_BLOCKS + i] * block, block)
        pieces.append(ref[pl.ds(start, block), :])
    return jnp.concatenate(pieces, axis=0)


def allowed(tile, tile_len, query_block, block, rows):
    key_pos = tile * tile_len + lax.broadcasted_iota(jnp.int32, (tile_len, rows), 0)
    row = lax.broadcasted_iota(jnp.int32, (tile_len, rows), 1)
    query_pos = query_block * block + lax.rem(row, block)
    return key_pos <= query_pos


def fold(value, how):
    return how(value.reshape(value.shape[0] // 8, 8, value.shape[1]), axis=0)


def merge_heads(pieces):
    return jnp.concatenate([piece[:, :HEAD_SIZE] for piece in pieces], axis=1)


def forward_kernel(
    batch, block, slot_of, owned, q_ref, k_ref, v_ref, o_ref, lse_ref, kn, vt, scores, acc, top, total
):
    tile_len = TILE_BLOCKS * block
    rows = GROUP * block
    counts = [(owned[m] + TILE_BLOCKS) // TILE_BLOCKS for m in range(2)]
    most = jnp.maximum(counts[0], counts[1])
    merged = [[None] * (HEADS_STEP * GROUP) for _ in range(2)]
    for first in range(0, HEADS_STEP, batch):

        def pack(tile, carry, first=first):
            k_rows = tile_rows(k_ref, slot_of, tile, block)
            v_rows = tile_rows(v_ref, slot_of, tile, block)
            start = pl.multiple_of(tile * tile_len, tile_len)
            for h in range(batch):
                kn[h, pl.ds(start, tile_len), :] = head_slice(k_rows, first + h)
                vt[h, :, pl.ds(start, tile_len)] = head_slice(v_rows, first + h).T
            return carry

        lax.fori_loop(0, most, pack, 0)
        for m in range(2):
            member = slice(m * block, (m + 1) * block)
            q_rows = q_ref[member, :]
            queries = [group_rows(q_rows, first + h) for h in range(batch)]
            for h in range(batch):
                top[h] = jnp.full((8, rows), NEGATIVE_FLOOR, F32)
                total[h] = jnp.zeros((8, rows), F32)
                acc[h] = jnp.zeros((LANES, rows), F32)

            def score_pass(tile, carry, queries=queries, m=m):
                start = pl.multiple_of(tile * tile_len, tile_len)
                mask = allowed(tile, tile_len, owned[m], block, rows)
                for h in range(batch):
                    value = dot_nt(kn[h, pl.ds(start, tile_len), :], queries[h])
                    value = jnp.where(mask, value * (SCALE * LOG2E), NEGATIVE_FLOOR)
                    scores[h, pl.ds(start, tile_len), :] = value
                    top[h] = jnp.maximum(top[h], fold(value, jnp.max))
                return carry

            lax.fori_loop(0, counts[m], score_pass, 0)
            peaks = [jnp.max(top[h], axis=0, keepdims=True) for h in range(batch)]

            def mix_pass(tile, carry, peaks=peaks):
                start = pl.multiple_of(tile * tile_len, tile_len)
                for h in range(batch):
                    weight = jnp.exp2(scores[h, pl.ds(start, tile_len), :] - peaks[h])
                    total[h] += fold(weight, jnp.sum)
                    acc[h] += dot_nn(vt[h, :, pl.ds(start, tile_len)], weight.astype(BF16))
                return carry

            lax.fori_loop(0, counts[m], mix_pass, 0)
            for h in range(batch):
                denom = jnp.sum(total[h], axis=0, keepdims=True)
                mixed = (acc[h] / denom).T.astype(BF16)
                for r in range(GROUP):
                    merged[m][(first + h) * GROUP + r] = mixed[r * block : (r + 1) * block, :]
                lse_ref[first + h, m : m + 1, :] = peaks[h] + jnp.log2(denom)
    for m in range(2):
        o_ref[m * block : (m + 1) * block, :] = merge_heads(merged[m])


def kv_specs(length, heads_width):
    mode = {} if length <= 4096 else {"pipeline_mode": pl.Buffered(1)}
    return [
        pl.BlockSpec((length, heads_width), lambda i, *_, base=base: (0, base + i), **mode)
        for base in (0, KEY_HEADS // HEADS_STEP)
    ]


def attention_forward(query, all_kv, slot_of, owned, block):
    rows = query.shape[0]
    length = all_kv.shape[0]
    batch = HEADS_STEP if length <= 4096 else 1
    steps = KEY_HEADS // HEADS_STEP
    key_width = HEADS_STEP * HEAD_SIZE
    query_width = key_width * GROUP
    pairs = GROUP * block
    query_spec = pl.BlockSpec((rows, query_width), lambda i, *_: (0, i))
    return pl.pallas_call(
        functools.partial(forward_kernel, batch, block),
        out_shape=(
            jax.ShapeDtypeStruct(query.shape, BF16),
            jax.ShapeDtypeStruct((KEY_HEADS, 2, pairs), F32),
        ),
        grid_spec=pltpu.PrefetchScalarGridSpec(
            num_scalar_prefetch=2,
            grid=(steps,),
            in_specs=[query_spec] + kv_specs(length, key_width),
            out_specs=[
                query_spec,
                pl.BlockSpec((HEADS_STEP, 2, pairs), lambda i, *_: (i, 0, 0)),
            ],
            scratch_shapes=[
                pltpu.VMEM((batch, length, LANES), BF16),
                pltpu.VMEM((batch, LANES, length), BF16),
                pltpu.VMEM((batch, length, pairs), F32),
                pltpu.VMEM((batch, LANES, pairs), F32),
                pltpu.VMEM((batch, 8, pairs), F32),
                pltpu.VMEM((batch, 8, pairs), F32),
            ],
        ),
        compiler_params=pltpu.CompilerParams(vmem_limit_bytes=VMEM_BYTES),
        name="attention_forward",
        cost_estimate=pl.CostEstimate(
            flops=4 * rows * length * query.shape[1] // 2,
            bytes_accessed=2 * all_kv.size,
            transcendentals=rows * length * QUERY_HEADS // 2,
        ),
    )(slot_of, owned, query, all_kv, all_kv)


def backward_kernel(
    batch,
    block,
    slot_of,
    owned,
    block_ids,
    q_ref,
    do_ref,
    o_ref,
    lse_ref,
    cos_ref,
    sin_ref,
    k_ref,
    v_ref,
    dq_ref,
    dk_out,
    dv_out,
    kn,
    vn,
    kt,
    dk,
    dv,
    acc,
):
    tile_len = TILE_BLOCKS * block
    rows = GROUP * block
    counts = [(owned[m] + TILE_BLOCKS) // TILE_BLOCKS for m in range(2)]
    most = jnp.maximum(counts[0], counts[1])
    merged = [[None] * (HEADS_STEP * GROUP) for _ in range(2)]
    for first in range(0, HEADS_STEP, batch):

        def pack(tile, carry, first=first):
            k_rows = tile_rows(k_ref, slot_of, tile, block)
            v_rows = tile_rows(v_ref, slot_of, tile, block)
            start = pl.multiple_of(tile * tile_len, tile_len)
            for h in range(batch):
                piece = head_slice(k_rows, first + h)
                kn[h, pl.ds(start, tile_len), :] = piece
                kt[h, :, pl.ds(start, tile_len)] = piece.T
                vn[h, pl.ds(start, tile_len), :] = head_slice(v_rows, first + h)
            return carry

        lax.fori_loop(0, most, pack, 0)
        dk[...] = jnp.zeros_like(dk)
        dv[...] = jnp.zeros_like(dv)
        for m in range(2):
            member = slice(m * block, (m + 1) * block)
            q_rows, g_rows, o_rows = q_ref[member, :], do_ref[member, :], o_ref[member, :]
            queries = [group_rows(q_rows, first + h) for h in range(batch)]
            grads = [group_rows(g_rows, first + h) for h in range(batch)]
            deltas = []
            for h in range(batch):
                product = grads[h].astype(F32) * group_rows(o_rows, first + h).astype(F32)
                deltas.append(jnp.sum(product.T, axis=0, keepdims=True))
                acc[h] = jnp.zeros((LANES, rows), F32)
            lses = [lse_ref[first + h, m : m + 1, :] for h in range(batch)]

            def grad_pass(tile, carry, queries=queries, grads=grads, deltas=deltas, lses=lses, m=m):
                start = pl.multiple_of(tile * tile_len, tile_len)
                mask = allowed(tile, tile_len, owned[m], block, rows)
                for h in range(batch):
                    value = dot_nt(kn[h, pl.ds(start, tile_len), :], queries[h])
                    value = jnp.where(mask, value * (SCALE * LOG2E) - lses[h], NEGATIVE_FLOOR)
                    prob = jnp.exp2(value)
                    weight = prob.astype(BF16)
                    grad_prob = dot_nt(vn[h, pl.ds(start, tile_len), :], grads[h])
                    grad_score = (prob * (grad_prob - deltas[h]) * SCALE).astype(BF16)
                    dk[h, pl.ds(start, tile_len), :] += dot_nn(grad_score, queries[h])
                    dv[h, pl.ds(start, tile_len), :] += dot_nn(weight, grads[h])
                    acc[h] += dot_nn(kt[h, :, pl.ds(start, tile_len)], grad_score)
                return carry

            lax.fori_loop(0, counts[m], grad_pass, 0)
            cosine = jnp.concatenate([cos_ref[member, :]] * GROUP, axis=0)
            sine = jnp.concatenate([sin_ref[member, :]] * GROUP, axis=0)
            for h in range(batch):
                grad = acc[h].T
                grad = (grad * cosine - swap_halves(grad) * sine).astype(BF16)
                for r in range(GROUP):
                    merged[m][(first + h) * GROUP + r] = grad[r * block : (r + 1) * block, :]

        def unpack(chunk, carry, first=first):
            for source, target in ((dk, dk_out), (dv, dv_out)):
                pieces = []
                for h in range(batch):
                    picked = []
                    for i in range(2):
                        start = pl.multiple_of(block_ids[2 * chunk + i] * block, block)
                        picked.append(source[h, pl.ds(start, block), :].astype(BF16))
                    pieces.append(jnp.concatenate(picked, axis=0))
                lanes = slice(first * HEAD_SIZE, (first + batch) * HEAD_SIZE)
                target[chunk, :, lanes] = merge_heads(pieces)
            return carry

        lax.fori_loop(0, dk_out.shape[0], unpack, 0)
    for m in range(2):
        dq_ref[m * block : (m + 1) * block, :] = merge_heads(merged[m])


def attention_backward(
    query, grad, mixed, lse, cosine, sine, all_kv, slot_of, owned, block_ids, block
):
    rows = query.shape[0]
    length = all_kv.shape[0]
    chunks = length // rows
    batch = HEADS_STEP if length <= 4096 else 1
    steps = KEY_HEADS // HEADS_STEP
    key_width = HEADS_STEP * HEAD_SIZE
    query_width = key_width * GROUP
    pairs = GROUP * block
    query_spec = pl.BlockSpec((rows, query_width), lambda i, *_: (0, i))
    mode = {} if length <= 4096 else {"pipeline_mode": pl.Buffered(1)}
    out_spec = pl.BlockSpec((chunks, rows, key_width), lambda i, *_: (0, 0, i), **mode)
    table = pl.BlockSpec((rows, LANES), lambda i, *_: (0, 0))
    grad_shape = jax.ShapeDtypeStruct((chunks, rows, all_kv.shape[1] // 2), BF16)
    return pl.pallas_call(
        functools.partial(backward_kernel, batch, block),
        out_shape=(jax.ShapeDtypeStruct(query.shape, BF16),) + (grad_shape,) * 2,
        grid_spec=pltpu.PrefetchScalarGridSpec(
            num_scalar_prefetch=3,
            grid=(steps,),
            in_specs=[
                query_spec,
                query_spec,
                query_spec,
                pl.BlockSpec((HEADS_STEP, 2, pairs), lambda i, *_: (i, 0, 0)),
                table,
                table,
            ]
            + kv_specs(length, key_width),
            out_specs=[query_spec] + [out_spec] * 2,
            scratch_shapes=[
                pltpu.VMEM((batch, length, LANES), BF16),
                pltpu.VMEM((batch, length, LANES), BF16),
                pltpu.VMEM((batch, LANES, length), BF16),
                pltpu.VMEM((batch, length, LANES), F32),
                pltpu.VMEM((batch, length, LANES), F32),
                pltpu.VMEM((batch, LANES, pairs), F32),
            ],
        ),
        compiler_params=pltpu.CompilerParams(vmem_limit_bytes=VMEM_BYTES),
        name="attention_backward",
        cost_estimate=pl.CostEstimate(
            flops=10 * rows * length * query.shape[1] // 2,
            bytes_accessed=4 * all_kv.size,
            transcendentals=rows * length * QUERY_HEADS // 2,
        ),
    )(slot_of, owned, block_ids, query, grad, mixed, lse, cosine, sine, all_kv, all_kv)


def place():
    me = lax.axis_index("ctx")
    return me // 4, me // 2 % 2, me % 2


def device_at(line, mid, core):
    return {"ctx": (line * 2 + mid) * 2 + core}


def greet(line, mid, core, count):
    barrier = pltpu.get_barrier_semaphore()

    def call(*where):
        pl.semaphore_signal(
            barrier, inc=1, device_id=device_at(*where), device_id_type=pl.DeviceIdType.MESH
        )

    call(line, 1 - mid, core)
    call(line, mid, 1 - core)

    @pl.when(line > 0)
    def _():
        call(line - 1, mid, core)

    @pl.when(line + 1 < count)
    def _():
        call(line + 1, mid, core)

    ends = jnp.where(line > 0, 1, 0) + jnp.where(line + 1 < count, 1, 0)
    pl.semaphore_wait(barrier, 2 + ends)


def remote(source, target, send, recv, where):
    return pltpu.make_async_remote_copy(
        src_ref=source,
        dst_ref=target,
        send_sem=send,
        recv_sem=recv,
        device_id=device_at(*where),
        device_id_type=pl.DeviceIdType.MESH,
    )


def gather_kernel(
    count, own, out, here, right_send, left_send, mid_send, core_send, line_recv, mid_recv, core_recv
):
    line, mid, core = place()
    rows = own.shape[0]
    greet(line, mid, core, count)

    def slot(j, m, k):
        start = pl.multiple_of(((j * 2 + m) * 2 + k) * rows, rows)
        return out.at[pl.ds(start, rows)]

    def to_right(j, source):
        return remote(source, slot(j, mid, core), right_send.at[j], line_recv.at[j], (line + 1, mid, core))

    def to_left(j, source):
        return remote(source, slot(j, mid, core), left_send.at[j], line_recv.at[j], (line - 1, mid, core))

    def to_mid(j, source):
        return remote(source, slot(j, mid, core), mid_send.at[j], mid_recv.at[j], (line, 1 - mid, core))

    def to_core(j, m, source):
        return remote(
            source, slot(j, m, core), core_send.at[2 * j + m], core_recv.at[2 * j + m], (line, mid, 1 - core)
        )

    keep = pltpu.make_async_copy(own, slot(line, mid, core), here)
    keep.start()
    to_mid(line, own).start()

    @pl.when(line + 1 < count)
    def _():
        to_right(line, own).start()

    @pl.when(line > 0)
    def _():
        to_left(line, own).start()

    to_core(line, mid, own).start()


    def arrived_line(j, step_right):
        block = slot(j, mid, core)
        to_right(j, block).wait_recv()
        if step_right:

            @pl.when(line + 1 < count)
            def _():
                to_right(j, block).start()

        else:

            @pl.when(line > 0)
            def _():
                to_left(j, block).start()

        to_mid(j, block).start()
        to_core(j, mid, block).start()

    def arrived_mid(j):
        block = slot(j, 1 - mid, core)
        remote(block, block, mid_send.at[j], mid_recv.at[j], (line, 1 - mid, core)).wait_recv()
        to_core(j, 1 - mid, block).start()

    for step in range(1, count + 1):
        if step < count:

            @pl.when(line - step >= 0)
            def _(step=step):
                arrived_line(line - step, True)

            @pl.when(line + step < count)
            def _(step=step):
                arrived_line(line + step, False)

        if step == 1:
            arrived_mid(line)
        else:

            @pl.when(line - (step - 1) >= 0)
            def _(step=step):
                arrived_mid(line - (step - 1))

            @pl.when(line + (step - 1) < count)
            def _(step=step):
                arrived_mid(line + (step - 1))

    for j in range(count):
        for m in range(2):
            block = slot(j, m, 1 - core)
            remote(
                block, block, core_send.at[2 * j + m], core_recv.at[2 * j + m], (line, mid, 1 - core)
            ).wait_recv()
    keep.wait()
    for j in range(count):
        block = slot(j, mid, core)
        to_mid(j, block).wait_send()
        for m in range(2):
            to_core(j, m, slot(j, m, core)).wait_send()

        @pl.when(jnp.logical_and(j <= line, line + 1 < count))
        def _(j=j, block=block):
            to_right(j, block).wait_send()

        @pl.when(jnp.logical_and(j >= line, line > 0))
        def _(j=j, block=block):
            to_left(j, block).wait_send()


def gather_ctx(own, collective_id):
    size = lax.axis_size("ctx")
    rows, width = own.shape
    count = size // 4
    dma = pltpu.SemaphoreType.DMA
    return pl.pallas_call(
        functools.partial(gather_kernel, count),
        out_shape=jax.ShapeDtypeStruct((size * rows, width), own.dtype),
        in_specs=[pl.BlockSpec(memory_space=pltpu.VMEM)],
        out_specs=pl.BlockSpec(memory_space=pl.ANY),
        scratch_shapes=[dma(())] + [dma((count,))] * 3 + [dma((2 * count,))] + [dma((count,))] * 2 + [dma((2 * count,))],
        compiler_params=pltpu.CompilerParams(collective_id=collective_id, has_side_effects=True),
        cost_estimate=pl.CostEstimate(
            flops=0, bytes_accessed=100 * size * rows * width, transcendentals=0
        ),
    )(own)


def reduce_kernel(count, parts, *refs):
    sources, outs = refs[:parts], refs[parts : 2 * parts]
    scratch = refs[2 * parts :]
    work, from_core, from_mid, from_right, from_left = (scratch[i * parts : (i + 1) * parts] for i in range(5))
    (load, core_send, core_recv, mid_send, mid_recv, left_send, right_send, right_recv, left_recv) = scratch[5 * parts :]
    line, mid, core = place()
    greet(line, mid, core, count)

    def nearest_last(visit):
        for step in range(count - 1, 0, -1):
            for j in (line - step, line + step):

                @pl.when(jnp.logical_and(j >= 0, j < count))
                def _(j=j):
                    visit(j)

        visit(line)

    def core_copy(s, j, m):
        index = 2 * j + m
        return remote(
            sources[s].at[2 * index + (1 - core)],
            from_core[s].at[index],
            core_send.at[s, index],
            core_recv.at[s, index],
            (line, mid, 1 - core),
        )

    def load_copy(s, j, m):
        index = 2 * j + m
        return pltpu.make_async_copy(sources[s].at[2 * index + core], work[s].at[index], load.at[s, index])

    def mid_copy(s, j):
        return remote(
            work[s].at[2 * j + (1 - mid)],
            from_mid[s].at[j],
            mid_send.at[s, j],
            mid_recv.at[s, j],
            (line, 1 - mid, core),
        )

    def left_copy(s, j):
        return remote(
            work[s].at[2 * j + mid],
            from_right[s].at[j],
            left_send.at[s, j],
            right_recv.at[s, j],
            (line - 1, mid, core),
        )

    def right_copy(s, j):
        return remote(
            work[s].at[2 * j + mid],
            from_left[s].at[j],
            right_send.at[s, j],
            left_recv.at[s, j],
            (line + 1, mid, core),
        )

    def add(s, index, other):
        work[s][index] = (work[s][index].astype(F32) + other.astype(F32)).astype(work[s].dtype)

    for m in (1 - mid, mid):

        def begin(j, m=m):
            for s in range(parts):
                core_copy(s, j, m).start()
                load_copy(s, j, m).start()

        nearest_last(begin)

    def core_sum(s, j, m):
        core_copy(s, j, m).wait_recv()
        load_copy(s, j, m).wait()
        add(s, 2 * j + m, from_core[s][2 * j + m])

    def to_mid(j):
        for s in range(parts):
            core_sum(s, j, 1 - mid)
            mid_copy(s, j).start()

    nearest_last(to_mid)

    def keep_mine(j):
        for s in range(parts):
            core_sum(s, j, mid)

    nearest_last(keep_mine)

    def along(j):
        for s in range(parts):
            mid_copy(s, j).wait_recv()
            add(s, 2 * j + mid, from_mid[s][j])

            @pl.when(j < line)
            def _(s=s):
                @pl.when(line + 1 < count)
                def _():
                    left_copy(s, j).wait_recv()
                    add(s, 2 * j + mid, from_right[s][j])

                left_copy(s, j).start()

            @pl.when(j > line)
            def _(s=s):
                @pl.when(line > 0)
                def _():
                    right_copy(s, j).wait_recv()
                    add(s, 2 * j + mid, from_left[s][j])

                right_copy(s, j).start()

    nearest_last(along)
    for s in range(parts):
        outs[s][...] = work[s][2 * line + mid].astype(F32)

        @pl.when(line + 1 < count)
        def _(s=s):
            left_copy(s, line).wait_recv()
            outs[s][...] += from_right[s][line].astype(F32)

        @pl.when(line > 0)
        def _(s=s):
            right_copy(s, line).wait_recv()
            outs[s][...] += from_left[s][line].astype(F32)

    for s in range(parts):
        for j in range(count):
            mid_copy(s, j).wait_send()
            for m in range(2):
                core_copy(s, j, m).wait_send()

            @pl.when(j < line)
            def _(s=s, j=j):
                left_copy(s, j).wait_send()

            @pl.when(j > line)
            def _(s=s, j=j):
                right_copy(s, j).wait_send()


def reduce_ctx(sources, collective_id):
    size = lax.axis_size("ctx")
    count = size // 4
    parts = len(sources)
    dma = pltpu.SemaphoreType.DMA

    def room(chunks):
        return [pltpu.VMEM((chunks,) + source.shape[1:], source.dtype) for source in sources]

    return pl.pallas_call(
        functools.partial(reduce_kernel, count, parts),
        out_shape=[jax.ShapeDtypeStruct(source.shape[1:], F32) for source in sources],
        in_specs=[pl.BlockSpec(memory_space=pl.ANY)] * parts,
        out_specs=[pl.BlockSpec(memory_space=pltpu.VMEM)] * parts,
        scratch_shapes=room(2 * count) + room(2 * count) + room(count) * 1 + room(count) + room(count)
        + [dma((parts, 2 * count))] * 3
        + [dma((parts, count))] * 6,
        compiler_params=pltpu.CompilerParams(
            collective_id=collective_id, has_side_effects=True, vmem_limit_bytes=VMEM_BYTES
        ),
        cost_estimate=pl.CostEstimate(
            flops=0, bytes_accessed=100 * sum(source.size for source in sources), transcendentals=0
        ),
    )(*sources)


def swap_fsdp(value):
    size = lax.axis_size("fsdp")
    return lax.ppermute(value, "fsdp", [(i, size - 1 - i) for i in range(size)])


def swap_bit(value, bit):
    size = lax.axis_size("ctx")
    return lax.ppermute(value, "ctx", [(i, i ^ (1 << bit)) for i in range(size)])


def bit_order(size, swapped=False):
    bits = list(range(size.bit_length() - 1))
    if swapped and len(bits) > 2:
        bits[1], bits[2] = bits[2], bits[1]
    return bits


def my_bit(bit):
    return lax.axis_index("ctx") >> bit & 1


def pick(value, axis, index):
    return lax.dynamic_index_in_dim(value, index, axis, keepdims=False)


def halve(keep, send, bits):
    left = sorted(bits[1:], reverse=True)
    for stage, bit in enumerate(bits):
        got = swap_bit(send, bit)
        total = keep.astype(F32) + got.astype(F32)
        if not left:
            return total
        axis = left.index(bits[stage + 1])
        mine = my_bit(bits[stage + 1])
        send = (
            pick(keep, axis, 1 - mine).astype(F32) + pick(got, axis, 1 - mine).astype(F32)
        ).astype(BF16)
        keep = (pick(keep, axis, mine).astype(F32) + pick(got, axis, mine).astype(F32)).astype(BF16)
        left = left[:axis] + left[axis + 1 :]


def weight_grad(left, right, bits):
    size = lax.axis_size("ctx")
    width, tokens = left.shape
    rows = width // size
    chunks = left.reshape(size // 2, 2, rows, tokens)

    def piece(core):
        flat = pick(chunks, 1, core).reshape(width // 2, tokens)
        product = dot_nn(flat, right).astype(BF16)
        return product.reshape((2,) * (len(bits) - 1) + (rows, right.shape[1]))

    core = my_bit(0)
    send = piece(1 - core)
    keep = piece(core)
    return halve(keep, send, bits)


def side_parts(left, right):
    size = lax.axis_size("ctx")
    width, tokens = left.shape
    rows = width // (2 * size)
    flat = pick(left.reshape(size, 2, rows, tokens), 1, lax.axis_index("fsdp"))
    product = dot_nn(flat.reshape(size * rows, tokens), right).astype(BF16)
    return product.reshape(size, rows, right.shape[1])


def after(value, anchor):
    return lax.optimization_barrier((value, anchor))[0]


def norm_stats(value):
    inverse = lax.rsqrt(jnp.mean(value * value, axis=-1, keepdims=True) + EPS)
    return (value * inverse, inverse)


def norm_back(grad, normed, inverse, gain):
    scaled = grad * gain
    return inverse * (scaled - normed * jnp.mean(scaled * normed, axis=-1, keepdims=True))


def local(
    block_input,
    out_grad,
    block_ids,
    gain_attn,
    gain_ffn,
    w_query,
    key_weight,
    value_weight,
    w_out,
    w_gate,
    w_up,
    w_down,
):
    ctx_size = lax.axis_size("ctx")
    side = lax.axis_index("fsdp")
    me = lax.axis_index("ctx")
    rows, width = block_input.shape[1:]
    half_width = width // 2
    block = rows // 2
    block_count = 2 * ctx_size

    def by_side(own, other, axis):
        return jnp.where(
            side == 0,
            jnp.concatenate([own, other], axis=axis),
            jnp.concatenate([other, own], axis=axis),
        )

    x_own = block_input[0]
    g_own = out_grad[0]
    x_other = swap_fsdp(x_own)

    block_range = jnp.arange(block_count, dtype=jnp.int32)
    slot_of = jnp.sum(
        jnp.where(block_ids[None, :] == block_range[:, None], block_range[None, :], 0), axis=1
    ).astype(jnp.int32)
    owned = lax.dynamic_slice(block_ids, (2 * me,), (2,))
    positions = (
        owned[:, None] * block + jnp.arange(block, dtype=jnp.int32)[None, :]
    ).reshape(rows)
    part = KEY_HEADS * HEAD_SIZE
    angles = positions.astype(F32)[:, None] * jnp.asarray(frequency_row(part))[None, :]
    cosine = jnp.cos(angles)
    sine = jnp.sin(angles) * jnp.asarray(sign_row(part))[None, :]
    bits, bits_z = bit_order(ctx_size), bit_order(ctx_size, True)

    x_f = x_own.astype(F32)
    normed_one, inverse_one = norm_stats(x_f)
    normed_both = jnp.concatenate([normed_one, norm_stats(x_other.astype(F32))[0]], axis=0)
    own_columns = lax.dynamic_slice_in_dim(normed_both, side * half_width, half_width, axis=1)
    left = (own_columns * gain_attn.astype(F32)).astype(BF16)

    def partial_product(weight):
        product = dot_nn(left, weight)
        return product[:rows], swap_fsdp(product[rows:].astype(BF16))

    k_own, k_got = partial_product(key_weight)
    v_own, v_got = partial_product(value_weight)
    q_own, q_got = partial_product(w_query)
    own_kv = rotary_kv(k_own, k_got, v_own, v_got, cosine, sine)
    all_kv = gather_ctx(own_kv, 1)
    query = rotary_sum(q_own, q_got, cosine, sine)

    g_other = swap_fsdp(after(g_own, v_own))
    gains = jnp.stack([gain_attn, gain_ffn])
    gains = by_side(gains, swap_fsdp(gains), 1).astype(F32)
    gain_one, gain_two = gains[0], gains[1]
    core = me % 2
    out_half = w_out.shape[0] // 2
    mine = lax.dynamic_slice_in_dim(w_out, core * out_half, out_half, axis=0)
    mine = swap_fsdp(after(mine, v_own))
    theirs = swap_bit(mine, 0)
    out_other = jnp.where(
        core == 0,
        jnp.concatenate([mine, theirs], axis=0),
        jnp.concatenate([theirs, mine], axis=0),
    )
    full_out = by_side(w_out, out_other, 1)
    n1_turned = (normed_both * gain_one).astype(BF16).T
    g_both = jnp.concatenate([g_own, g_other], axis=0)

    wide_rows = width // ctx_size
    wide_start = me % (ctx_size // 2) * wide_rows
    w_rows = [
        lax.dynamic_slice_in_dim(w, wide_start, wide_rows, axis=0).reshape(2, -1, w.shape[1])
        for w in (w_query, key_weight, value_weight)
    ]
    w_rows = jnp.concatenate(w_rows, axis=2)
    w_got = swap_fsdp(after(pick(w_rows, 0, 1 - side), v_own))
    w_rows = jnp.where(side == me // (ctx_size // 2), pick(w_rows, 0, side), w_got)

    mixed, lse = attention_forward(query, all_kv, slot_of, owned, block)
    mixed_other = swap_fsdp(mixed)
    resid_mid = x_f + dot_nn(mixed, full_out)
    normed_two, inverse_two = norm_stats(resid_mid)
    n2 = (normed_two * gain_two).astype(BF16)
    n2_both = jnp.concatenate([n2, swap_fsdp(n2)], axis=0)

    gate = dot_nn(n2_both, w_gate)
    up = dot_nn(n2_both, w_up)
    sig = jax.nn.sigmoid(gate)
    silu = gate * sig
    hidden = (silu * up).astype(BF16)
    hidden_grad = dot_nt(g_both, w_down)
    gate_grad = (hidden_grad * up * sig * (1.0 + gate * (1.0 - sig))).astype(BF16)
    up_grad = (hidden_grad * silu).astype(BF16)
    n2_grad = dot_nt(gate_grad, w_gate) + dot_nt(up_grad, w_up)
    n2_grad = n2_grad[:rows] + swap_fsdp(n2_grad[rows:].astype(BF16)).astype(F32)
    ffn = dot_nn(hidden, w_down)
    ffn = ffn[:rows] + swap_fsdp(ffn[rows:].astype(BF16)).astype(F32)
    block_output = (resid_mid + ffn).astype(BF16)
    n2_turned = n2_both.T
    grad_gate = weight_grad(n2_turned, gate_grad, bits)
    grad_up = weight_grad(n2_turned, up_grad, bits)
    grad_down = weight_grad(g_both.T, hidden, bits_z).T

    mid_grad = g_own.astype(F32) + norm_back(n2_grad, normed_two, inverse_two, gain_two)
    mid_grad_b = mid_grad.astype(BF16)
    mid_both = jnp.concatenate([mid_grad_b, swap_fsdp(mid_grad_b)], axis=0)
    mixed_both = jnp.concatenate([mixed, mixed_other], axis=0)
    mixed_grad = dot_nt(mid_grad_b, full_out).astype(BF16)
    cosine_pad = jnp.where(jnp.arange(LANES) < HEAD_SIZE, cosine[:, :LANES], 0.0)
    sine_pad = jnp.where(jnp.arange(LANES) < HEAD_SIZE, sine[:, :LANES], 0.0)
    dq, dk_parts, dv_parts = attention_backward(
        query,
        mixed_grad,
        mixed,
        lse,
        cosine_pad,
        sine_pad,
        all_kv,
        slot_of,
        owned,
        block_ids,
        block,
    )
    dk_sum, dv_sum = reduce_ctx([dk_parts, dv_parts], 2)
    dkv = rotary_back(dk_sum, dv_sum, cosine, sine)
    dkv_both = jnp.concatenate([dkv, swap_fsdp(dkv)], axis=0)
    dq_both = jnp.concatenate([dq, swap_fsdp(dq)], axis=0)

    n1_grad = (
        dot_nt(dq_both, w_query)
        + dot_nt(dkv_both[:, :part], key_weight)
        + dot_nt(dkv_both[:, part:], value_weight)
    )
    n1_got = swap_fsdp(n1_grad[rows:].astype(BF16)).astype(F32)
    n1_grad = by_side(n1_grad[:rows], n1_got, 1)
    input_grad = mid_grad + norm_back(n1_grad, normed_one, inverse_one, gain_one)

    out_parts = side_parts(mid_both.T, mixed_both)
    query_parts = side_parts(n1_turned, dq_both)
    kv_parts = side_parts(n1_turned, dkv_both)
    grad_out, grad_query, grad_kv = reduce_ctx([out_parts, query_parts, kv_parts], 3)
    grad_out = grad_out.T
    grad_key, grad_value = grad_kv[:, :part], grad_kv[:, part:]

    own_rows = wide_rows // 2
    first_row = (2 * me + side) * own_rows
    own_gains = lax.dynamic_slice_in_dim(gains, first_row, own_rows, axis=1)
    grads_one = jnp.concatenate([grad_query, grad_kv], axis=1)
    gain_one_grad = jnp.sum(w_rows.astype(F32) * grads_one, axis=1) / own_gains[0]
    gate_rows = lax.dynamic_slice_in_dim(w_gate, me * wide_rows, wide_rows, axis=0).astype(F32)
    up_rows = lax.dynamic_slice_in_dim(w_up, me * wide_rows, wide_rows, axis=0).astype(F32)
    sums = jnp.sum(gate_rows * grad_gate + up_rows * grad_up, axis=1).reshape(2, own_rows)
    sums = pick(sums, 0, side) + swap_fsdp(pick(sums, 0, 1 - side))
    gain_two_grad = sums / own_gains[1]

    return (
        block_output[None],
        input_grad[None],
        gain_one_grad,
        gain_two_grad,
        grad_query,
        grad_key,
        grad_value,
        grad_out,
        grad_gate,
        grad_up,
        grad_down,
    )


def solution(mesh):
    return jax.shard_map(
        local,
        mesh=mesh,
        in_specs=(
            P("fsdp", "ctx", None),
            P("fsdp", "ctx", None),
            P(),
            P("fsdp"),
            P("fsdp"),
            P("fsdp", None),
            P("fsdp", None),
            P("fsdp", None),
            P(None, "fsdp"),
            P(None, "fsdp"),
            P(None, "fsdp"),
            P("fsdp", None),
        ),
        out_specs=(
            P("fsdp", "ctx", None),
            P("fsdp", "ctx", None),
            P(("ctx", "fsdp")),
            P(("ctx", "fsdp")),
            P(("ctx", "fsdp"), None),
            P(("ctx", "fsdp"), None),
            P(("ctx", "fsdp"), None),
            P(None, ("ctx", "fsdp")),
            P("ctx", "fsdp"),
            P("ctx", "fsdp"),
            P("fsdp", "ctx"),
        ),
        check_vma=False,
    )
```

```python
import functools
import math

import jax
import jax.numpy as jnp
import numpy as np
from jax import lax
from jax.experimental import pallas as pl
from jax.experimental.pallas import tpu as pltpu
from jax.sharding import PartitionSpec as P


QUERY_HEADS = 16
KEY_HEADS = 8
HEAD_SIZE = 96
GROUP = QUERY_HEADS // KEY_HEADS
LANES = 128
PAIR_LANES = 256
HEADS_STEP = 4
TILE_BLOCKS = 4

EPS = 1e-05
THETA = 100000.0
NEGATIVE_FLOOR = -1e30
LOG2E = math.log2(math.e)
SCALE = HEAD_SIZE ** (-0.5)
VMEM_BYTES = 66_000_000
SMALL_VMEM_BYTES = 24_000_000

F32 = jnp.float32
BF16 = jnp.bfloat16


def dot_nn(left, right):
    return lax.dot_general(left, right, (((1,), (0,)), ((), ())), preferred_element_type=F32)


def dot_nt(left, right):
    return lax.dot_general(left, right, (((1,), (1,)), ((), ())), preferred_element_type=F32)


def frequency_row(width):
    lane = np.arange(width)
    half = HEAD_SIZE // 2
    freq = np.exp(-math.log(THETA) * 2.0 * (lane % HEAD_SIZE % half) / HEAD_SIZE)
    return freq.astype(np.float32)


def sign_row(width):
    lane = np.arange(width)
    return np.where(lane % HEAD_SIZE < HEAD_SIZE // 2, -1.0, 1.0).astype(np.float32)


def swap_halves(value):
    width = value.shape[1]
    half = HEAD_SIZE // 2
    lane = lax.broadcasted_iota(jnp.int32, value.shape, 1)
    lower = lax.rem(lane, HEAD_SIZE) < half
    return jnp.where(lower, pltpu.roll(value, width - half, 1), pltpu.roll(value, half, 1))


def rotary_kernel(sign, first, second, cosine, sine, out):
    total = first[...].astype(F32) + second[...].astype(F32)
    out[...] = (total * cosine[...] + sign * swap_halves(total) * sine[...]).astype(BF16)


def rotary_sum(first, second, cosine, sine):
    rows, width = first.shape
    part = cosine.shape[1]
    spec = pl.BlockSpec((rows, part), lambda i: (0, i))
    table = pl.BlockSpec((rows, part), lambda i: (0, 0))
    return pl.pallas_call(
        functools.partial(rotary_kernel, 1.0),
        out_shape=jax.ShapeDtypeStruct((rows, width), BF16),
        grid=(width // part,),
        in_specs=[spec, spec, table, table],
        out_specs=spec,
        name="rotary_sum",
        cost_estimate=pl.CostEstimate(
            flops=6 * rows * width, bytes_accessed=8 * rows * width, transcendentals=0
        ),
    )(first, second, cosine, sine)


def rotary_kv_kernel(k_own, k_got, v_own, v_got, cosine, sine, out):
    width = k_own.shape[1]
    keys = k_own[...] + k_got[...].astype(F32)
    out[:, :width] = (keys * cosine[...] + swap_halves(keys) * sine[...]).astype(BF16)
    out[:, width:] = (v_own[...] + v_got[...].astype(F32)).astype(BF16)


def rotary_kv(k_own, k_got, v_own, v_got, cosine, sine):
    rows, width = k_own.shape
    return pl.pallas_call(
        rotary_kv_kernel,
        out_shape=jax.ShapeDtypeStruct((rows, 2 * width), BF16),
        name="rotary_kv",
        cost_estimate=pl.CostEstimate(
            flops=8 * rows * width, bytes_accessed=20 * rows * width, transcendentals=0
        ),
    )(k_own, k_got, v_own, v_got, cosine, sine)


def rotary_back_kernel(keys, values, cosine, sine, out):
    width = keys.shape[1]
    total = keys[...]
    out[:, :width] = (total * cosine[...] - swap_halves(total) * sine[...]).astype(BF16)
    out[:, width:] = values[...].astype(BF16)


def rotary_back(keys, values, cosine, sine):
    rows, width = keys.shape
    return pl.pallas_call(
        rotary_back_kernel,
        out_shape=jax.ShapeDtypeStruct((rows, 2 * width), BF16),
        name="rotary_back",
        cost_estimate=pl.CostEstimate(
            flops=6 * rows * width, bytes_accessed=20 * rows * width, transcendentals=0
        ),
    )(keys, values, cosine, sine)


def pair_lanes(pair):
    return slice(pair * LANES, pair * LANES + PAIR_LANES)


def pair_rows(rows, pair):
    blocks = []
    for i in range(2 * GROUP):
        head = 2 * GROUP * pair + i
        offset = (2 * pair + i // GROUP) * HEAD_SIZE - pair * LANES
        pieces = [rows[:, head * HEAD_SIZE : (head + 1) * HEAD_SIZE]]
        if offset:
            pieces.insert(0, jnp.zeros((rows.shape[0], offset), rows.dtype))
        rest = PAIR_LANES - HEAD_SIZE - offset
        if rest:
            pieces.append(jnp.zeros((rows.shape[0], rest), rows.dtype))
        blocks.append(jnp.concatenate(pieces, axis=1))
    return jnp.concatenate(blocks, axis=0)


def tile_rows(ref, slot_of, tile, block):
    pieces = []
    for i in range(TILE_BLOCKS):
        start = pl.multiple_of(slot_of[tile * TILE_BLOCKS + i] * block, block)
        pieces.append(ref[pl.ds(start, block), :])
    return jnp.concatenate(pieces, axis=0)


def allowed(tile, tile_len, query_block, block, columns):
    key_pos = tile * tile_len + lax.broadcasted_iota(jnp.int32, (tile_len, columns), 0)
    column = lax.broadcasted_iota(jnp.int32, (tile_len, columns), 1)
    query_pos = query_block * block + lax.rem(column, block)
    return key_pos <= query_pos


def vmem_for(length):
    return SMALL_VMEM_BYTES if length <= 4096 else VMEM_BYTES


def fold(value, how):
    return how(value.reshape(value.shape[0] // 8, 8, value.shape[1]), axis=0)


def head_rows(turned, block):
    upright = turned.T.astype(BF16)
    return [upright[r * block : (r + 1) * block, :] for r in range(GROUP)]


def forward_kernel(block, slot_of, owned, q_ref, k_ref, v_ref, o_ref, lse_ref, scores, acc, top, total):
    tile_len = TILE_BLOCKS * block
    pairs = HEADS_STEP // 2
    columns = 2 * GROUP * block
    per_head = GROUP * block
    for m in range(2):
        count = (owned[m] + TILE_BLOCKS) // TILE_BLOCKS
        q_rows = q_ref[m * block : (m + 1) * block, :]
        queries = [pair_rows(q_rows, p) for p in range(pairs)]
        top[...] = jnp.full(top.shape, NEGATIVE_FLOOR, F32)
        total[...] = jnp.zeros(total.shape, F32)
        acc[...] = jnp.zeros(acc.shape, F32)

        def score_pass(tile, carry, queries=queries, m=m):
            start = pl.multiple_of(tile * tile_len, tile_len)
            mask = allowed(tile, tile_len, owned[m], block, columns)
            keys = tile_rows(k_ref, slot_of, tile, block)
            for p in range(pairs):
                value = dot_nt(keys[:, pair_lanes(p)], queries[p])
                value = jnp.where(mask, value * (SCALE * LOG2E), NEGATIVE_FLOOR)
                scores[p, pl.ds(start, tile_len), :] = value
                top[p] = jnp.maximum(top[p], fold(value, jnp.max))
            return carry

        lax.fori_loop(0, count, score_pass, 0)
        peaks = [jnp.max(top[p], axis=0, keepdims=True) for p in range(pairs)]

        def mix_pass(tile, carry, peaks=peaks):
            start = pl.multiple_of(tile * tile_len, tile_len)
            turned = tile_rows(v_ref, slot_of, tile, block).T
            for p in range(pairs):
                weight = jnp.exp2(scores[p, pl.ds(start, tile_len), :] - peaks[p])
                total[p] += fold(weight, jnp.sum)
                weight = weight.astype(BF16)
                for i in range(2):
                    h = 2 * p + i
                    acc[h] += dot_nn(
                        turned[h * HEAD_SIZE : (h + 1) * HEAD_SIZE, :],
                        weight[:, i * per_head : (i + 1) * per_head],
                    )
            return carry

        lax.fori_loop(0, count, mix_pass, 0)
        merged = []
        for p in range(pairs):
            denom = jnp.sum(total[p], axis=0, keepdims=True)
            lse_ref[p, m : m + 1, :] = peaks[p] + jnp.log2(denom)
            for i in range(2):
                merged += head_rows(acc[2 * p + i] / denom[:, i * per_head : (i + 1) * per_head], block)
        o_ref[m * block : (m + 1) * block, :] = jnp.concatenate(merged, axis=1)


def kv_specs(length, heads_width):
    mode = {} if length <= 4096 else {"pipeline_mode": pl.Buffered(1)}
    return [
        pl.BlockSpec((length, heads_width), lambda i, *_, base=base: (0, base + i), **mode)
        for base in (0, KEY_HEADS // HEADS_STEP)
    ]


def attention_forward(query, all_kv, slot_of, owned, block):
    rows = query.shape[0]
    length = all_kv.shape[0]
    steps = KEY_HEADS // HEADS_STEP
    pairs = HEADS_STEP // 2
    key_width = HEADS_STEP * HEAD_SIZE
    columns = 2 * GROUP * block
    query_spec = pl.BlockSpec((rows, key_width * GROUP), lambda i, *_: (0, i))
    return pl.pallas_call(
        functools.partial(forward_kernel, block),
        out_shape=(
            jax.ShapeDtypeStruct(query.shape, BF16),
            jax.ShapeDtypeStruct((KEY_HEADS // 2, 2, columns), F32),
        ),
        grid_spec=pltpu.PrefetchScalarGridSpec(
            num_scalar_prefetch=2,
            grid=(steps,),
            in_specs=[query_spec] + kv_specs(length, key_width),
            out_specs=[query_spec, pl.BlockSpec((pairs, 2, columns), lambda i, *_: (i, 0, 0))],
            scratch_shapes=[
                pltpu.VMEM((pairs, length, columns), F32),
                pltpu.VMEM((HEADS_STEP, HEAD_SIZE, GROUP * block), F32),
                pltpu.VMEM((pairs, 8, columns), F32),
                pltpu.VMEM((pairs, 8, columns), F32),
            ],
        ),
        compiler_params=pltpu.CompilerParams(vmem_limit_bytes=VMEM_BYTES),
        name="attention_forward",
        cost_estimate=pl.CostEstimate(
            flops=4 * rows * length * query.shape[1] // 2,
            bytes_accessed=2 * all_kv.size,
            transcendentals=rows * length * QUERY_HEADS // 2,
        ),
    )(slot_of, owned, query, all_kv, all_kv)


def backward_kernel(
    block,
    slot_of,
    owned,
    block_ids,
    q_ref,
    do_ref,
    o_ref,
    lse_ref,
    cos_ref,
    sin_ref,
    k_ref,
    v_ref,
    dq_ref,
    dk_out,
    dv_out,
    dk,
    dv,
    acc,
):
    tile_len = TILE_BLOCKS * block
    pairs = HEADS_STEP // 2
    columns = 2 * GROUP * block
    per_head = GROUP * block
    dk[...] = jnp.zeros_like(dk)
    dv[...] = jnp.zeros_like(dv)
    for m in range(2):
        count = (owned[m] + TILE_BLOCKS) // TILE_BLOCKS
        member = slice(m * block, (m + 1) * block)
        q_rows, g_rows, o_rows = q_ref[member, :], do_ref[member, :], o_ref[member, :]
        queries = [pair_rows(q_rows, p) for p in range(pairs)]
        grads = [pair_rows(g_rows, p) for p in range(pairs)]
        deltas = []
        for p in range(pairs):
            product = grads[p].astype(F32) * pair_rows(o_rows, p).astype(F32)
            deltas.append(jnp.sum(product.T, axis=0, keepdims=True))
        lses = [lse_ref[p, m : m + 1, :] for p in range(pairs)]
        acc[...] = jnp.zeros(acc.shape, F32)

        def grad_pass(tile, carry, queries=queries, grads=grads, deltas=deltas, lses=lses, m=m):
            start = pl.multiple_of(tile * tile_len, tile_len)
            mask = allowed(tile, tile_len, owned[m], block, columns)
            keys = tile_rows(k_ref, slot_of, tile, block)
            values = tile_rows(v_ref, slot_of, tile, block)
            turned = keys.T
            for p in range(pairs):
                lanes = pair_lanes(p)
                value = dot_nt(keys[:, lanes], queries[p])
                value = jnp.where(mask, value * (SCALE * LOG2E) - lses[p], NEGATIVE_FLOOR)
                prob = jnp.exp2(value)
                grad_prob = dot_nt(values[:, lanes], grads[p])
                grad_score = (prob * (grad_prob - deltas[p]) * SCALE).astype(BF16)
                dk[pl.ds(start, tile_len), lanes] += dot_nn(grad_score, queries[p])
                dv[pl.ds(start, tile_len), lanes] += dot_nn(prob.astype(BF16), grads[p])
                for i in range(2):
                    h = 2 * p + i
                    acc[h] += dot_nn(
                        turned[h * HEAD_SIZE : (h + 1) * HEAD_SIZE, :],
                        grad_score[:, i * per_head : (i + 1) * per_head],
                    )
            return carry

        lax.fori_loop(0, count, grad_pass, 0)
        merged = []
        for h in range(HEADS_STEP):
            grad = acc[h]
            middle = HEAD_SIZE // 2
            swapped = jnp.concatenate([grad[middle:], grad[:middle]], axis=0)
            merged += head_rows(grad * cos_ref[m] - swapped * sin_ref[m], block)
        dq_ref[member, :] = jnp.concatenate(merged, axis=1)

    def unpack(chunk, carry):
        for source, target in ((dk, dk_out), (dv, dv_out)):
            for i in range(2):
                start = pl.multiple_of(block_ids[2 * chunk + i] * block, block)
                target[chunk, i * block : (i + 1) * block, :] = source[pl.ds(start, block), :].astype(BF16)
        return carry

    lax.fori_loop(0, dk_out.shape[0], unpack, 0)


def attention_backward(
    query, grad, mixed, lse, cosine, sine, all_kv, slot_of, owned, block_ids, block
):
    rows = query.shape[0]
    length = all_kv.shape[0]
    chunks = length // rows
    steps = KEY_HEADS // HEADS_STEP
    pairs = HEADS_STEP // 2
    key_width = HEADS_STEP * HEAD_SIZE
    columns = 2 * GROUP * block
    query_spec = pl.BlockSpec((rows, key_width * GROUP), lambda i, *_: (0, i))
    mode = {} if length <= 4096 else {"pipeline_mode": pl.Buffered(1)}
    out_spec = pl.BlockSpec((chunks, rows, key_width), lambda i, *_: (0, 0, i), **mode)
    table = pl.BlockSpec(cosine.shape, lambda i, *_: (0, 0, 0))
    grad_shape = jax.ShapeDtypeStruct((chunks, rows, all_kv.shape[1] // 2), BF16)
    return pl.pallas_call(
        functools.partial(backward_kernel, block),
        out_shape=(jax.ShapeDtypeStruct(query.shape, BF16),) + (grad_shape,) * 2,
        grid_spec=pltpu.PrefetchScalarGridSpec(
            num_scalar_prefetch=3,
            grid=(steps,),
            in_specs=[
                query_spec,
                query_spec,
                query_spec,
                pl.BlockSpec((pairs, 2, columns), lambda i, *_: (i, 0, 0)),
                table,
                table,
            ]
            + kv_specs(length, key_width),
            out_specs=[query_spec] + [out_spec] * 2,
            scratch_shapes=[
                pltpu.VMEM((length, key_width), F32),
                pltpu.VMEM((length, key_width), F32),
                pltpu.VMEM((HEADS_STEP, HEAD_SIZE, GROUP * block), F32),
            ],
        ),
        compiler_params=pltpu.CompilerParams(vmem_limit_bytes=VMEM_BYTES),
        name="attention_backward",
        cost_estimate=pl.CostEstimate(
            flops=10 * rows * length * query.shape[1] // 2,
            bytes_accessed=4 * all_kv.size,
            transcendentals=rows * length * QUERY_HEADS // 2,
        ),
    )(slot_of, owned, block_ids, query, grad, mixed, lse, cosine, sine, all_kv, all_kv)


def place():
    me = lax.axis_index("ctx")
    return me // 4, me // 2 % 2, me % 2


def device_at(line, mid, core):
    return {"ctx": (line * 2 + mid) * 2 + core}


def greet(line, mid, core, count):
    barrier = pltpu.get_barrier_semaphore()

    def call(*where):
        pl.semaphore_signal(
            barrier, inc=1, device_id=device_at(*where), device_id_type=pl.DeviceIdType.MESH
        )

    call(line, 1 - mid, core)
    call(line, mid, 1 - core)

    @pl.when(line > 0)
    def _():
        call(line - 1, mid, core)

    @pl.when(line + 1 < count)
    def _():
        call(line + 1, mid, core)

    ends = jnp.where(line > 0, 1, 0) + jnp.where(line + 1 < count, 1, 0)
    pl.semaphore_wait(barrier, 2 + ends)


def remote(source, target, send, recv, where):
    return pltpu.make_async_remote_copy(
        src_ref=source,
        dst_ref=target,
        send_sem=send,
        recv_sem=recv,
        device_id=device_at(*where),
        device_id_type=pl.DeviceIdType.MESH,
    )


def gather_kernel(
    count, own, out, here, right_send, left_send, mid_send, core_send, line_recv, mid_recv, core_recv
):
    line, mid, core = place()
    rows = own.shape[0]
    greet(line, mid, core, count)

    def slot(j, m, k):
        start = pl.multiple_of(((j * 2 + m) * 2 + k) * rows, rows)
        return out.at[pl.ds(start, rows)]

    def to_right(j, source):
        return remote(source, slot(j, mid, core), right_send.at[j], line_recv.at[j], (line + 1, mid, core))

    def to_left(j, source):
        return remote(source, slot(j, mid, core), left_send.at[j], line_recv.at[j], (line - 1, mid, core))

    def to_mid(j, source):
        return remote(source, slot(j, mid, core), mid_send.at[j], mid_recv.at[j], (line, 1 - mid, core))

    def to_core(j, m, source):
        return remote(
            source, slot(j, m, core), core_send.at[2 * j + m], core_recv.at[2 * j + m], (line, mid, 1 - core)
        )

    keep = pltpu.make_async_copy(own, slot(line, mid, core), here)
    keep.start()
    to_mid(line, own).start()

    @pl.when(line + 1 < count)
    def _():
        to_right(line, own).start()

    @pl.when(line > 0)
    def _():
        to_left(line, own).start()

    to_core(line, mid, own).start()


    def arrived_line(j, step_right):
        block = slot(j, mid, core)
        to_right(j, block).wait_recv()
        if step_right:

            @pl.when(line + 1 < count)
            def _():
                to_right(j, block).start()

        else:

            @pl.when(line > 0)
            def _():
                to_left(j, block).start()

        to_mid(j, block).start()
        to_core(j, mid, block).start()

    def arrived_mid(j):
        block = slot(j, 1 - mid, core)
        remote(block, block, mid_send.at[j], mid_recv.at[j], (line, 1 - mid, core)).wait_recv()
        to_core(j, 1 - mid, block).start()

    for step in range(1, count + 1):
        if step < count:

            @pl.when(line - step >= 0)
            def _(step=step):
                arrived_line(line - step, True)

            @pl.when(line + step < count)
            def _(step=step):
                arrived_line(line + step, False)

        if step == 1:
            arrived_mid(line)
        else:

            @pl.when(line - (step - 1) >= 0)
            def _(step=step):
                arrived_mid(line - (step - 1))

            @pl.when(line + (step - 1) < count)
            def _(step=step):
                arrived_mid(line + (step - 1))

    for j in range(count):
        for m in range(2):
            block = slot(j, m, 1 - core)
            remote(
                block, block, core_send.at[2 * j + m], core_recv.at[2 * j + m], (line, mid, 1 - core)
            ).wait_recv()
    keep.wait()
    for j in range(count):
        block = slot(j, mid, core)
        to_mid(j, block).wait_send()
        for m in range(2):
            to_core(j, m, slot(j, m, core)).wait_send()

        @pl.when(jnp.logical_and(j <= line, line + 1 < count))
        def _(j=j, block=block):
            to_right(j, block).wait_send()

        @pl.when(jnp.logical_and(j >= line, line > 0))
        def _(j=j, block=block):
            to_left(j, block).wait_send()


def gather_ctx(own, collective_id):
    size = lax.axis_size("ctx")
    rows, width = own.shape
    count = size // 4
    dma = pltpu.SemaphoreType.DMA
    return pl.pallas_call(
        functools.partial(gather_kernel, count),
        out_shape=jax.ShapeDtypeStruct((size * rows, width), own.dtype),
        in_specs=[pl.BlockSpec(memory_space=pltpu.VMEM)],
        out_specs=pl.BlockSpec(memory_space=pl.ANY),
        scratch_shapes=[dma(())] + [dma((count,))] * 3 + [dma((2 * count,))] + [dma((count,))] * 2 + [dma((2 * count,))],
        compiler_params=pltpu.CompilerParams(
            collective_id=collective_id, has_side_effects=True, vmem_limit_bytes=SMALL_VMEM_BYTES
        ),
        cost_estimate=pl.CostEstimate(
            flops=0, bytes_accessed=100 * size * rows * width, transcendentals=0
        ),
    )(own)


def reduce_kernel(count, parts, *refs):
    sources, outs = refs[:parts], refs[parts : 2 * parts]
    scratch = refs[2 * parts :]
    work, from_core, from_mid, from_right, from_left = (scratch[i * parts : (i + 1) * parts] for i in range(5))
    (load, core_send, core_recv, mid_send, mid_recv, left_send, right_send, right_recv, left_recv) = scratch[5 * parts :]
    line, mid, core = place()
    greet(line, mid, core, count)

    def nearest_last(visit):
        for step in range(count - 1, 0, -1):
            for j in (line - step, line + step):

                @pl.when(jnp.logical_and(j >= 0, j < count))
                def _(j=j):
                    visit(j)

        visit(line)

    def core_copy(s, j, m):
        index = 2 * j + m
        return remote(
            sources[s].at[2 * index + (1 - core)],
            from_core[s].at[index],
            core_send.at[s, index],
            core_recv.at[s, index],
            (line, mid, 1 - core),
        )

    def load_copy(s, j, m):
        index = 2 * j + m
        return pltpu.make_async_copy(sources[s].at[2 * index + core], work[s].at[index], load.at[s, index])

    def mid_copy(s, j):
        return remote(
            work[s].at[2 * j + (1 - mid)],
            from_mid[s].at[j],
            mid_send.at[s, j],
            mid_recv.at[s, j],
            (line, 1 - mid, core),
        )

    def left_copy(s, j):
        return remote(
            work[s].at[2 * j + mid],
            from_right[s].at[j],
            left_send.at[s, j],
            right_recv.at[s, j],
            (line - 1, mid, core),
        )

    def right_copy(s, j):
        return remote(
            work[s].at[2 * j + mid],
            from_left[s].at[j],
            right_send.at[s, j],
            left_recv.at[s, j],
            (line + 1, mid, core),
        )

    def add(s, index, other):
        work[s][index] = (work[s][index].astype(F32) + other.astype(F32)).astype(work[s].dtype)

    for m in (1 - mid, mid):

        def begin(j, m=m):
            for s in range(parts):
                core_copy(s, j, m).start()
                load_copy(s, j, m).start()

        nearest_last(begin)

    def core_sum(s, j, m):
        core_copy(s, j, m).wait_recv()
        load_copy(s, j, m).wait()
        add(s, 2 * j + m, from_core[s][2 * j + m])

    def to_mid(j):
        for s in range(parts):
            core_sum(s, j, 1 - mid)
            mid_copy(s, j).start()

    nearest_last(to_mid)

    def keep_mine(j):
        for s in range(parts):
            core_sum(s, j, mid)

    nearest_last(keep_mine)

    def along(j):
        for s in range(parts):
            mid_copy(s, j).wait_recv()
            add(s, 2 * j + mid, from_mid[s][j])

            @pl.when(j < line)
            def _(s=s):
                @pl.when(line + 1 < count)
                def _():
                    left_copy(s, j).wait_recv()
                    add(s, 2 * j + mid, from_right[s][j])

                left_copy(s, j).start()

            @pl.when(j > line)
            def _(s=s):
                @pl.when(line > 0)
                def _():
                    right_copy(s, j).wait_recv()
                    add(s, 2 * j + mid, from_left[s][j])

                right_copy(s, j).start()

    nearest_last(along)
    for s in range(parts):
        outs[s][...] = work[s][2 * line + mid].astype(F32)

        @pl.when(line + 1 < count)
        def _(s=s):
            left_copy(s, line).wait_recv()
            outs[s][...] += from_right[s][line].astype(F32)

        @pl.when(line > 0)
        def _(s=s):
            right_copy(s, line).wait_recv()
            outs[s][...] += from_left[s][line].astype(F32)

    for s in range(parts):
        for j in range(count):
            mid_copy(s, j).wait_send()
            for m in range(2):
                core_copy(s, j, m).wait_send()

            @pl.when(j < line)
            def _(s=s, j=j):
                left_copy(s, j).wait_send()

            @pl.when(j > line)
            def _(s=s, j=j):
                right_copy(s, j).wait_send()


def reduce_ctx(sources, collective_id):
    size = lax.axis_size("ctx")
    count = size // 4
    parts = len(sources)
    dma = pltpu.SemaphoreType.DMA

    def room(chunks):
        return [pltpu.VMEM((chunks,) + source.shape[1:], source.dtype) for source in sources]

    return pl.pallas_call(
        functools.partial(reduce_kernel, count, parts),
        out_shape=[jax.ShapeDtypeStruct(source.shape[1:], F32) for source in sources],
        in_specs=[pl.BlockSpec(memory_space=pl.ANY)] * parts,
        out_specs=[pl.BlockSpec(memory_space=pltpu.VMEM)] * parts,
        scratch_shapes=room(2 * count) + room(2 * count) + room(count) * 1 + room(count) + room(count)
        + [dma((parts, 2 * count))] * 3
        + [dma((parts, count))] * 6,
        compiler_params=pltpu.CompilerParams(
            collective_id=collective_id,
            has_side_effects=True,
            vmem_limit_bytes=vmem_for(size * sources[0].shape[1]),
        ),
        cost_estimate=pl.CostEstimate(
            flops=0, bytes_accessed=100 * sum(source.size for source in sources), transcendentals=0
        ),
    )(*sources)


def swap_fsdp(value):
    size = lax.axis_size("fsdp")
    return lax.ppermute(value, "fsdp", [(i, size - 1 - i) for i in range(size)])


def swap_bit(value, bit):
    size = lax.axis_size("ctx")
    return lax.ppermute(value, "ctx", [(i, i ^ (1 << bit)) for i in range(size)])


def bit_order(size, swapped=False):
    bits = list(range(size.bit_length() - 1))
    if swapped and len(bits) > 2:
        bits[1], bits[2] = bits[2], bits[1]
    return bits


def relative_order(bits):
    last = len(bits) - 1
    return [
        sum(((p >> (last - i)) & 1) << bit for i, bit in enumerate(bits)) for p in range(2 << last)
    ]


def chunk_places(bits):
    place_of = np.argsort(np.asarray(relative_order(bits))).astype(np.int32)
    me = lax.axis_index("ctx")
    distance = jnp.arange(len(place_of), dtype=jnp.int32) ^ me
    found = distance[:, None] == jnp.arange(len(place_of), dtype=jnp.int32)[None, :]
    return jnp.sum(jnp.where(found, jnp.asarray(place_of)[None, :], 0), axis=1)


def pick(value, axis, index):
    return lax.dynamic_index_in_dim(value, index, axis, keepdims=False)


def halve(keep, send, bits):
    for bit in bits:
        got = swap_bit(send, bit)
        if keep.shape[0] == 1:
            return keep[0].astype(F32) + got[0].astype(F32)
        mid = keep.shape[0] // 2
        send = (keep[mid:].astype(F32) + got[mid:].astype(F32)).astype(BF16)
        keep = (keep[:mid].astype(F32) + got[:mid].astype(F32)).astype(BF16)


def weight_grad(left, right, bits):
    count, rows, tokens = left.shape

    def piece(part):
        product = dot_nn(part.reshape(count // 2 * rows, tokens), right)
        return product.astype(BF16).reshape(count // 2, rows, right.shape[1])

    send = piece(left[count // 2 :])
    keep = piece(left[: count // 2])
    return halve(keep, send, bits)


def ffn_kernel(
    places, n_own, n_other, g_own, g_other, w_gate, w_up, w_down,
    gate_out, up_out, hidden_out, n_chunks, g_chunks, ng_own, ng_send, ffn_own, ffn_send,
    n_both, g_both, n_grad, ffn_sum,
):
    step, steps = pl.program_id(0), pl.num_programs(0)
    rows = n_own.shape[0]
    count, chunk, _ = n_chunks.shape

    @pl.when(step == 0)
    def _():
        n_both[:rows], n_both[rows:] = n_own[...], n_other[...]
        g_both[:rows], g_both[rows:] = g_own[...], g_other[...]
        for source, target, base in ((n_both, n_chunks, 0), (g_both, g_chunks, count)):
            turned = source[...].astype(F32).T
            for c in range(count):
                target[places[base + c]] = turned[c * chunk : (c + 1) * chunk, :].astype(BF16)
        n_grad[...] = jnp.zeros(n_grad.shape, F32)
        ffn_sum[...] = jnp.zeros(ffn_sum.shape, F32)

    wg, wu, wd = w_gate[...], w_up[...], w_down[...]
    gate = dot_nn(n_both[...], wg)
    up = dot_nn(n_both[...], wu)
    hidden_grad = dot_nt(g_both[...], wd)
    sig = jax.nn.sigmoid(gate)
    silu = gate * sig
    hidden = (silu * up).astype(BF16)
    gate_grad = (hidden_grad * up * sig * (1.0 + gate * (1.0 - sig))).astype(BF16)
    up_grad = (hidden_grad * silu).astype(BF16)
    gate_out[...], up_out[...], hidden_out[...] = gate_grad, up_grad, hidden
    n_grad[...] += dot_nt(gate_grad, wg) + dot_nt(up_grad, wu)
    ffn_sum[...] += dot_nn(hidden, wd)

    @pl.when(step == steps - 1)
    def _():
        ng_own[...], ng_send[...] = n_grad[:rows], n_grad[rows:].astype(BF16)
        ffn_own[...], ffn_send[...] = ffn_sum[:rows], ffn_sum[rows:].astype(BF16)


def ffn(n_own, n_other, g_own, g_other, w_gate, w_up, w_down, places):
    rows, width = n_own.shape
    hidden = w_gate.shape[1]
    count = places.shape[0] // 2
    tile = min(256, hidden)
    whole = pl.BlockSpec((rows, width), lambda i, *_: (0, 0))
    columns = pl.BlockSpec((width, tile), lambda i, *_: (0, i))
    acts = pl.BlockSpec((2 * rows, tile), lambda i, *_: (0, i))
    chunks = pl.BlockSpec((count, width // count, 2 * rows), lambda i, *_: (0, 0, 0))
    act = jax.ShapeDtypeStruct((2 * rows, hidden), BF16)
    turned = jax.ShapeDtypeStruct((count, width // count, 2 * rows), BF16)
    own = jax.ShapeDtypeStruct((rows, width), F32)
    send = jax.ShapeDtypeStruct((rows, width), BF16)
    return pl.pallas_call(
        ffn_kernel,
        out_shape=(act, act, act, turned, turned, own, send, own, send),
        grid_spec=pltpu.PrefetchScalarGridSpec(
            num_scalar_prefetch=1,
            grid=(hidden // tile,),
            in_specs=[whole] * 4
            + [columns, columns, pl.BlockSpec((tile, width), lambda i, *_: (i, 0))],
            out_specs=[acts] * 3 + [chunks] * 2 + [whole] * 4,
            scratch_shapes=[
                pltpu.VMEM((2 * rows, width), BF16),
                pltpu.VMEM((2 * rows, width), BF16),
                pltpu.VMEM((2 * rows, width), F32),
                pltpu.VMEM((2 * rows, width), F32),
            ],
        ),
        compiler_params=pltpu.CompilerParams(vmem_limit_bytes=2 * SMALL_VMEM_BYTES),
        name="ffn",
        cost_estimate=pl.CostEstimate(
            flops=24 * rows * width * hidden,
            bytes_accessed=6 * width * hidden + 12 * rows * hidden,
            transcendentals=2 * rows * hidden,
        ),
    )(places, n_own, n_other, g_own, g_other, w_gate, w_up, w_down)


def side_parts(left, right):
    size = lax.axis_size("ctx")
    width, tokens = left.shape
    rows = width // (2 * size)
    flat = pick(left.reshape(size, 2, rows, tokens), 1, lax.axis_index("fsdp"))
    product = dot_nn(flat.reshape(size * rows, tokens), right).astype(BF16)
    return product.reshape(size, rows, right.shape[1])


def after(value, anchor):
    return lax.optimization_barrier((value, anchor))[0]


def norm_stats(value):
    inverse = lax.rsqrt(jnp.mean(value * value, axis=-1, keepdims=True) + EPS)
    return (value * inverse, inverse)


def norm_back(grad, normed, inverse, gain):
    scaled = grad * gain
    return inverse * (scaled - normed * jnp.mean(scaled * normed, axis=-1, keepdims=True))


def local(
    block_input,
    out_grad,
    block_ids,
    gain_attn,
    gain_ffn,
    w_query,
    key_weight,
    value_weight,
    w_out,
    w_gate,
    w_up,
    w_down,
):
    ctx_size = lax.axis_size("ctx")
    side = lax.axis_index("fsdp")
    me = lax.axis_index("ctx")
    rows, width = block_input.shape[1:]
    half_width = width // 2
    block = rows // 2
    block_count = 2 * ctx_size

    def by_side(own, other, axis):
        return jnp.where(
            side == 0,
            jnp.concatenate([own, other], axis=axis),
            jnp.concatenate([other, own], axis=axis),
        )

    x_own = block_input[0]
    g_own = out_grad[0]
    x_other = swap_fsdp(x_own)

    block_range = jnp.arange(block_count, dtype=jnp.int32)
    slot_of = jnp.sum(
        jnp.where(block_ids[None, :] == block_range[:, None], block_range[None, :], 0), axis=1
    ).astype(jnp.int32)
    owned = lax.dynamic_slice(block_ids, (2 * me,), (2,))
    positions = (
        owned[:, None] * block + jnp.arange(block, dtype=jnp.int32)[None, :]
    ).reshape(rows)
    part = KEY_HEADS * HEAD_SIZE
    angles = positions.astype(F32)[:, None] * jnp.asarray(frequency_row(part))[None, :]
    cosine = jnp.cos(angles)
    sine = jnp.sin(angles) * jnp.asarray(sign_row(part))[None, :]
    bits, bits_z = bit_order(ctx_size), bit_order(ctx_size, True)

    x_f = x_own.astype(F32)
    normed_one, inverse_one = norm_stats(x_f)
    normed_both = jnp.concatenate([normed_one, norm_stats(x_other.astype(F32))[0]], axis=0)
    own_columns = lax.dynamic_slice_in_dim(normed_both, side * half_width, half_width, axis=1)
    left = (own_columns * gain_attn.astype(F32)).astype(BF16)

    def partial_product(weight):
        product = dot_nn(left, weight)
        return product[:rows], swap_fsdp(product[rows:].astype(BF16))

    k_own, k_got = partial_product(key_weight)
    v_own, v_got = partial_product(value_weight)
    q_own, q_got = partial_product(w_query)
    own_kv = rotary_kv(k_own, k_got, v_own, v_got, cosine, sine)
    all_kv = gather_ctx(own_kv, 1)
    query = rotary_sum(q_own, q_got, cosine, sine)

    g_other = swap_fsdp(after(g_own, v_own))
    gains = jnp.stack([gain_attn, gain_ffn])
    gains = by_side(gains, swap_fsdp(gains), 1).astype(F32)
    gain_one, gain_two = gains[0], gains[1]
    core = me % 2
    out_half = w_out.shape[0] // 2
    mine = lax.dynamic_slice_in_dim(w_out, core * out_half, out_half, axis=0)
    mine = swap_fsdp(after(mine, v_own))
    theirs = swap_bit(mine, 0)
    out_other = jnp.where(
        core == 0,
        jnp.concatenate([mine, theirs], axis=0),
        jnp.concatenate([theirs, mine], axis=0),
    )
    full_out = by_side(w_out, out_other, 1)
    n1_turned = (normed_both * gain_one).astype(BF16).T

    mixed, lse = attention_forward(query, all_kv, slot_of, owned, block)
    mixed_other = swap_fsdp(mixed)
    resid_mid = x_f + dot_nn(mixed, full_out)
    normed_two, inverse_two = norm_stats(resid_mid)
    n2 = (normed_two * gain_two).astype(BF16)

    places = jnp.concatenate([chunk_places(bits), chunk_places(bits_z)])
    gate_grad, up_grad, hidden, n2_chunks, g_chunks, n2_grad, n2_send, ffn_own, ffn_send = ffn(
        n2, swap_fsdp(n2), g_own, g_other, w_gate, w_up, w_down, places
    )
    n2_grad = n2_grad + swap_fsdp(n2_send).astype(F32)
    ffn_got = swap_fsdp(ffn_send)
    grad_gate = weight_grad(n2_chunks, gate_grad, bits)
    grad_up = weight_grad(n2_chunks, up_grad, bits)
    grad_down = weight_grad(g_chunks, hidden, bits_z).T

    mid_grad = g_own.astype(F32) + norm_back(n2_grad, normed_two, inverse_two, gain_two)
    mid_grad_b = mid_grad.astype(BF16)
    mid_both = jnp.concatenate([mid_grad_b, swap_fsdp(mid_grad_b)], axis=0)
    mixed_both = jnp.concatenate([mixed, mixed_other], axis=0)
    mixed_grad = dot_nt(mid_grad_b, full_out).astype(BF16)
    row_pos = jnp.concatenate([positions.reshape(2, block)] * GROUP, axis=1).astype(F32)
    turned_angles = row_pos[:, None, :] * jnp.asarray(frequency_row(HEAD_SIZE))[None, :, None]
    turned_cosine = jnp.cos(turned_angles)
    turned_sine = jnp.sin(turned_angles) * jnp.asarray(sign_row(HEAD_SIZE))[None, :, None]
    dq, dk_parts, dv_parts = attention_backward(
        query,
        mixed_grad,
        mixed,
        lse,
        turned_cosine,
        turned_sine,
        all_kv,
        slot_of,
        owned,
        block_ids,
        block,
    )
    dk_sum, dv_sum = reduce_ctx([dk_parts, dv_parts], 2)
    dkv = rotary_back(dk_sum, dv_sum, cosine, sine)
    block_output = (resid_mid + (ffn_own + after(ffn_got, dq).astype(F32))).astype(BF16)
    dkv_both = jnp.concatenate([dkv, swap_fsdp(dkv)], axis=0)
    dq_both = jnp.concatenate([dq, swap_fsdp(dq)], axis=0)

    wide_rows = width // ctx_size
    wide_start = me % (ctx_size // 2) * wide_rows
    w_rows = [
        lax.dynamic_slice_in_dim(w, wide_start, wide_rows, axis=0).reshape(2, -1, w.shape[1])
        for w in after((w_query, key_weight, value_weight), dkv_both)
    ]
    w_rows = jnp.concatenate(w_rows, axis=2)
    w_got = swap_fsdp(pick(w_rows, 0, 1 - side))
    w_rows = jnp.where(side == me // (ctx_size // 2), pick(w_rows, 0, side), w_got)

    n1_grad = (
        dot_nt(dq_both, w_query)
        + dot_nt(dkv_both[:, :part], key_weight)
        + dot_nt(dkv_both[:, part:], value_weight)
    )
    n1_got = swap_fsdp(n1_grad[rows:].astype(BF16)).astype(F32)
    n1_grad = by_side(n1_grad[:rows], n1_got, 1)
    input_grad = mid_grad + norm_back(n1_grad, normed_one, inverse_one, gain_one)

    out_parts = side_parts(mid_both.T, mixed_both)
    query_parts = side_parts(n1_turned, dq_both)
    kv_parts = side_parts(n1_turned, dkv_both)
    grad_out, grad_query, grad_kv = reduce_ctx([out_parts, query_parts, kv_parts], 3)
    grad_out = grad_out.T
    grad_key, grad_value = grad_kv[:, :part], grad_kv[:, part:]

    own_rows = wide_rows // 2
    first_row = (2 * me + side) * own_rows
    own_gains = lax.dynamic_slice_in_dim(gains, first_row, own_rows, axis=1)
    grads_one = jnp.concatenate([grad_query, grad_kv], axis=1)
    gain_one_grad = jnp.sum(w_rows.astype(F32) * grads_one, axis=1) / own_gains[0]
    gate_rows = lax.dynamic_slice_in_dim(w_gate, me * wide_rows, wide_rows, axis=0).astype(F32)
    up_rows = lax.dynamic_slice_in_dim(w_up, me * wide_rows, wide_rows, axis=0).astype(F32)
    sums = jnp.sum(gate_rows * grad_gate + up_rows * grad_up, axis=1).reshape(2, own_rows)
    sums = pick(sums, 0, side) + swap_fsdp(pick(sums, 0, 1 - side))
    gain_two_grad = sums / own_gains[1]

    return (
        block_output[None],
        input_grad[None],
        gain_one_grad,
        gain_two_grad,
        grad_query,
        grad_key,
        grad_value,
        grad_out,
        grad_gate,
        grad_up,
        grad_down,
    )


def solution(mesh):
    return jax.shard_map(
        local,
        mesh=mesh,
        in_specs=(
            P("fsdp", "ctx", None),
            P("fsdp", "ctx", None),
            P(),
            P("fsdp"),
            P("fsdp"),
            P("fsdp", None),
            P("fsdp", None),
            P("fsdp", None),
            P(None, "fsdp"),
            P(None, "fsdp"),
            P(None, "fsdp"),
            P("fsdp", None),
        ),
        out_specs=(
            P("fsdp", "ctx", None),
            P("fsdp", "ctx", None),
            P(("ctx", "fsdp")),
            P(("ctx", "fsdp")),
            P(("ctx", "fsdp"), None),
            P(("ctx", "fsdp"), None),
            P(("ctx", "fsdp"), None),
            P(None, ("ctx", "fsdp")),
            P("ctx", "fsdp"),
            P("ctx", "fsdp"),
            P("fsdp", "ctx"),
        ),
        check_vma=False,
    )
```

```python
import functools
import math

import jax
import jax.numpy as jnp
import numpy as np
from jax import lax
from jax.experimental import pallas as pl
from jax.experimental.pallas import tpu as pltpu
from jax.sharding import PartitionSpec as P


QUERY_HEADS = 16
KEY_HEADS = 8
HEAD_SIZE = 96
GROUP = QUERY_HEADS // KEY_HEADS
LANES = 128
PAIR_LANES = 256
HEADS_STEP = 4
CTX, FSDP = "ctx", "fsdp"
TILE_BLOCKS = 4

EPS = 1e-05
THETA = 100000.0
NEGATIVE_FLOOR = -1e30
LOG2E = math.log2(math.e)
SCALE = HEAD_SIZE ** (-0.5)
VMEM_BYTES = 66_000_000
SMALL_VMEM_BYTES = 24_000_000

F32 = jnp.float32
BF16 = jnp.bfloat16


def dot_nn(left, right):
    return lax.dot_general(left, right, (((1,), (0,)), ((), ())), preferred_element_type=F32)


def dot_nt(left, right):
    return lax.dot_general(left, right, (((1,), (1,)), ((), ())), preferred_element_type=F32)


def frequency_row(width):
    lane = np.arange(width)
    half = HEAD_SIZE // 2
    freq = np.exp(-math.log(THETA) * 2.0 * (lane % HEAD_SIZE % half) / HEAD_SIZE)
    return freq.astype(np.float32)


def sign_row(width):
    lane = np.arange(width)
    return np.where(lane % HEAD_SIZE < HEAD_SIZE // 2, -1.0, 1.0).astype(np.float32)


def swap_halves(value):
    width = value.shape[1]
    half = HEAD_SIZE // 2
    lane = lax.broadcasted_iota(jnp.int32, value.shape, 1)
    lower = lax.rem(lane, HEAD_SIZE) < half
    return jnp.where(lower, pltpu.roll(value, width - half, 1), pltpu.roll(value, half, 1))


def rotary_kv_kernel(k_own, k_got, v_own, v_got, cosine, sine, out):
    width = k_own.shape[1]
    keys = k_own[...] + k_got[...].astype(F32)
    out[:, :width] = (keys * cosine[...] + swap_halves(keys) * sine[...]).astype(BF16)
    out[:, width:] = (v_own[...] + v_got[...].astype(F32)).astype(BF16)


def rotary_kv(k_own, k_got, v_own, v_got, cosine, sine):
    rows, width = k_own.shape
    return pl.pallas_call(
        rotary_kv_kernel,
        out_shape=jax.ShapeDtypeStruct((rows, 2 * width), BF16),
        cost_estimate=pl.CostEstimate(
            flops=8 * rows * width, bytes_accessed=20 * rows * width, transcendentals=0
        ),
    )(k_own, k_got, v_own, v_got, cosine, sine)


def rotary_back_kernel(keys, values, cosine, sine, out):
    width = keys.shape[1]
    total = keys[...]
    out[:, :width] = (total * cosine[...] - swap_halves(total) * sine[...]).astype(BF16)
    out[:, width:] = values[...].astype(BF16)


def rotary_back(keys, values, cosine, sine):
    rows, width = keys.shape
    return pl.pallas_call(
        rotary_back_kernel,
        out_shape=jax.ShapeDtypeStruct((rows, 2 * width), BF16),
        cost_estimate=pl.CostEstimate(
            flops=6 * rows * width, bytes_accessed=20 * rows * width, transcendentals=0
        ),
    )(keys, values, cosine, sine)


def pair_lanes(pair):
    return slice(pair * LANES, pair * LANES + PAIR_LANES)


def pair_rows(rows, pair):
    blocks = []
    for i in range(2 * GROUP):
        head = 2 * GROUP * pair + i
        offset = (2 * pair + i // GROUP) * HEAD_SIZE - pair * LANES
        pieces = [rows[:, head * HEAD_SIZE : (head + 1) * HEAD_SIZE]]
        if offset:
            pieces.insert(0, jnp.zeros((rows.shape[0], offset), rows.dtype))
        rest = PAIR_LANES - HEAD_SIZE - offset
        if rest:
            pieces.append(jnp.zeros((rows.shape[0], rest), rows.dtype))
        blocks.append(jnp.concatenate(pieces, axis=1))
    return jnp.concatenate(blocks, axis=0)


def tile_rows(ref, slot_of, tile, block):
    pieces = []
    for i in range(TILE_BLOCKS):
        start = pl.multiple_of(slot_of[tile * TILE_BLOCKS + i] * block, block)
        pieces.append(ref[pl.ds(start, block), :])
    return jnp.concatenate(pieces, axis=0)


def allowed(tile, tile_len, query_block, block, columns):
    key_pos = tile * tile_len + lax.broadcasted_iota(jnp.int32, (tile_len, columns), 0)
    column = lax.broadcasted_iota(jnp.int32, (tile_len, columns), 1)
    query_pos = query_block * block + lax.rem(column, block)
    return key_pos <= query_pos


def vmem_for(length):
    return SMALL_VMEM_BYTES if length <= 4096 else VMEM_BYTES


def fold(value, how):
    return how(value.reshape(value.shape[0] // 8, 8, value.shape[1]), axis=0)


def head_rows(turned, block):
    upright = turned.T.astype(BF16)
    return [upright[r * block : (r + 1) * block, :] for r in range(GROUP)]


def forward_kernel(
    block, slot_of, owned, q_own, q_got, cosine, sine, k_ref, v_ref, o_ref, lse_ref, q_ref, scores, acc, top, total
):
    query = q_own[...] + q_got[...].astype(F32)
    q_ref[...] = (query * cosine[...] + swap_halves(query) * sine[...]).astype(BF16)
    tile_len = TILE_BLOCKS * block
    pairs = HEADS_STEP // 2
    columns = 2 * GROUP * block
    per_head = GROUP * block
    for m in range(2):
        count = (owned[m] + TILE_BLOCKS) // TILE_BLOCKS
        q_rows = q_ref[m * block : (m + 1) * block, :]
        queries = [pair_rows(q_rows, p) for p in range(pairs)]
        top[...] = jnp.full(top.shape, NEGATIVE_FLOOR, F32)
        total[...] = jnp.zeros(total.shape, F32)
        acc[...] = jnp.zeros(acc.shape, F32)

        def score_pass(tile, carry, queries=queries, m=m):
            start = pl.multiple_of(tile * tile_len, tile_len)
            mask = allowed(tile, tile_len, owned[m], block, columns)
            keys = tile_rows(k_ref, slot_of, tile, block)
            for p in range(pairs):
                value = dot_nt(keys[:, pair_lanes(p)], queries[p])
                value = jnp.where(mask, value * (SCALE * LOG2E), NEGATIVE_FLOOR)
                scores[p, pl.ds(start, tile_len), :] = value
                top[p] = jnp.maximum(top[p], fold(value, jnp.max))
            return carry

        lax.fori_loop(0, count, score_pass, 0)
        peaks = [jnp.max(top[p], axis=0, keepdims=True) for p in range(pairs)]

        def mix_pass(tile, carry, peaks=peaks):
            start = pl.multiple_of(tile * tile_len, tile_len)
            turned = tile_rows(v_ref, slot_of, tile, block).T
            for p in range(pairs):
                weight = jnp.exp2(scores[p, pl.ds(start, tile_len), :] - peaks[p])
                total[p] += fold(weight, jnp.sum)
                weight = weight.astype(BF16)
                for i in range(2):
                    h = 2 * p + i
                    acc[h] += dot_nn(
                        turned[h * HEAD_SIZE : (h + 1) * HEAD_SIZE, :],
                        weight[:, i * per_head : (i + 1) * per_head],
                    )
            return carry

        lax.fori_loop(0, count, mix_pass, 0)
        merged = []
        for p in range(pairs):
            denom = jnp.sum(total[p], axis=0, keepdims=True)
            lse_ref[p, m : m + 1, :] = peaks[p] + jnp.log2(denom)
            for i in range(2):
                merged += head_rows(acc[2 * p + i] / denom[:, i * per_head : (i + 1) * per_head], block)
        o_ref[m * block : (m + 1) * block, :] = jnp.concatenate(merged, axis=1)


def kv_specs(length, heads_width):
    mode = {} if length <= 4096 else {"pipeline_mode": pl.Buffered(1)}
    return [
        pl.BlockSpec((length, heads_width), lambda i, *_, base=base: (0, base + i), **mode)
        for base in (0, KEY_HEADS // HEADS_STEP)
    ]


def attention_forward(q_own, q_got, cosine, sine, all_kv, slot_of, owned, block):
    rows = q_own.shape[0]
    length = all_kv.shape[0]
    steps = KEY_HEADS // HEADS_STEP
    pairs = HEADS_STEP // 2
    key_width = HEADS_STEP * HEAD_SIZE
    columns = 2 * GROUP * block
    query_spec = pl.BlockSpec((rows, key_width * GROUP), lambda i, *_: (0, i))
    table = pl.BlockSpec(cosine.shape, lambda i, *_: (0, 0))
    return pl.pallas_call(
        functools.partial(forward_kernel, block),
        out_shape=(
            jax.ShapeDtypeStruct(q_own.shape, BF16),
            jax.ShapeDtypeStruct((KEY_HEADS // 2, 2, columns), F32),
            jax.ShapeDtypeStruct(q_own.shape, BF16),
        ),
        grid_spec=pltpu.PrefetchScalarGridSpec(
            num_scalar_prefetch=2,
            grid=(steps,),
            in_specs=[query_spec, query_spec, table, table] + kv_specs(length, key_width),
            out_specs=[
                query_spec,
                pl.BlockSpec((pairs, 2, columns), lambda i, *_: (i, 0, 0)),
                query_spec,
            ],
            scratch_shapes=[
                pltpu.VMEM((pairs, length, columns), F32),
                pltpu.VMEM((HEADS_STEP, HEAD_SIZE, GROUP * block), F32),
                pltpu.VMEM((pairs, 8, columns), F32),
                pltpu.VMEM((pairs, 8, columns), F32),
            ],
        ),
        compiler_params=pltpu.CompilerParams(vmem_limit_bytes=VMEM_BYTES),
        cost_estimate=pl.CostEstimate(
            flops=4 * rows * length * q_own.shape[1] // 2,
            bytes_accessed=2 * all_kv.size,
            transcendentals=rows * length * QUERY_HEADS // 2,
        ),
    )(slot_of, owned, q_own, q_got, cosine, sine, all_kv, all_kv)


def backward_kernel(
    block,
    slot_of,
    owned,
    block_ids,
    q_ref,
    do_ref,
    o_ref,
    lse_ref,
    cos_ref,
    sin_ref,
    k_ref,
    v_ref,
    dq_ref,
    dk_out,
    dv_out,
    dk,
    dv,
    acc,
):
    tile_len = TILE_BLOCKS * block
    pairs = HEADS_STEP // 2
    columns = 2 * GROUP * block
    per_head = GROUP * block
    dk[...] = jnp.zeros_like(dk)
    dv[...] = jnp.zeros_like(dv)
    for m in range(2):
        count = (owned[m] + TILE_BLOCKS) // TILE_BLOCKS
        member = slice(m * block, (m + 1) * block)
        q_rows, g_rows, o_rows = q_ref[member, :], do_ref[member, :], o_ref[member, :]
        queries = [pair_rows(q_rows, p) for p in range(pairs)]
        grads = [pair_rows(g_rows, p) for p in range(pairs)]
        deltas = []
        for p in range(pairs):
            product = grads[p].astype(F32) * pair_rows(o_rows, p).astype(F32)
            deltas.append(jnp.sum(product.T, axis=0, keepdims=True))
        lses = [lse_ref[p, m : m + 1, :] for p in range(pairs)]
        acc[...] = jnp.zeros(acc.shape, F32)

        def grad_pass(tile, carry, queries=queries, grads=grads, deltas=deltas, lses=lses, m=m):
            start = pl.multiple_of(tile * tile_len, tile_len)
            mask = allowed(tile, tile_len, owned[m], block, columns)
            keys = tile_rows(k_ref, slot_of, tile, block)
            values = tile_rows(v_ref, slot_of, tile, block)
            turned = keys.T
            for p in range(pairs):
                lanes = pair_lanes(p)
                value = dot_nt(keys[:, lanes], queries[p])
                value = jnp.where(mask, value * (SCALE * LOG2E) - lses[p], NEGATIVE_FLOOR)
                prob = jnp.exp2(value)
                grad_prob = dot_nt(values[:, lanes], grads[p])
                grad_score = (prob * (grad_prob - deltas[p]) * SCALE).astype(BF16)
                dk[pl.ds(start, tile_len), lanes] += dot_nn(grad_score, queries[p])
                dv[pl.ds(start, tile_len), lanes] += dot_nn(prob.astype(BF16), grads[p])
                for i in range(2):
                    h = 2 * p + i
                    acc[h] += dot_nn(
                        turned[h * HEAD_SIZE : (h + 1) * HEAD_SIZE, :],
                        grad_score[:, i * per_head : (i + 1) * per_head],
                    )
            return carry

        lax.fori_loop(0, count, grad_pass, 0)
        merged = []
        for h in range(HEADS_STEP):
            grad = acc[h]
            middle = HEAD_SIZE // 2
            swapped = jnp.concatenate([grad[middle:], grad[:middle]], axis=0)
            merged += head_rows(grad * cos_ref[m] - swapped * sin_ref[m], block)
        dq_ref[member, :] = jnp.concatenate(merged, axis=1)

    def unpack(chunk, carry):
        for source, target in ((dk, dk_out), (dv, dv_out)):
            for i in range(2):
                start = pl.multiple_of(block_ids[2 * chunk + i] * block, block)
                target[chunk, i * block : (i + 1) * block, :] = source[pl.ds(start, block), :].astype(BF16)
        return carry

    lax.fori_loop(0, dk_out.shape[0], unpack, 0)


def attention_backward(
    query, grad, mixed, lse, cosine, sine, all_kv, slot_of, owned, block_ids, block
):
    rows = query.shape[0]
    length = all_kv.shape[0]
    chunks = length // rows
    steps = KEY_HEADS // HEADS_STEP
    pairs = HEADS_STEP // 2
    key_width = HEADS_STEP * HEAD_SIZE
    columns = 2 * GROUP * block
    query_spec = pl.BlockSpec((rows, key_width * GROUP), lambda i, *_: (0, i))
    mode = {} if length <= 4096 else {"pipeline_mode": pl.Buffered(1)}
    out_spec = pl.BlockSpec((chunks, rows, key_width), lambda i, *_: (0, 0, i), **mode)
    table = pl.BlockSpec(cosine.shape, lambda i, *_: (0, 0, 0))
    grad_shape = jax.ShapeDtypeStruct((chunks, rows, all_kv.shape[1] // 2), BF16)
    return pl.pallas_call(
        functools.partial(backward_kernel, block),
        out_shape=(jax.ShapeDtypeStruct(query.shape, BF16),) + (grad_shape,) * 2,
        grid_spec=pltpu.PrefetchScalarGridSpec(
            num_scalar_prefetch=3,
            grid=(steps,),
            in_specs=[
                query_spec,
                query_spec,
                query_spec,
                pl.BlockSpec((pairs, 2, columns), lambda i, *_: (i, 0, 0)),
                table,
                table,
            ]
            + kv_specs(length, key_width),
            out_specs=[query_spec] + [out_spec] * 2,
            scratch_shapes=[
                pltpu.VMEM((length, key_width), F32),
                pltpu.VMEM((length, key_width), F32),
                pltpu.VMEM((HEADS_STEP, HEAD_SIZE, GROUP * block), F32),
            ],
        ),
        compiler_params=pltpu.CompilerParams(vmem_limit_bytes=VMEM_BYTES),
        cost_estimate=pl.CostEstimate(
            flops=10 * rows * length * query.shape[1] // 2,
            bytes_accessed=4 * all_kv.size,
            transcendentals=rows * length * QUERY_HEADS // 2,
        ),
    )(slot_of, owned, block_ids, query, grad, mixed, lse, cosine, sine, all_kv, all_kv)


def place():
    me = lax.axis_index(CTX)
    return me // 4, me // 2 % 2, me % 2


def device_at(line, mid, core):
    return {CTX: (line * 2 + mid) * 2 + core}


def greet(line, mid, core, count):
    barrier = pltpu.get_barrier_semaphore()

    def call(*where):
        pl.semaphore_signal(
            barrier, inc=1, device_id=device_at(*where), device_id_type=pl.DeviceIdType.MESH
        )

    call(line, 1 - mid, core)
    call(line, mid, 1 - core)

    @pl.when(line > 0)
    def _():
        call(line - 1, mid, core)

    @pl.when(line + 1 < count)
    def _():
        call(line + 1, mid, core)

    ends = jnp.where(line > 0, 1, 0) + jnp.where(line + 1 < count, 1, 0)
    pl.semaphore_wait(barrier, 2 + ends)


def remote(source, target, send, recv, where):
    return pltpu.make_async_remote_copy(
        src_ref=source,
        dst_ref=target,
        send_sem=send,
        recv_sem=recv,
        device_id=device_at(*where),
        device_id_type=pl.DeviceIdType.MESH,
    )


def gather_kernel(
    count, own, out, here, right_send, left_send, mid_send, core_send, line_recv, mid_recv, core_recv
):
    line, mid, core = place()
    rows = own.shape[0]
    greet(line, mid, core, count)

    def slot(j, m, k):
        start = pl.multiple_of(((j * 2 + m) * 2 + k) * rows, rows)
        return out.at[pl.ds(start, rows)]

    def to_right(j, source):
        return remote(source, slot(j, mid, core), right_send.at[j], line_recv.at[j], (line + 1, mid, core))

    def to_left(j, source):
        return remote(source, slot(j, mid, core), left_send.at[j], line_recv.at[j], (line - 1, mid, core))

    def to_mid(j, source):
        return remote(source, slot(j, mid, core), mid_send.at[j], mid_recv.at[j], (line, 1 - mid, core))

    def to_core(j, m, source):
        return remote(
            source, slot(j, m, core), core_send.at[2 * j + m], core_recv.at[2 * j + m], (line, mid, 1 - core)
        )

    keep = pltpu.make_async_copy(own, slot(line, mid, core), here)
    keep.start()
    to_mid(line, own).start()

    @pl.when(line + 1 < count)
    def _():
        to_right(line, own).start()

    @pl.when(line > 0)
    def _():
        to_left(line, own).start()

    to_core(line, mid, own).start()


    def arrived_line(j, step_right):
        block = slot(j, mid, core)
        to_right(j, block).wait_recv()
        if step_right:

            @pl.when(line + 1 < count)
            def _():
                to_right(j, block).start()

        else:

            @pl.when(line > 0)
            def _():
                to_left(j, block).start()

        to_mid(j, block).start()
        to_core(j, mid, block).start()

    def arrived_mid(j):
        block = slot(j, 1 - mid, core)
        remote(block, block, mid_send.at[j], mid_recv.at[j], (line, 1 - mid, core)).wait_recv()
        to_core(j, 1 - mid, block).start()

    for step in range(1, count + 1):
        if step < count:

            @pl.when(line - step >= 0)
            def _(step=step):
                arrived_line(line - step, True)

            @pl.when(line + step < count)
            def _(step=step):
                arrived_line(line + step, False)

        if step == 1:
            arrived_mid(line)
        else:

            @pl.when(line - (step - 1) >= 0)
            def _(step=step):
                arrived_mid(line - (step - 1))

            @pl.when(line + (step - 1) < count)
            def _(step=step):
                arrived_mid(line + (step - 1))

    for j in range(count):
        for m in range(2):
            block = slot(j, m, 1 - core)
            remote(
                block, block, core_send.at[2 * j + m], core_recv.at[2 * j + m], (line, mid, 1 - core)
            ).wait_recv()
    keep.wait()
    for j in range(count):
        block = slot(j, mid, core)
        to_mid(j, block).wait_send()
        for m in range(2):
            to_core(j, m, slot(j, m, core)).wait_send()

        @pl.when(jnp.logical_and(j <= line, line + 1 < count))
        def _(j=j, block=block):
            to_right(j, block).wait_send()

        @pl.when(jnp.logical_and(j >= line, line > 0))
        def _(j=j, block=block):
            to_left(j, block).wait_send()


def gather_ctx(own, collective_id):
    size = lax.axis_size(CTX)
    rows, width = own.shape
    count = size // 4
    dma = pltpu.SemaphoreType.DMA
    return pl.pallas_call(
        functools.partial(gather_kernel, count),
        out_shape=jax.ShapeDtypeStruct((size * rows, width), own.dtype),
        in_specs=[pl.BlockSpec(memory_space=pltpu.VMEM)],
        out_specs=pl.BlockSpec(memory_space=pl.ANY),
        scratch_shapes=[dma(())] + [dma((count,))] * 3 + [dma((2 * count,))] + [dma((count,))] * 2 + [dma((2 * count,))],
        compiler_params=pltpu.CompilerParams(
            collective_id=collective_id, has_side_effects=True, vmem_limit_bytes=SMALL_VMEM_BYTES
        ),
        cost_estimate=pl.CostEstimate(
            flops=0, bytes_accessed=100 * size * rows * width, transcendentals=0
        ),
    )(own)


def reduce_kernel(count, parts, *refs):
    sources, outs = refs[:parts], refs[parts : 2 * parts]
    scratch = refs[2 * parts :]
    work, from_core, from_mid, from_right, from_left = (scratch[i * parts : (i + 1) * parts] for i in range(5))
    (load, core_send, core_recv, mid_send, mid_recv, left_send, right_send, right_recv, left_recv) = scratch[5 * parts :]
    line, mid, core = place()
    greet(line, mid, core, count)

    def nearest_last(visit):
        for step in range(count - 1, 0, -1):
            for j in (line - step, line + step):

                @pl.when(jnp.logical_and(j >= 0, j < count))
                def _(j=j):
                    visit(j)

        visit(line)

    def core_copy(s, j, m):
        index = 2 * j + m
        return remote(
            sources[s].at[2 * index + (1 - core)],
            from_core[s].at[index],
            core_send.at[s, index],
            core_recv.at[s, index],
            (line, mid, 1 - core),
        )

    def load_copy(s, j, m):
        index = 2 * j + m
        return pltpu.make_async_copy(sources[s].at[2 * index + core], work[s].at[index], load.at[s, index])

    def mid_copy(s, j):
        return remote(
            work[s].at[2 * j + (1 - mid)],
            from_mid[s].at[j],
            mid_send.at[s, j],
            mid_recv.at[s, j],
            (line, 1 - mid, core),
        )

    def left_copy(s, j):
        return remote(
            work[s].at[2 * j + mid],
            from_right[s].at[j],
            left_send.at[s, j],
            right_recv.at[s, j],
            (line - 1, mid, core),
        )

    def right_copy(s, j):
        return remote(
            work[s].at[2 * j + mid],
            from_left[s].at[j],
            right_send.at[s, j],
            left_recv.at[s, j],
            (line + 1, mid, core),
        )

    def add(s, index, other):
        work[s][index] = (work[s][index].astype(F32) + other.astype(F32)).astype(work[s].dtype)

    for m in (1 - mid, mid):

        def begin(j, m=m):
            for s in range(parts):
                core_copy(s, j, m).start()
                load_copy(s, j, m).start()

        nearest_last(begin)

    def core_sum(s, j, m):
        core_copy(s, j, m).wait_recv()
        load_copy(s, j, m).wait()
        add(s, 2 * j + m, from_core[s][2 * j + m])

    def to_mid(j):
        for s in range(parts):
            core_sum(s, j, 1 - mid)
            mid_copy(s, j).start()

    nearest_last(to_mid)

    def keep_mine(j):
        for s in range(parts):
            core_sum(s, j, mid)

    nearest_last(keep_mine)

    def along(j):
        for s in range(parts):
            mid_copy(s, j).wait_recv()
            add(s, 2 * j + mid, from_mid[s][j])

            @pl.when(j < line)
            def _(s=s):
                @pl.when(line + 1 < count)
                def _():
                    left_copy(s, j).wait_recv()
                    add(s, 2 * j + mid, from_right[s][j])

                left_copy(s, j).start()

            @pl.when(j > line)
            def _(s=s):
                @pl.when(line > 0)
                def _():
                    right_copy(s, j).wait_recv()
                    add(s, 2 * j + mid, from_left[s][j])

                right_copy(s, j).start()

    nearest_last(along)
    for s in range(parts):
        outs[s][...] = work[s][2 * line + mid].astype(F32)

        @pl.when(line + 1 < count)
        def _(s=s):
            left_copy(s, line).wait_recv()
            outs[s][...] += from_right[s][line].astype(F32)

        @pl.when(line > 0)
        def _(s=s):
            right_copy(s, line).wait_recv()
            outs[s][...] += from_left[s][line].astype(F32)

    for s in range(parts):
        for j in range(count):
            mid_copy(s, j).wait_send()
            for m in range(2):
                core_copy(s, j, m).wait_send()

            @pl.when(j < line)
            def _(s=s, j=j):
                left_copy(s, j).wait_send()

            @pl.when(j > line)
            def _(s=s, j=j):
                right_copy(s, j).wait_send()


def reduce_ctx(sources, collective_id):
    size = lax.axis_size(CTX)
    count = size // 4
    parts = len(sources)
    dma = pltpu.SemaphoreType.DMA

    def room(chunks):
        return [pltpu.VMEM((chunks,) + source.shape[1:], source.dtype) for source in sources]

    return pl.pallas_call(
        functools.partial(reduce_kernel, count, parts),
        out_shape=[jax.ShapeDtypeStruct(source.shape[1:], F32) for source in sources],
        in_specs=[pl.BlockSpec(memory_space=pl.ANY)] * parts,
        out_specs=[pl.BlockSpec(memory_space=pltpu.VMEM)] * parts,
        scratch_shapes=room(2 * count) + room(2 * count) + room(count) * 1 + room(count) + room(count)
        + [dma((parts, 2 * count))] * 3
        + [dma((parts, count))] * 6,
        compiler_params=pltpu.CompilerParams(
            collective_id=collective_id,
            has_side_effects=True,
            vmem_limit_bytes=vmem_for(size * sources[0].shape[1]),
        ),
        cost_estimate=pl.CostEstimate(
            flops=0, bytes_accessed=100 * sum(source.size for source in sources), transcendentals=0
        ),
    )(*sources)


def swap_fsdp(value):
    size = lax.axis_size(FSDP)
    return lax.ppermute(value, FSDP, [(i, size - 1 - i) for i in range(size)])


def swap_bit(value, bit):
    size = lax.axis_size(CTX)
    return lax.ppermute(value, CTX, [(i, i ^ (1 << bit)) for i in range(size)])


def bit_order(size, swapped=False):
    bits = list(range(size.bit_length() - 1))
    if swapped and len(bits) > 2:
        bits[1], bits[2] = bits[2], bits[1]
    return bits


def relative_order(bits):
    last = len(bits) - 1
    return [
        sum(((p >> (last - i)) & 1) << bit for i, bit in enumerate(bits)) for p in range(2 << last)
    ]


def chunk_places(bits):
    place_of = np.argsort(np.asarray(relative_order(bits))).astype(np.int32)
    me = lax.axis_index(CTX)
    distance = jnp.arange(len(place_of), dtype=jnp.int32) ^ me
    found = distance[:, None] == jnp.arange(len(place_of), dtype=jnp.int32)[None, :]
    return jnp.sum(jnp.where(found, jnp.asarray(place_of)[None, :], 0), axis=1)


def pick(value, axis, index):
    return lax.dynamic_index_in_dim(value, index, axis, keepdims=False)


def halve(keep, send, bits):
    for bit in bits:
        got = swap_bit(send, bit)
        if keep.shape[0] == 1:
            return keep[0].astype(F32) + got[0].astype(F32)
        mid = keep.shape[0] // 2
        send = (keep[mid:].astype(F32) + got[mid:].astype(F32)).astype(BF16)
        keep = (keep[:mid].astype(F32) + got[:mid].astype(F32)).astype(BF16)


def weight_grad(left, right, bits):
    count, rows, tokens = left.shape

    def piece(part):
        product = dot_nn(part.reshape(count // 2 * rows, tokens), right)
        return product.astype(BF16).reshape(count // 2, rows, right.shape[1])

    send = piece(left[count // 2 :])
    keep = piece(left[: count // 2])
    return halve(keep, send, bits)


def ffn_kernel(
    places, n_own, n_other, g_own, g_other, w_gate, w_up, w_down,
    gate_out, up_out, hidden_out, n_chunks, g_chunks, ng_own, ng_send, ffn_own, ffn_send,
    n_both, g_both, n_grad, ffn_sum,
):
    step, steps = pl.program_id(0), pl.num_programs(0)
    rows = n_own.shape[0]
    count, chunk, _ = n_chunks.shape

    @pl.when(step == 0)
    def _():
        n_both[:rows], n_both[rows:] = n_own[...], n_other[...]
        g_both[:rows], g_both[rows:] = g_own[...], g_other[...]
        for source, target, base in ((n_both, n_chunks, 0), (g_both, g_chunks, count)):
            turned = source[...].astype(F32).T
            for c in range(count):
                target[places[base + c]] = turned[c * chunk : (c + 1) * chunk, :].astype(BF16)
        n_grad[...] = jnp.zeros(n_grad.shape, F32)
        ffn_sum[...] = jnp.zeros(ffn_sum.shape, F32)

    wg, wu, wd = w_gate[...], w_up[...], w_down[...]
    gate = dot_nn(n_both[...], wg)
    up = dot_nn(n_both[...], wu)
    hidden_grad = dot_nt(g_both[...], wd)
    sig = jax.nn.sigmoid(gate)
    silu = gate * sig
    hidden = (silu * up).astype(BF16)
    gate_grad = (hidden_grad * up * sig * (1.0 + gate * (1.0 - sig))).astype(BF16)
    up_grad = (hidden_grad * silu).astype(BF16)
    gate_out[...], up_out[...], hidden_out[...] = gate_grad, up_grad, hidden
    n_grad[...] += dot_nt(gate_grad, wg) + dot_nt(up_grad, wu)
    ffn_sum[...] += dot_nn(hidden, wd)

    @pl.when(step == steps - 1)
    def _():
        ng_own[...], ng_send[...] = n_grad[:rows], n_grad[rows:].astype(BF16)
        ffn_own[...], ffn_send[...] = ffn_sum[:rows], ffn_sum[rows:].astype(BF16)


def ffn(n_own, n_other, g_own, g_other, w_gate, w_up, w_down, places):
    rows, width = n_own.shape
    hidden = w_gate.shape[1]
    count = places.shape[0] // 2
    tile = min(256, hidden)
    whole = pl.BlockSpec((rows, width), lambda i, *_: (0, 0))
    columns = pl.BlockSpec((width, tile), lambda i, *_: (0, i))
    acts = pl.BlockSpec((2 * rows, tile), lambda i, *_: (0, i))
    chunks = pl.BlockSpec((count, width // count, 2 * rows), lambda i, *_: (0, 0, 0))
    act = jax.ShapeDtypeStruct((2 * rows, hidden), BF16)
    turned = jax.ShapeDtypeStruct((count, width // count, 2 * rows), BF16)
    own = jax.ShapeDtypeStruct((rows, width), F32)
    send = jax.ShapeDtypeStruct((rows, width), BF16)
    return pl.pallas_call(
        ffn_kernel,
        out_shape=(act, act, act, turned, turned, own, send, own, send),
        grid_spec=pltpu.PrefetchScalarGridSpec(
            num_scalar_prefetch=1,
            grid=(hidden // tile,),
            in_specs=[whole] * 4
            + [columns, columns, pl.BlockSpec((tile, width), lambda i, *_: (i, 0))],
            out_specs=[acts] * 3 + [chunks] * 2 + [whole] * 4,
            scratch_shapes=[
                pltpu.VMEM((2 * rows, width), BF16),
                pltpu.VMEM((2 * rows, width), BF16),
                pltpu.VMEM((2 * rows, width), F32),
                pltpu.VMEM((2 * rows, width), F32),
            ],
        ),
        compiler_params=pltpu.CompilerParams(vmem_limit_bytes=2 * SMALL_VMEM_BYTES),
        cost_estimate=pl.CostEstimate(
            flops=24 * rows * width * hidden,
            bytes_accessed=6 * width * hidden + 12 * rows * hidden,
            transcendentals=2 * rows * hidden,
        ),
    )(places, n_own, n_other, g_own, g_other, w_gate, w_up, w_down)


def side_parts(left, right):
    size = lax.axis_size(CTX)
    width, tokens = left.shape
    rows = width // (2 * size)
    flat = pick(left.reshape(size, 2, rows, tokens), 1, lax.axis_index(FSDP))
    product = dot_nn(flat.reshape(size * rows, tokens), right).astype(BF16)
    return product.reshape(size, rows, right.shape[1])


def after(value, anchor):
    return lax.optimization_barrier((value, anchor))[0]


def norm_stats(value):
    inverse = lax.rsqrt(jnp.mean(value * value, axis=-1, keepdims=True) + EPS)
    return (value * inverse, inverse)


def norm_back(grad, normed, inverse, gain):
    scaled = grad * gain
    return inverse * (scaled - normed * jnp.mean(scaled * normed, axis=-1, keepdims=True))


def local(
    block_input,
    out_grad,
    block_ids,
    gain_attn,
    gain_ffn,
    w_query,
    key_weight,
    value_weight,
    w_out,
    w_gate,
    w_up,
    w_down,
):
    ctx_size = lax.axis_size(CTX)
    side = lax.axis_index(FSDP)
    me = lax.axis_index(CTX)
    rows, width = block_input.shape[1:]
    block = rows // 2
    block_count = 2 * ctx_size

    def by_side(own, other, axis):
        return jnp.where(
            side == 0,
            jnp.concatenate([own, other], axis=axis),
            jnp.concatenate([other, own], axis=axis),
        )

    x_own = block_input[0]
    g_own = out_grad[0]
    x_other = swap_fsdp(x_own)

    block_range = jnp.arange(block_count, dtype=jnp.int32)
    slot_of = jnp.sum(
        jnp.where(block_ids[None, :] == block_range[:, None], block_range[None, :], 0), axis=1
    ).astype(jnp.int32)
    owned = lax.dynamic_slice(block_ids, (2 * me,), (2,))
    positions = (
        owned[:, None] * block + jnp.arange(block, dtype=jnp.int32)[None, :]
    ).reshape(rows)
    part = KEY_HEADS * HEAD_SIZE
    angles = positions.astype(F32)[:, None] * jnp.asarray(frequency_row(part))[None, :]
    cosine = jnp.cos(angles)
    sine = jnp.sin(angles) * jnp.asarray(sign_row(part))[None, :]
    bits, bits_z = bit_order(ctx_size), bit_order(ctx_size, True)

    x_f = x_own.astype(F32)
    normed_one, inverse_one = norm_stats(x_f)
    normed_both = jnp.concatenate([normed_one, norm_stats(x_other.astype(F32))[0]], axis=0)
    half_width = width // 2
    own_columns = lax.dynamic_slice_in_dim(normed_both, side * half_width, half_width, axis=1)
    left = (own_columns * gain_attn.astype(F32)).astype(BF16)

    def partial_product(weight):
        product = dot_nn(left, weight)
        return product[:rows], swap_fsdp(product[rows:].astype(BF16))

    k_own, k_got = partial_product(key_weight)
    v_own, v_got = partial_product(value_weight)
    q_own, q_got = partial_product(w_query)
    own_kv = rotary_kv(k_own, k_got, v_own, v_got, cosine, sine)
    all_kv = gather_ctx(own_kv, 1)

    g_other = swap_fsdp(after(g_own, v_own))
    gains = jnp.stack([gain_attn, gain_ffn])
    gains = by_side(gains, swap_fsdp(gains), 1).astype(F32)
    gain_one, gain_two = gains[0], gains[1]
    core = me % 2
    out_half = w_out.shape[0] // 2
    mine = lax.dynamic_slice_in_dim(w_out, core * out_half, out_half, axis=0)
    mine = swap_fsdp(after(mine, v_own))
    theirs = swap_bit(mine, 0)
    out_other = jnp.where(
        core == 0,
        jnp.concatenate([mine, theirs], axis=0),
        jnp.concatenate([theirs, mine], axis=0),
    )
    full_out = by_side(w_out, out_other, 1)
    n1_turned = (normed_both * gain_one).astype(BF16).T

    mixed, lse, query = attention_forward(q_own, q_got, cosine, sine, all_kv, slot_of, owned, block)
    mixed_other = swap_fsdp(mixed)
    resid_mid = x_f + dot_nn(mixed, full_out)
    normed_two, inverse_two = norm_stats(resid_mid)
    n2 = (normed_two * gain_two).astype(BF16)

    places = jnp.concatenate([chunk_places(bits), chunk_places(bits_z)])
    gate_grad, up_grad, hidden, n2_chunks, g_chunks, n2_grad, n2_send, ffn_own, ffn_send = ffn(
        n2, swap_fsdp(n2), g_own, g_other, w_gate, w_up, w_down, places
    )
    n2_grad = n2_grad + swap_fsdp(n2_send).astype(F32)
    ffn_got = swap_fsdp(ffn_send)
    grad_gate = weight_grad(n2_chunks, gate_grad, bits)
    grad_up = weight_grad(n2_chunks, up_grad, bits)
    grad_down = weight_grad(g_chunks, hidden, bits_z).T

    mid_grad = g_own.astype(F32) + norm_back(n2_grad, normed_two, inverse_two, gain_two)
    mid_grad_b = mid_grad.astype(BF16)
    mid_other = swap_fsdp(mid_grad_b)
    mixed_grad = dot_nt(mid_grad_b, full_out).astype(BF16)
    row_pos = jnp.concatenate([positions.reshape(2, block)] * GROUP, axis=1).astype(F32)
    turned_angles = row_pos[:, None, :] * jnp.asarray(frequency_row(HEAD_SIZE))[None, :, None]
    turned_cosine = jnp.cos(turned_angles)
    turned_sine = jnp.sin(turned_angles) * jnp.asarray(sign_row(HEAD_SIZE))[None, :, None]
    dq, dk_parts, dv_parts = attention_backward(
        query,
        mixed_grad,
        mixed,
        lse,
        turned_cosine,
        turned_sine,
        all_kv,
        slot_of,
        owned,
        block_ids,
        block,
    )
    dk_sum, dv_sum = reduce_ctx([dk_parts, dv_parts], 2)
    dkv = rotary_back(dk_sum, dv_sum, cosine, sine)
    ffn_got = after(ffn_got, dq)
    mid_both = jnp.concatenate([mid_grad_b, mid_other], axis=0)
    mixed_both = jnp.concatenate([mixed, mixed_other], axis=0)
    block_output = (resid_mid + (ffn_own + ffn_got.astype(F32))).astype(BF16)
    dkv_both = jnp.concatenate([dkv, swap_fsdp(dkv)], axis=0)
    dq_both = jnp.concatenate([dq, swap_fsdp(dq)], axis=0)

    wide_rows = width // ctx_size
    wide_start = me % (ctx_size // 2) * wide_rows
    w_rows = [
        lax.dynamic_slice_in_dim(w, wide_start, wide_rows, axis=0).reshape(2, -1, w.shape[1])
        for w in after((w_query, key_weight, value_weight), dkv_both)
    ]
    w_rows = jnp.concatenate(w_rows, axis=2)
    w_got = swap_fsdp(pick(w_rows, 0, 1 - side))
    w_rows = jnp.where(side == me // (ctx_size // 2), pick(w_rows, 0, side), w_got)

    n1_grad = (
        dot_nt(dq_both, w_query)
        + dot_nt(dkv_both[:, :part], key_weight)
        + dot_nt(dkv_both[:, part:], value_weight)
    )
    n1_got = swap_fsdp(n1_grad[rows:].astype(BF16)).astype(F32)
    n1_grad = by_side(n1_grad[:rows], n1_got, 1)
    input_grad = mid_grad + norm_back(n1_grad, normed_one, inverse_one, gain_one)

    out_parts = side_parts(mid_both.T, mixed_both)
    query_parts = side_parts(n1_turned, dq_both)
    kv_parts = side_parts(n1_turned, dkv_both)
    grad_out, grad_query, grad_kv = reduce_ctx(
        [out_parts, query_parts, kv_parts], 3
    )
    grad_out = grad_out.T
    grad_key, grad_value = grad_kv[:, :part], grad_kv[:, part:]

    own_rows = wide_rows // 2
    first_row = (2 * me + side) * own_rows
    own_gains = lax.dynamic_slice_in_dim(gains, first_row, own_rows, axis=1)
    grads_one = jnp.concatenate([grad_query, grad_kv], axis=1)
    gain_one_grad = jnp.sum(w_rows.astype(F32) * grads_one, axis=1) / own_gains[0]
    gate_rows = lax.dynamic_slice_in_dim(w_gate, me * wide_rows, wide_rows, axis=0).astype(F32)
    up_rows = lax.dynamic_slice_in_dim(w_up, me * wide_rows, wide_rows, axis=0).astype(F32)
    sums = jnp.sum(gate_rows * grad_gate + up_rows * grad_up, axis=1).reshape(2, own_rows)
    sums = pick(sums, 0, side) + swap_fsdp(pick(sums, 0, 1 - side))
    gain_two_grad = sums / own_gains[1]

    return (
        block_output[None],
        input_grad[None],
        gain_one_grad,
        gain_two_grad,
        grad_query,
        grad_key,
        grad_value,
        grad_out,
        grad_gate,
        grad_up,
        grad_down,
    )


def solution(mesh):
    tokens, rows, columns, both = P(FSDP, CTX), P(FSDP), P(None, FSDP), P((CTX, FSDP))
    return jax.shard_map(
        local,
        mesh=mesh,
        in_specs=(tokens, tokens, P()) + (rows,) * 5 + (columns,) * 3 + (rows,),
        out_specs=(tokens, tokens) + (both,) * 5 + (P(None, (CTX, FSDP)),)
        + (P(CTX, FSDP),) * 2
        + (P(FSDP, CTX),),
        check_vma=False,
    )
```

```python
import functools
import math

import jax
import jax.numpy as jnp
import numpy as np
from jax import lax
from jax.experimental import pallas as pl
from jax.experimental.pallas import tpu as pltpu
from jax.sharding import PartitionSpec as P


QUERY_HEADS = 16
KEY_HEADS = 8
HEAD_SIZE = 96
GROUP = QUERY_HEADS // KEY_HEADS
LANES = 128
PAIR_LANES = 256
HEADS_STEP = 4
CTX, FSDP = "ctx", "fsdp"
TILE_BLOCKS = 4

EPS = 1e-05
THETA = 100000.0
NEGATIVE_FLOOR = -1e30
LOG2E = math.log2(math.e)
SCALE = HEAD_SIZE ** (-0.5)
VMEM_BYTES = 66_000_000
SMALL_VMEM_BYTES = 24_000_000

F32 = jnp.float32
BF16 = jnp.bfloat16


def dot_nn(left, right):
    return lax.dot_general(left, right, (((1,), (0,)), ((), ())), preferred_element_type=F32)


def dot_nt(left, right):
    return lax.dot_general(left, right, (((1,), (1,)), ((), ())), preferred_element_type=F32)


def frequency_row(width):
    lane = np.arange(width)
    half = HEAD_SIZE // 2
    freq = np.exp(-math.log(THETA) * 2.0 * (lane % HEAD_SIZE % half) / HEAD_SIZE)
    return freq.astype(np.float32)


def sign_row(width):
    lane = np.arange(width)
    return np.where(lane % HEAD_SIZE < HEAD_SIZE // 2, -1.0, 1.0).astype(np.float32)


def swap_halves(value):
    width = value.shape[1]
    half = HEAD_SIZE // 2
    lane = lax.broadcasted_iota(jnp.int32, value.shape, 1)
    lower = lax.rem(lane, HEAD_SIZE) < half
    return jnp.where(lower, pltpu.roll(value, width - half, 1), pltpu.roll(value, half, 1))


def rotary_kv_kernel(k_own, k_got, v_own, v_got, cosine, sine, out):
    width = k_own.shape[1]
    keys = k_own[...] + k_got[...].astype(F32)
    out[:, :width] = (keys * cosine[...] + swap_halves(keys) * sine[...]).astype(BF16)
    out[:, width:] = (v_own[...] + v_got[...].astype(F32)).astype(BF16)


def rotary_kv(k_own, k_got, v_own, v_got, cosine, sine):
    rows, width = k_own.shape
    return pl.pallas_call(
        rotary_kv_kernel,
        out_shape=jax.ShapeDtypeStruct((rows, 2 * width), BF16),
        cost_estimate=pl.CostEstimate(
            flops=8 * rows * width, bytes_accessed=20 * rows * width, transcendentals=0
        ),
    )(k_own, k_got, v_own, v_got, cosine, sine)


def rotary_back_kernel(keys, values, cosine, sine, out):
    width = keys.shape[1]
    total = keys[...]
    out[:, :width] = (total * cosine[...] - swap_halves(total) * sine[...]).astype(BF16)
    out[:, width:] = values[...].astype(BF16)


def rotary_back(keys, values, cosine, sine):
    rows, width = keys.shape
    return pl.pallas_call(
        rotary_back_kernel,
        out_shape=jax.ShapeDtypeStruct((rows, 2 * width), BF16),
        cost_estimate=pl.CostEstimate(
            flops=6 * rows * width, bytes_accessed=20 * rows * width, transcendentals=0
        ),
    )(keys, values, cosine, sine)


def pair_lanes(pair):
    return slice(pair * LANES, pair * LANES + PAIR_LANES)


def pair_rows(rows, pair):
    blocks = []
    for i in range(2 * GROUP):
        head = 2 * GROUP * pair + i
        offset = (2 * pair + i // GROUP) * HEAD_SIZE - pair * LANES
        pieces = [rows[:, head * HEAD_SIZE : (head + 1) * HEAD_SIZE]]
        if offset:
            pieces.insert(0, jnp.zeros((rows.shape[0], offset), rows.dtype))
        rest = PAIR_LANES - HEAD_SIZE - offset
        if rest:
            pieces.append(jnp.zeros((rows.shape[0], rest), rows.dtype))
        blocks.append(jnp.concatenate(pieces, axis=1))
    return jnp.concatenate(blocks, axis=0)


def tile_rows(ref, slot_of, tile, block):
    pieces = []
    for i in range(TILE_BLOCKS):
        start = pl.multiple_of(slot_of[tile * TILE_BLOCKS + i] * block, block)
        pieces.append(ref[pl.ds(start, block), :])
    return jnp.concatenate(pieces, axis=0)


def allowed(tile, tile_len, query_block, block, columns):
    key_pos = tile * tile_len + lax.broadcasted_iota(jnp.int32, (tile_len, columns), 0)
    column = lax.broadcasted_iota(jnp.int32, (tile_len, columns), 1)
    query_pos = query_block * block + lax.rem(column, block)
    return key_pos <= query_pos


def vmem_for(length):
    return SMALL_VMEM_BYTES if length <= 4096 else VMEM_BYTES


def fold(value, how):
    return how(value.reshape(value.shape[0] // 8, 8, value.shape[1]), axis=0)


def head_rows(turned, block):
    upright = turned.T.astype(BF16)
    return [upright[r * block : (r + 1) * block, :] for r in range(GROUP)]


def forward_kernel(
    block, slot_of, owned, q_own, q_got, cosine, sine, k_ref, v_ref, o_ref, lse_ref, q_ref, scores, acc, top, total
):
    query = q_own[...] + q_got[...].astype(F32)
    q_ref[...] = (query * cosine[...] + swap_halves(query) * sine[...]).astype(BF16)
    tile_len = TILE_BLOCKS * block
    pairs = HEADS_STEP // 2
    columns = 2 * GROUP * block
    per_head = GROUP * block

    def member(m, carry_all):
        first = pl.multiple_of(m * block, block)
        count = (owned[m] + TILE_BLOCKS) // TILE_BLOCKS
        q_rows = q_ref[pl.ds(first, block), :]
        queries = [pair_rows(q_rows, p) for p in range(pairs)]
        top[...] = jnp.full(top.shape, NEGATIVE_FLOOR, F32)
        total[...] = jnp.zeros(total.shape, F32)
        acc[...] = jnp.zeros(acc.shape, F32)

        def score_pass(tile, carry, queries=queries, m=m):
            start = pl.multiple_of(tile * tile_len, tile_len)
            mask = allowed(tile, tile_len, owned[m], block, columns)
            keys = tile_rows(k_ref, slot_of, tile, block)
            for p in range(pairs):
                value = dot_nt(keys[:, pair_lanes(p)], queries[p])
                value = jnp.where(mask, value * (SCALE * LOG2E), NEGATIVE_FLOOR)
                scores[p, pl.ds(start, tile_len), :] = value
                top[p] = jnp.maximum(top[p], fold(value, jnp.max))
            return carry

        lax.fori_loop(0, count, score_pass, 0)
        peaks = [jnp.max(top[p], axis=0, keepdims=True) for p in range(pairs)]

        def mix_pass(tile, carry, peaks=peaks):
            start = pl.multiple_of(tile * tile_len, tile_len)
            turned = tile_rows(v_ref, slot_of, tile, block).T
            for p in range(pairs):
                weight = jnp.exp2(scores[p, pl.ds(start, tile_len), :] - peaks[p])
                total[p] += fold(weight, jnp.sum)
                weight = weight.astype(BF16)
                for i in range(2):
                    h = 2 * p + i
                    acc[h] += dot_nn(
                        turned[h * HEAD_SIZE : (h + 1) * HEAD_SIZE, :],
                        weight[:, i * per_head : (i + 1) * per_head],
                    )
            return carry

        lax.fori_loop(0, count, mix_pass, 0)
        merged = []
        for p in range(pairs):
            denom = jnp.sum(total[p], axis=0, keepdims=True)
            lse_ref[p, pl.ds(m, 1), :] = peaks[p] + jnp.log2(denom)
            for i in range(2):
                merged += head_rows(acc[2 * p + i] / denom[:, i * per_head : (i + 1) * per_head], block)
        o_ref[pl.ds(first, block), :] = jnp.concatenate(merged, axis=1)
        return carry_all

    lax.fori_loop(0, 2, member, 0)


def kv_specs(length, heads_width):
    mode = {} if length <= 4096 else {"pipeline_mode": pl.Buffered(1)}
    return [
        pl.BlockSpec((length, heads_width), lambda i, *_, base=base: (0, base + i), **mode)
        for base in (0, KEY_HEADS // HEADS_STEP)
    ]


def attention_forward(q_own, q_got, cosine, sine, all_kv, slot_of, owned, block):
    rows = q_own.shape[0]
    length = all_kv.shape[0]
    steps = KEY_HEADS // HEADS_STEP
    pairs = HEADS_STEP // 2
    key_width = HEADS_STEP * HEAD_SIZE
    columns = 2 * GROUP * block
    query_spec = pl.BlockSpec((rows, key_width * GROUP), lambda i, *_: (0, i))
    table = pl.BlockSpec(cosine.shape, lambda i, *_: (0, 0))
    return pl.pallas_call(
        functools.partial(forward_kernel, block),
        out_shape=(
            jax.ShapeDtypeStruct(q_own.shape, BF16),
            jax.ShapeDtypeStruct((KEY_HEADS // 2, 2, columns), F32),
            jax.ShapeDtypeStruct(q_own.shape, BF16),
        ),
        grid_spec=pltpu.PrefetchScalarGridSpec(
            num_scalar_prefetch=2,
            grid=(steps,),
            in_specs=[query_spec, query_spec, table, table] + kv_specs(length, key_width),
            out_specs=[
                query_spec,
                pl.BlockSpec((pairs, 2, columns), lambda i, *_: (i, 0, 0)),
                query_spec,
            ],
            scratch_shapes=[
                pltpu.VMEM((pairs, length, columns), F32),
                pltpu.VMEM((HEADS_STEP, HEAD_SIZE, GROUP * block), F32),
                pltpu.VMEM((pairs, 8, columns), F32),
                pltpu.VMEM((pairs, 8, columns), F32),
            ],
        ),
        compiler_params=pltpu.CompilerParams(vmem_limit_bytes=VMEM_BYTES),
        cost_estimate=pl.CostEstimate(
            flops=4 * rows * length * q_own.shape[1] // 2,
            bytes_accessed=2 * all_kv.size,
            transcendentals=rows * length * QUERY_HEADS // 2,
        ),
    )(slot_of, owned, q_own, q_got, cosine, sine, all_kv, all_kv)


def backward_kernel(
    block,
    slot_of,
    owned,
    block_ids,
    q_ref,
    do_ref,
    o_ref,
    lse_ref,
    cos_ref,
    sin_ref,
    k_ref,
    v_ref,
    dq_ref,
    dk_out,
    dv_out,
    dk,
    dv,
    acc,
):
    tile_len = TILE_BLOCKS * block
    pairs = HEADS_STEP // 2
    columns = 2 * GROUP * block
    per_head = GROUP * block
    dk[...] = jnp.zeros_like(dk)
    dv[...] = jnp.zeros_like(dv)

    def one_member(m, carry_all):
        count = (owned[m] + TILE_BLOCKS) // TILE_BLOCKS
        member = pl.ds(pl.multiple_of(m * block, block), block)
        q_rows, g_rows, o_rows = q_ref[member, :], do_ref[member, :], o_ref[member, :]
        queries = [pair_rows(q_rows, p) for p in range(pairs)]
        grads = [pair_rows(g_rows, p) for p in range(pairs)]
        deltas = []
        for p in range(pairs):
            product = grads[p].astype(F32) * pair_rows(o_rows, p).astype(F32)
            deltas.append(jnp.sum(product.T, axis=0, keepdims=True))
        lses = [lse_ref[p, pl.ds(m, 1), :] for p in range(pairs)]
        acc[...] = jnp.zeros(acc.shape, F32)

        def grad_pass(tile, carry, queries=queries, grads=grads, deltas=deltas, lses=lses, m=m):
            start = pl.multiple_of(tile * tile_len, tile_len)
            mask = allowed(tile, tile_len, owned[m], block, columns)
            keys = tile_rows(k_ref, slot_of, tile, block)
            values = tile_rows(v_ref, slot_of, tile, block)
            turned = keys.T
            for p in range(pairs):
                lanes = pair_lanes(p)
                value = dot_nt(keys[:, lanes], queries[p])
                value = jnp.where(mask, value * (SCALE * LOG2E) - lses[p], NEGATIVE_FLOOR)
                prob = jnp.exp2(value)
                grad_prob = dot_nt(values[:, lanes], grads[p])
                grad_score = (prob * (grad_prob - deltas[p]) * SCALE).astype(BF16)
                dk[pl.ds(start, tile_len), lanes] += dot_nn(grad_score, queries[p])
                dv[pl.ds(start, tile_len), lanes] += dot_nn(prob.astype(BF16), grads[p])
                for i in range(2):
                    h = 2 * p + i
                    acc[h] += dot_nn(
                        turned[h * HEAD_SIZE : (h + 1) * HEAD_SIZE, :],
                        grad_score[:, i * per_head : (i + 1) * per_head],
                    )
            return carry

        lax.fori_loop(0, count, grad_pass, 0)
        merged = []
        for h in range(HEADS_STEP):
            grad = acc[h]
            middle = HEAD_SIZE // 2
            swapped = jnp.concatenate([grad[middle:], grad[:middle]], axis=0)
            merged += head_rows(grad * cos_ref[m] - swapped * sin_ref[m], block)
        dq_ref[member, :] = jnp.concatenate(merged, axis=1)
        return carry_all

    lax.fori_loop(0, 2, one_member, 0)

    def unpack(chunk, carry):
        for source, target in ((dk, dk_out), (dv, dv_out)):
            for i in range(2):
                start = pl.multiple_of(block_ids[2 * chunk + i] * block, block)
                target[chunk, i * block : (i + 1) * block, :] = source[pl.ds(start, block), :].astype(BF16)
        return carry

    lax.fori_loop(0, dk_out.shape[0], unpack, 0)


def attention_backward(
    query, grad, mixed, lse, cosine, sine, all_kv, slot_of, owned, block_ids, block
):
    rows = query.shape[0]
    length = all_kv.shape[0]
    chunks = length // rows
    steps = KEY_HEADS // HEADS_STEP
    pairs = HEADS_STEP // 2
    key_width = HEADS_STEP * HEAD_SIZE
    columns = 2 * GROUP * block
    query_spec = pl.BlockSpec((rows, key_width * GROUP), lambda i, *_: (0, i))
    mode = {} if length <= 4096 else {"pipeline_mode": pl.Buffered(1)}
    out_spec = pl.BlockSpec((chunks, rows, key_width), lambda i, *_: (0, 0, i), **mode)
    table = pl.BlockSpec(cosine.shape, lambda i, *_: (0, 0, 0))
    grad_shape = jax.ShapeDtypeStruct((chunks, rows, all_kv.shape[1] // 2), BF16)
    return pl.pallas_call(
        functools.partial(backward_kernel, block),
        out_shape=(jax.ShapeDtypeStruct(query.shape, BF16),) + (grad_shape,) * 2,
        grid_spec=pltpu.PrefetchScalarGridSpec(
            num_scalar_prefetch=3,
            grid=(steps,),
            in_specs=[
                query_spec,
                query_spec,
                query_spec,
                pl.BlockSpec((pairs, 2, columns), lambda i, *_: (i, 0, 0)),
                table,
                table,
            ]
            + kv_specs(length, key_width),
            out_specs=[query_spec] + [out_spec] * 2,
            scratch_shapes=[
                pltpu.VMEM((length, key_width), F32),
                pltpu.VMEM((length, key_width), F32),
                pltpu.VMEM((HEADS_STEP, HEAD_SIZE, GROUP * block), F32),
            ],
        ),
        compiler_params=pltpu.CompilerParams(vmem_limit_bytes=VMEM_BYTES),
        cost_estimate=pl.CostEstimate(
            flops=10 * rows * length * query.shape[1] // 2,
            bytes_accessed=4 * all_kv.size,
            transcendentals=rows * length * QUERY_HEADS // 2,
        ),
    )(slot_of, owned, block_ids, query, grad, mixed, lse, cosine, sine, all_kv, all_kv)


def place():
    me = lax.axis_index(CTX)
    return me // 4, me // 2 % 2, me % 2


def device_at(line, mid, core):
    return {CTX: (line * 2 + mid) * 2 + core}


def greet(line, mid, core, count):
    barrier = pltpu.get_barrier_semaphore()

    def call(*where):
        pl.semaphore_signal(
            barrier, inc=1, device_id=device_at(*where), device_id_type=pl.DeviceIdType.MESH
        )

    call(line, 1 - mid, core)
    call(line, mid, 1 - core)

    @pl.when(line > 0)
    def _():
        call(line - 1, mid, core)

    @pl.when(line + 1 < count)
    def _():
        call(line + 1, mid, core)

    ends = jnp.where(line > 0, 1, 0) + jnp.where(line + 1 < count, 1, 0)
    pl.semaphore_wait(barrier, 2 + ends)


def remote(source, target, send, recv, where):
    return pltpu.make_async_remote_copy(
        src_ref=source,
        dst_ref=target,
        send_sem=send,
        recv_sem=recv,
        device_id=device_at(*where),
        device_id_type=pl.DeviceIdType.MESH,
    )


def gather_kernel(
    count, own, out, here, right_send, left_send, mid_send, core_send, line_recv, mid_recv, core_recv
):
    line, mid, core = place()
    rows = own.shape[0]
    greet(line, mid, core, count)

    def slot(j, m, k):
        start = pl.multiple_of(((j * 2 + m) * 2 + k) * rows, rows)
        return out.at[pl.ds(start, rows)]

    def to_right(j, source):
        return remote(source, slot(j, mid, core), right_send.at[j], line_recv.at[j], (line + 1, mid, core))

    def to_left(j, source):
        return remote(source, slot(j, mid, core), left_send.at[j], line_recv.at[j], (line - 1, mid, core))

    def to_mid(j, source):
        return remote(source, slot(j, mid, core), mid_send.at[j], mid_recv.at[j], (line, 1 - mid, core))

    def to_core(j, m, source):
        return remote(
            source, slot(j, m, core), core_send.at[2 * j + m], core_recv.at[2 * j + m], (line, mid, 1 - core)
        )

    keep = pltpu.make_async_copy(own, slot(line, mid, core), here)
    keep.start()
    to_mid(line, own).start()

    @pl.when(line + 1 < count)
    def _():
        to_right(line, own).start()

    @pl.when(line > 0)
    def _():
        to_left(line, own).start()

    to_core(line, mid, own).start()


    def arrived_line(j, step_right):
        block = slot(j, mid, core)
        to_right(j, block).wait_recv()
        if step_right:

            @pl.when(line + 1 < count)
            def _():
                to_right(j, block).start()

        else:

            @pl.when(line > 0)
            def _():
                to_left(j, block).start()

        to_mid(j, block).start()
        to_core(j, mid, block).start()

    def arrived_mid(j):
        block = slot(j, 1 - mid, core)
        remote(block, block, mid_send.at[j], mid_recv.at[j], (line, 1 - mid, core)).wait_recv()
        to_core(j, 1 - mid, block).start()

    for step in range(1, count + 1):
        if step < count:

            @pl.when(line - step >= 0)
            def _(step=step):
                arrived_line(line - step, True)

            @pl.when(line + step < count)
            def _(step=step):
                arrived_line(line + step, False)

        if step == 1:
            arrived_mid(line)
        else:

            @pl.when(line - (step - 1) >= 0)
            def _(step=step):
                arrived_mid(line - (step - 1))

            @pl.when(line + (step - 1) < count)
            def _(step=step):
                arrived_mid(line + (step - 1))

    for j in range(count):
        for m in range(2):
            block = slot(j, m, 1 - core)
            remote(
                block, block, core_send.at[2 * j + m], core_recv.at[2 * j + m], (line, mid, 1 - core)
            ).wait_recv()
    keep.wait()
    for j in range(count):
        block = slot(j, mid, core)
        to_mid(j, block).wait_send()
        for m in range(2):
            to_core(j, m, slot(j, m, core)).wait_send()

        @pl.when(jnp.logical_and(j <= line, line + 1 < count))
        def _(j=j, block=block):
            to_right(j, block).wait_send()

        @pl.when(jnp.logical_and(j >= line, line > 0))
        def _(j=j, block=block):
            to_left(j, block).wait_send()


def gather_ctx(own, collective_id):
    size = lax.axis_size(CTX)
    rows, width = own.shape
    count = size // 4
    dma = pltpu.SemaphoreType.DMA
    return pl.pallas_call(
        functools.partial(gather_kernel, count),
        out_shape=jax.ShapeDtypeStruct((size * rows, width), own.dtype),
        in_specs=[pl.BlockSpec(memory_space=pltpu.VMEM)],
        out_specs=pl.BlockSpec(memory_space=pl.ANY),
        scratch_shapes=[dma(())] + [dma((count,))] * 3 + [dma((2 * count,))] + [dma((count,))] * 2 + [dma((2 * count,))],
        compiler_params=pltpu.CompilerParams(
            collective_id=collective_id, has_side_effects=True, vmem_limit_bytes=SMALL_VMEM_BYTES
        ),
        cost_estimate=pl.CostEstimate(
            flops=0, bytes_accessed=100 * size * rows * width, transcendentals=0
        ),
    )(own)


def reduce_kernel(count, parts, *refs):
    sources, outs = refs[:parts], refs[parts : 2 * parts]
    scratch = refs[2 * parts :]
    work, from_core, from_mid, from_right, from_left = (scratch[i * parts : (i + 1) * parts] for i in range(5))
    (load, core_send, core_recv, mid_send, mid_recv, left_send, right_send, right_recv, left_recv) = scratch[5 * parts :]
    line, mid, core = place()
    greet(line, mid, core, count)

    def nearest_last(visit):
        def body(i, carry):
            step = count - 1 - i // 2
            j = line + step * (2 * (i % 2) - 1)

            @pl.when(jnp.logical_and(j >= 0, j < count))
            def _():
                visit(j)

            return carry

        lax.fori_loop(0, 2 * count - 1, body, 0)

    def core_copy(s, j, m):
        index = 2 * j + m
        return remote(
            sources[s].at[2 * index + (1 - core)],
            from_core[s].at[index],
            core_send.at[s, index],
            core_recv.at[s, index],
            (line, mid, 1 - core),
        )

    def load_copy(s, j, m):
        index = 2 * j + m
        return pltpu.make_async_copy(sources[s].at[2 * index + core], work[s].at[index], load.at[s, index])

    def mid_copy(s, j):
        return remote(
            work[s].at[2 * j + (1 - mid)],
            from_mid[s].at[j],
            mid_send.at[s, j],
            mid_recv.at[s, j],
            (line, 1 - mid, core),
        )

    def left_copy(s, j):
        return remote(
            work[s].at[2 * j + mid],
            from_right[s].at[j],
            left_send.at[s, j],
            right_recv.at[s, j],
            (line - 1, mid, core),
        )

    def right_copy(s, j):
        return remote(
            work[s].at[2 * j + mid],
            from_left[s].at[j],
            right_send.at[s, j],
            left_recv.at[s, j],
            (line + 1, mid, core),
        )

    def add(s, index, other):
        work[s][index] = (work[s][index].astype(F32) + other.astype(F32)).astype(work[s].dtype)

    for m in (1 - mid, mid):

        def begin(j, m=m):
            for s in range(parts):
                core_copy(s, j, m).start()
                load_copy(s, j, m).start()

        nearest_last(begin)

    def core_sum(s, j, m):
        core_copy(s, j, m).wait_recv()
        load_copy(s, j, m).wait()
        add(s, 2 * j + m, from_core[s][2 * j + m])

    def to_mid(j):
        for s in range(parts):
            core_sum(s, j, 1 - mid)
            mid_copy(s, j).start()

    nearest_last(to_mid)

    def keep_mine(j):
        for s in range(parts):
            core_sum(s, j, mid)

    nearest_last(keep_mine)

    def along(j):
        for s in range(parts):
            mid_copy(s, j).wait_recv()
            add(s, 2 * j + mid, from_mid[s][j])

            @pl.when(j < line)
            def _(s=s):
                @pl.when(line + 1 < count)
                def _():
                    left_copy(s, j).wait_recv()
                    add(s, 2 * j + mid, from_right[s][j])

                left_copy(s, j).start()

            @pl.when(j > line)
            def _(s=s):
                @pl.when(line > 0)
                def _():
                    right_copy(s, j).wait_recv()
                    add(s, 2 * j + mid, from_left[s][j])

                right_copy(s, j).start()

    nearest_last(along)
    for s in range(parts):
        outs[s][...] = work[s][2 * line + mid].astype(F32)

        @pl.when(line + 1 < count)
        def _(s=s):
            left_copy(s, line).wait_recv()
            outs[s][...] += from_right[s][line].astype(F32)

        @pl.when(line > 0)
        def _(s=s):
            right_copy(s, line).wait_recv()
            outs[s][...] += from_left[s][line].astype(F32)

    for s in range(parts):
        for j in range(count):
            mid_copy(s, j).wait_send()
            for m in range(2):
                core_copy(s, j, m).wait_send()

            @pl.when(j < line)
            def _(s=s, j=j):
                left_copy(s, j).wait_send()

            @pl.when(j > line)
            def _(s=s, j=j):
                right_copy(s, j).wait_send()


def reduce_ctx(sources, collective_id):
    size = lax.axis_size(CTX)
    count = size // 4
    parts = len(sources)
    dma = pltpu.SemaphoreType.DMA

    def room(chunks):
        return [pltpu.VMEM((chunks,) + source.shape[1:], source.dtype) for source in sources]

    return pl.pallas_call(
        functools.partial(reduce_kernel, count, parts),
        out_shape=[jax.ShapeDtypeStruct(source.shape[1:], F32) for source in sources],
        in_specs=[pl.BlockSpec(memory_space=pl.ANY)] * parts,
        out_specs=[pl.BlockSpec(memory_space=pltpu.VMEM)] * parts,
        scratch_shapes=room(2 * count) + room(2 * count) + room(count) * 1 + room(count) + room(count)
        + [dma((parts, 2 * count))] * 3
        + [dma((parts, count))] * 6,
        compiler_params=pltpu.CompilerParams(
            collective_id=collective_id,
            has_side_effects=True,
            vmem_limit_bytes=vmem_for(size * sources[0].shape[1]),
        ),
        cost_estimate=pl.CostEstimate(
            flops=0, bytes_accessed=100 * sum(source.size for source in sources), transcendentals=0
        ),
    )(*sources)


def swap_fsdp(value):
    size = lax.axis_size(FSDP)
    return lax.ppermute(value, FSDP, [(i, size - 1 - i) for i in range(size)])


def swap_bit(value, bit):
    size = lax.axis_size(CTX)
    return lax.ppermute(value, CTX, [(i, i ^ (1 << bit)) for i in range(size)])


def bit_order(size, swapped=False):
    bits = list(range(size.bit_length() - 1))
    if swapped and len(bits) > 2:
        bits[1], bits[2] = bits[2], bits[1]
    return bits


def relative_order(bits):
    last = len(bits) - 1
    return [
        sum(((p >> (last - i)) & 1) << bit for i, bit in enumerate(bits)) for p in range(2 << last)
    ]


def chunk_places(bits):
    place_of = np.argsort(np.asarray(relative_order(bits))).astype(np.int32)
    me = lax.axis_index(CTX)
    distance = jnp.arange(len(place_of), dtype=jnp.int32) ^ me
    found = distance[:, None] == jnp.arange(len(place_of), dtype=jnp.int32)[None, :]
    return jnp.sum(jnp.where(found, jnp.asarray(place_of)[None, :], 0), axis=1)


def pick(value, axis, index):
    return lax.dynamic_index_in_dim(value, index, axis, keepdims=False)


def halve(keep, send, bits):
    for bit in bits:
        got = swap_bit(send, bit)
        if keep.shape[0] == 1:
            return keep[0].astype(F32) + got[0].astype(F32)
        mid = keep.shape[0] // 2
        send = (keep[mid:].astype(F32) + got[mid:].astype(F32)).astype(BF16)
        keep = (keep[:mid].astype(F32) + got[:mid].astype(F32)).astype(BF16)


def weight_grad(left, right, bits):
    count, rows, tokens = left.shape

    def piece(part):
        product = dot_nn(part.reshape(count // 2 * rows, tokens), right)
        return product.astype(BF16).reshape(count // 2, rows, right.shape[1])

    send = piece(left[count // 2 :])
    keep = piece(left[: count // 2])
    return halve(keep, send, bits)


def ffn_kernel(
    places, n_own, n_other, g_own, g_other, w_gate, w_up, w_down,
    gate_out, up_out, hidden_out, n_chunks, g_chunks, ng_own, ng_send, ffn_own, ffn_send,
    n_both, g_both, n_grad, ffn_sum,
):
    step, steps = pl.program_id(0), pl.num_programs(0)
    rows = n_own.shape[0]
    count, chunk, _ = n_chunks.shape

    @pl.when(step == 0)
    def _():
        n_both[:rows], n_both[rows:] = n_own[...], n_other[...]
        g_both[:rows], g_both[rows:] = g_own[...], g_other[...]
        for source, target, base in ((n_both, n_chunks, 0), (g_both, g_chunks, count)):
            turned = source[...].astype(F32).T
            for c in range(count):
                target[places[base + c]] = turned[c * chunk : (c + 1) * chunk, :].astype(BF16)
        n_grad[...] = jnp.zeros(n_grad.shape, F32)
        ffn_sum[...] = jnp.zeros(ffn_sum.shape, F32)

    wg, wu, wd = w_gate[...], w_up[...], w_down[...]
    gate = dot_nn(n_both[...], wg)
    up = dot_nn(n_both[...], wu)
    hidden_grad = dot_nt(g_both[...], wd)
    sig = jax.nn.sigmoid(gate)
    silu = gate * sig
    hidden = (silu * up).astype(BF16)
    gate_grad = (hidden_grad * up * sig * (1.0 + gate * (1.0 - sig))).astype(BF16)
    up_grad = (hidden_grad * silu).astype(BF16)
    gate_out[...], up_out[...], hidden_out[...] = gate_grad, up_grad, hidden
    n_grad[...] += dot_nt(gate_grad, wg) + dot_nt(up_grad, wu)
    ffn_sum[...] += dot_nn(hidden, wd)

    @pl.when(step == steps - 1)
    def _():
        ng_own[...], ng_send[...] = n_grad[:rows], n_grad[rows:].astype(BF16)
        ffn_own[...], ffn_send[...] = ffn_sum[:rows], ffn_sum[rows:].astype(BF16)


def ffn(n_own, n_other, g_own, g_other, w_gate, w_up, w_down, places):
    rows, width = n_own.shape
    hidden = w_gate.shape[1]
    count = places.shape[0] // 2
    tile = min(256, hidden)
    whole = pl.BlockSpec((rows, width), lambda i, *_: (0, 0))
    columns = pl.BlockSpec((width, tile), lambda i, *_: (0, i))
    acts = pl.BlockSpec((2 * rows, tile), lambda i, *_: (0, i))
    chunks = pl.BlockSpec((count, width // count, 2 * rows), lambda i, *_: (0, 0, 0))
    act = jax.ShapeDtypeStruct((2 * rows, hidden), BF16)
    turned = jax.ShapeDtypeStruct((count, width // count, 2 * rows), BF16)
    own = jax.ShapeDtypeStruct((rows, width), F32)
    send = jax.ShapeDtypeStruct((rows, width), BF16)
    return pl.pallas_call(
        ffn_kernel,
        out_shape=(act, act, act, turned, turned, own, send, own, send),
        grid_spec=pltpu.PrefetchScalarGridSpec(
            num_scalar_prefetch=1,
            grid=(hidden // tile,),
            in_specs=[whole] * 4
            + [columns, columns, pl.BlockSpec((tile, width), lambda i, *_: (i, 0))],
            out_specs=[acts] * 3 + [chunks] * 2 + [whole] * 4,
            scratch_shapes=[
                pltpu.VMEM((2 * rows, width), BF16),
                pltpu.VMEM((2 * rows, width), BF16),
                pltpu.VMEM((2 * rows, width), F32),
                pltpu.VMEM((2 * rows, width), F32),
            ],
        ),
        compiler_params=pltpu.CompilerParams(vmem_limit_bytes=2 * SMALL_VMEM_BYTES),
        cost_estimate=pl.CostEstimate(
            flops=24 * rows * width * hidden,
            bytes_accessed=6 * width * hidden + 12 * rows * hidden,
            transcendentals=2 * rows * hidden,
        ),
    )(places, n_own, n_other, g_own, g_other, w_gate, w_up, w_down)


def side_parts(left, right):
    size = lax.axis_size(CTX)
    width, tokens = left.shape
    rows = width // (2 * size)
    flat = pick(left.reshape(size, 2, rows, tokens), 1, lax.axis_index(FSDP))
    product = dot_nn(flat.reshape(size * rows, tokens), right).astype(BF16)
    return product.reshape(size, rows, right.shape[1])


def after(value, anchor):
    return lax.optimization_barrier((value, anchor))[0]


def norm_stats(value):
    inverse = lax.rsqrt(jnp.mean(value * value, axis=-1, keepdims=True) + EPS)
    return (value * inverse, inverse)


def norm_back(grad, normed, inverse, gain):
    scaled = grad * gain
    return inverse * (scaled - normed * jnp.mean(scaled * normed, axis=-1, keepdims=True))


def local(
    block_input,
    out_grad,
    block_ids,
    gain_attn,
    gain_ffn,
    w_query,
    key_weight,
    value_weight,
    w_out,
    w_gate,
    w_up,
    w_down,
):
    ctx_size = lax.axis_size(CTX)
    side = lax.axis_index(FSDP)
    me = lax.axis_index(CTX)
    rows, width = block_input.shape[1:]
    block = rows // 2
    block_count = 2 * ctx_size

    def by_side(own, other, axis):
        return jnp.where(
            side == 0,
            jnp.concatenate([own, other], axis=axis),
            jnp.concatenate([other, own], axis=axis),
        )

    x_own = block_input[0]
    g_own = out_grad[0]
    x_other = swap_fsdp(x_own)

    block_range = jnp.arange(block_count, dtype=jnp.int32)
    slot_of = jnp.sum(
        jnp.where(block_ids[None, :] == block_range[:, None], block_range[None, :], 0), axis=1
    ).astype(jnp.int32)
    owned = lax.dynamic_slice(block_ids, (2 * me,), (2,))
    positions = (
        owned[:, None] * block + jnp.arange(block, dtype=jnp.int32)[None, :]
    ).reshape(rows)
    part = KEY_HEADS * HEAD_SIZE
    angles = positions.astype(F32)[:, None] * jnp.asarray(frequency_row(part))[None, :]
    cosine = jnp.cos(angles)
    sine = jnp.sin(angles) * jnp.asarray(sign_row(part))[None, :]
    bits, bits_z = bit_order(ctx_size), bit_order(ctx_size, True)

    x_f = x_own.astype(F32)
    normed_one, inverse_one = norm_stats(x_f)
    normed_both = jnp.concatenate([normed_one, norm_stats(x_other.astype(F32))[0]], axis=0)
    half_width = width // 2
    own_columns = lax.dynamic_slice_in_dim(normed_both, side * half_width, half_width, axis=1)
    left = (own_columns * gain_attn.astype(F32)).astype(BF16)

    def partial_product(weight):
        product = dot_nn(left, weight)
        return product[:rows], swap_fsdp(product[rows:].astype(BF16))

    k_own, k_got = partial_product(key_weight)
    v_own, v_got = partial_product(value_weight)
    q_own, q_got = partial_product(w_query)
    own_kv = rotary_kv(k_own, k_got, v_own, v_got, cosine, sine)
    all_kv = gather_ctx(own_kv, 1)

    g_other = swap_fsdp(after(g_own, v_own))
    gains = jnp.stack([gain_attn, gain_ffn])
    gains = by_side(gains, swap_fsdp(gains), 1).astype(F32)
    gain_one, gain_two = gains[0], gains[1]
    core = me % 2
    out_half = w_out.shape[0] // 2
    mine = lax.dynamic_slice_in_dim(w_out, core * out_half, out_half, axis=0)
    mine = swap_fsdp(after(mine, v_own))
    theirs = swap_bit(mine, 0)
    out_other = jnp.where(
        core == 0,
        jnp.concatenate([mine, theirs], axis=0),
        jnp.concatenate([theirs, mine], axis=0),
    )
    full_out = by_side(w_out, out_other, 1)
    n1_turned = (normed_both * gain_one).astype(BF16).T

    mixed, lse, query = attention_forward(q_own, q_got, cosine, sine, all_kv, slot_of, owned, block)
    mixed_other = swap_fsdp(mixed)
    resid_mid = x_f + dot_nn(mixed, full_out)
    normed_two, inverse_two = norm_stats(resid_mid)
    n2 = (normed_two * gain_two).astype(BF16)

    places = jnp.concatenate([chunk_places(bits), chunk_places(bits_z)])
    gate_grad, up_grad, hidden, n2_chunks, g_chunks, n2_grad, n2_send, ffn_own, ffn_send = ffn(
        n2, swap_fsdp(n2), g_own, g_other, w_gate, w_up, w_down, places
    )
    n2_grad = n2_grad + swap_fsdp(n2_send).astype(F32)
    ffn_got = swap_fsdp(ffn_send)
    grad_gate = weight_grad(n2_chunks, gate_grad, bits)
    grad_up = weight_grad(n2_chunks, up_grad, bits)
    grad_down = weight_grad(g_chunks, hidden, bits_z).T

    mid_grad = g_own.astype(F32) + norm_back(n2_grad, normed_two, inverse_two, gain_two)
    mid_grad_b = mid_grad.astype(BF16)
    mid_other = swap_fsdp(mid_grad_b)
    mixed_grad = dot_nt(mid_grad_b, full_out).astype(BF16)
    row_pos = jnp.concatenate([positions.reshape(2, block)] * GROUP, axis=1).astype(F32)
    turned_angles = row_pos[:, None, :] * jnp.asarray(frequency_row(HEAD_SIZE))[None, :, None]
    turned_cosine = jnp.cos(turned_angles)
    turned_sine = jnp.sin(turned_angles) * jnp.asarray(sign_row(HEAD_SIZE))[None, :, None]
    dq, dk_parts, dv_parts = attention_backward(
        query,
        mixed_grad,
        mixed,
        lse,
        turned_cosine,
        turned_sine,
        all_kv,
        slot_of,
        owned,
        block_ids,
        block,
    )
    dk_sum, dv_sum = reduce_ctx([dk_parts, dv_parts], 2)
    dkv = rotary_back(dk_sum, dv_sum, cosine, sine)
    ffn_got = after(ffn_got, dq)
    mid_both = jnp.concatenate([mid_grad_b, mid_other], axis=0)
    mixed_both = jnp.concatenate([mixed, mixed_other], axis=0)
    block_output = (resid_mid + (ffn_own + ffn_got.astype(F32))).astype(BF16)
    dkv_both = jnp.concatenate([dkv, swap_fsdp(dkv)], axis=0)
    dq_both = jnp.concatenate([dq, swap_fsdp(dq)], axis=0)

    wide_rows = width // ctx_size
    wide_start = me % (ctx_size // 2) * wide_rows
    w_rows = [
        lax.dynamic_slice_in_dim(w, wide_start, wide_rows, axis=0).reshape(2, -1, w.shape[1])
        for w in after((w_query, key_weight, value_weight), dkv_both)
    ]
    w_rows = jnp.concatenate(w_rows, axis=2)
    w_got = swap_fsdp(pick(w_rows, 0, 1 - side))
    w_rows = jnp.where(side == me // (ctx_size // 2), pick(w_rows, 0, side), w_got)

    n1_grad = (
        dot_nt(dq_both, w_query)
        + dot_nt(dkv_both[:, :part], key_weight)
        + dot_nt(dkv_both[:, part:], value_weight)
    )
    n1_got = swap_fsdp(n1_grad[rows:].astype(BF16)).astype(F32)
    n1_grad = by_side(n1_grad[:rows], n1_got, 1)
    input_grad = mid_grad + norm_back(n1_grad, normed_one, inverse_one, gain_one)

    out_parts = side_parts(mid_both.T, mixed_both)
    query_parts = side_parts(n1_turned, dq_both)
    kv_parts = side_parts(n1_turned, dkv_both)
    grad_out, grad_query, grad_kv = reduce_ctx(
        [out_parts, query_parts, kv_parts], 3
    )
    grad_out = grad_out.T
    grad_key, grad_value = grad_kv[:, :part], grad_kv[:, part:]

    own_rows = wide_rows // 2
    first_row = (2 * me + side) * own_rows
    own_gains = lax.dynamic_slice_in_dim(gains, first_row, own_rows, axis=1)
    grads_one = jnp.concatenate([grad_query, grad_kv], axis=1)
    gain_one_grad = jnp.sum(w_rows.astype(F32) * grads_one, axis=1) / own_gains[0]
    gate_rows = lax.dynamic_slice_in_dim(w_gate, me * wide_rows, wide_rows, axis=0).astype(F32)
    up_rows = lax.dynamic_slice_in_dim(w_up, me * wide_rows, wide_rows, axis=0).astype(F32)
    sums = jnp.sum(gate_rows * grad_gate + up_rows * grad_up, axis=1).reshape(2, own_rows)
    sums = pick(sums, 0, side) + swap_fsdp(pick(sums, 0, 1 - side))
    gain_two_grad = sums / own_gains[1]

    return (
        block_output[None],
        input_grad[None],
        gain_one_grad,
        gain_two_grad,
        grad_query,
        grad_key,
        grad_value,
        grad_out,
        grad_gate,
        grad_up,
        grad_down,
    )


def solution(mesh):
    tokens, rows, columns, both = P(FSDP, CTX), P(FSDP), P(None, FSDP), P((CTX, FSDP))
    return jax.shard_map(
        local,
        mesh=mesh,
        in_specs=(tokens, tokens, P()) + (rows,) * 5 + (columns,) * 3 + (rows,),
        out_specs=(tokens, tokens) + (both,) * 5 + (P(None, (CTX, FSDP)),)
        + (P(CTX, FSDP),) * 2
        + (P(FSDP, CTX),),
        check_vma=False,
    )
```
